32 devices in a mesh: grp: 4 (over y, core), rep: 8 (over z, x).
Axes of the slice: x: 2, y: 2, z: 4, core: 2. Of those that a mesh axis runs over, the one named last changes fastest.
Arguments:
- embeddings: bfloat16 [16384, 768], P(('grp', 'rep')), may hold values from -6 to 6
- cluster_ids: int32 [16384], P(('grp', 'rep')), may hold values from 0 to 12287, as said below
- owner_bounds: int32 [32], replicated, may hold values from 0 to 12287, as said below
Outputs:
- distance: float32 [16384], P(('grp', 'rep'))
- slot_index: int32 [16384], P(('grp', 'rep'))
- centroids: bfloat16 [32, 576, 768], P(('grp', 'rep'))
The draws below stay inside these ranges and needn't reach their ends.
Inputs may be any that keep to these rules, and one draw needn't show every extreme that they name: `cluster_ids`: in the rows of one device at most 48 rows belong to the clusters of one owner (owner o holds clusters owner_bounds[o] up to the next bound); in every draw some owner gets exactly 48 rows from every device. `owner_bounds`: owners are ordered grp first, then rep. The bounds rise from 0; each owner holds from 192 to 576 clusters, the last owner ending at 12288; some owner holds exactly 576.
All inputs are finite; a program needn't handle non-finite values.
Results may differ from the reference program's by a relative error of at most 0.004.
Values may be sent and summed in bfloat16 or wider, within the bound.
A program may use at most 128 MiB of HBM per device.

```python
import jax
import jax.numpy as jnp
from jax import lax

D = 768
ROWS_DEV = 512
CL_DEV = 384
OWNERS = 32
ROWS = 16384
SLOT = 48
OWN_MAX = 576


def owner_layout(key):
    half_count = OWNERS // 2
    spread = CL_DEV // 2
    base_key = jax.random.fold_in(key, 11)
    first_key, second_key, third_key, fourth_key = jax.random.split(base_key, 4)
    deltas = jax.random.randint(first_key, (half_count,), -spread, spread + 1)
    chosen = jax.random.randint(second_key, (), 0, half_count)
    deltas = jnp.where(jnp.arange(half_count) == chosen, spread, deltas)
    widths = jnp.concatenate([CL_DEV + deltas, CL_DEV - deltas]).astype(jnp.int32)
    widths = jax.random.permutation(third_key, widths)
    bounds = (jnp.cumsum(widths) - widths).astype(jnp.int32)
    busy_owner = jax.random.randint(fourth_key, (), 0, OWNERS).astype(jnp.int32)
    return (bounds, widths, busy_owner)


def draw_owner_bounds(key, part):
    return owner_layout(key)[0]


def draw_cluster_ids(key, part):
    bounds, widths, busy_owner = owner_layout(key)
    pool_size = (OWNERS - 1) * (SLOT - 1)

    def one_device(device_index):
        device_key = jax.random.fold_in(jax.random.fold_in(key, 23), device_index)
        first_key, second_key, third_key = jax.random.split(device_key, 3)
        owner_pool = jnp.arange(pool_size, dtype=jnp.int32) % (OWNERS - 1)
        chosen = jax.random.permutation(first_key, owner_pool)[:ROWS_DEV - SLOT]
        chosen = chosen + (chosen >= busy_owner).astype(jnp.int32)
        owner_of = jnp.concatenate([jnp.full((SLOT,), busy_owner, jnp.int32), chosen])
        offsets = jax.random.randint(second_key, (ROWS_DEV,), 0, 1 << 30) % widths[owner_of]
        identity = (bounds[owner_of] + offsets).astype(jnp.int32)
        return jax.random.permutation(third_key, identity)
    return jax.vmap(one_device)(jnp.arange(OWNERS)).reshape(-1)


def block_scale(rng, shape, shards, smallest, top_value):
    factor_of = 1.0
    for axis_at, shards_of in shards:
        heights = jax.random.uniform(jax.random.fold_in(jax.random.fold_in(rng, 6), axis_at), (shards_of,), jnp.float32, smallest / len(shards), top_value / len(shards))
        factor_of = factor_of * jnp.repeat(jnp.exp(heights), shape[axis_at] // shards_of).reshape((-1,) + (1,) * (len(shape) - 1 - axis_at))
    return factor_of


def noise(own_key, extent, deviation, bound, cuts=(), kind=jnp.bfloat16):
    array = deviation * jax.random.normal(own_key, extent, jnp.float32)
    if cuts:
        array = array * block_scale(own_key, extent, cuts, -0.22, 0.18)
    return jnp.clip(array, -bound, bound).astype(kind)


def setup_inputs(seed: int = 0) -> dict:
    key_list = jax.random.split(jax.random.key(seed), 4)
    embeddings = noise(key_list[0], (ROWS, D), 1.0, 6.0, ((0, 32),))
    cluster_ids = draw_cluster_ids(jax.random.fold_in(key_list[3], 71), 0)
    owner_bounds = draw_owner_bounds(jax.random.fold_in(key_list[3], 71), 0)
    return dict(embeddings=embeddings, cluster_ids=cluster_ids, owner_bounds=owner_bounds)


epsilon = 1e-06
norm_floor = 0.25

def normalize(block):
    values = block.astype(jnp.float32)
    return (values * lax.rsqrt(lax.optimization_barrier(jnp.sum(values * values, axis=1, keepdims=True)) + epsilon)).astype(jnp.bfloat16)

def reference(embeddings, cluster_ids, owner_bounds):
    clusters = CL_DEV * OWNERS
    row_count = embeddings.shape[0]
    unit_blocks = lax.map(normalize, embeddings.reshape(OWNERS, ROWS_DEV, D))
    id_blocks = cluster_ids.reshape(OWNERS, ROWS_DEV)

    def accumulate(block, carry):
        block_rows = lax.dynamic_index_in_dim(unit_blocks, block, 0, keepdims=False)
        block_ids = lax.dynamic_index_in_dim(id_blocks, block, 0, keepdims=False)
        return carry + jax.ops.segment_sum(block_rows.astype(jnp.float32), block_ids, num_segments=clusters)
    member_sums = lax.fori_loop(0, OWNERS, accumulate, jnp.zeros((clusters, D), jnp.float32))
    members = jax.ops.segment_sum(jnp.ones((row_count,), jnp.float32), cluster_ids, num_segments=clusters)
    centroid = member_sums / jnp.maximum(members, 1.0)[:, None]
    centroid_norm = jnp.sqrt(lax.optimization_barrier(jnp.sum(centroid * centroid, axis=1)))
    unit_centroid = (centroid / jnp.maximum(centroid_norm, norm_floor)[:, None]).astype(jnp.bfloat16)

    def measure(pair):
        block_rows, block_ids = pair
        picked = unit_centroid[block_ids]
        return 1.0 - lax.optimization_barrier(jnp.sum(block_rows.astype(jnp.float32) * picked.astype(jnp.float32), axis=1))
    distance = lax.map(measure, (unit_blocks, id_blocks)).reshape(-1)
    sorted_rows = jnp.argsort(cluster_ids, stable=True).astype(jnp.int32)
    sorted_place = jnp.zeros((row_count,), jnp.int32).at[sorted_rows].set(jnp.arange(row_count, dtype=jnp.int32))
    sorted_ids = cluster_ids[sorted_rows]
    slot_index = (sorted_place - jnp.searchsorted(sorted_ids, cluster_ids, side='left').astype(jnp.int32)).astype(jnp.int32)
    range_ends = jnp.concatenate([owner_bounds[1:], jnp.full((1,), clusters, jnp.int32)])
    wanted = owner_bounds[:, None] + jnp.arange(OWN_MAX, dtype=jnp.int32)[None, :]
    inside = wanted < range_ends[:, None]
    table = unit_centroid[jnp.minimum(wanted, clusters - 1)]
    centroids = jnp.where(inside[:, :, None], table, jnp.zeros_like(table)).astype(jnp.bfloat16)
    return (distance, slot_index, centroids)
```

```python
import functools

import jax
import jax.numpy as jnp
from jax import lax
from jax.experimental import pallas as pl
from jax.experimental.pallas import tpu as pltpu
from jax.sharding import PartitionSpec as P

CL_DEV = 384
LANES = 128

epsilon = 1e-06
norm_floor = 0.25
MESH = pl.DeviceIdType.MESH
F32 = jnp.float32
BF16 = jnp.bfloat16
EXACT = lax.Precision.HIGHEST
NT = (((1,), (1,)), ((), ()))


def iota(shape, dim):
    return lax.broadcasted_iota(jnp.int32, shape, dim)


def ones_at(mask, kind):
    return jnp.where(mask, 1.0, 0.0).astype(kind)


def digits_dot(table, place):
    high = jnp.floor(table * (1.0 / 32.0))
    low = table - 32.0 * high
    upper = jnp.dot(high.astype(BF16), place, preferred_element_type=F32)
    lower = jnp.dot(low.astype(BF16), place, preferred_element_type=F32)
    return 32.0 * upper + lower


def kernel(
    groups, replicas, direct, extra,
    emb_ref, ids_ref, bounds_ref,
    cent_ref, dist_ref, rank_ref, over_ref,
    unit, send_rows, got_rows, send_ids, got_ids, member, total, ret, got_ret, slot_mat,
    row_send, row_recv, id_send, id_recv, ret_send, ret_recv,
    near_send, near_recv, far_send, far_recv,
):
    my_group = lax.axis_index("grp")
    my_replica = lax.axis_index("rep")
    me = my_group * replicas + my_replica
    owners = groups * replicas
    rows, width = emb_ref.shape
    limit = cent_ref.shape[0]
    slots = direct + extra
    block = replicas * slots
    sent = replicas * direct

    def peer(dg, dr):
        return lax.rem(my_group + dg, groups), lax.rem(my_replica + dr, replicas)

    def source(dg, dr):
        return (
            lax.rem(my_group + groups - dg, groups),
            lax.rem(my_replica + replicas - dr, replicas),
        )

    def every(dg, act):
        def one(dr, carry):
            act(dr)
            return carry

        lax.fori_loop(1 if dg == 0 else 0, replicas, one, 0)

    def copy(src, dst, ssem, rsem, pair, here, there):
        return pltpu.make_async_remote_copy(
            src_ref=src.at[there],
            dst_ref=dst.at[here, pl.ds(0, direct)] if dst is got_rows else dst.at[here],
            send_sem=ssem.at[there],
            recv_sem=rsem.at[here],
            device_id=pair,
            device_id_type=MESH,
        )

    def start(bufs, dg, dr):
        pair = peer(dg, dr)
        copy(*bufs, pair, me, pair[0] * replicas + pair[1]).start()

    def wait_send(bufs, dg, dr):
        pair = peer(dg, dr)
        copy(*bufs, pair, me, pair[0] * replicas + pair[1]).wait_send()

    def wait_recv(bufs, dg, dr):
        pair = source(dg, dr)
        there = pair[0] * replicas + pair[1]
        copy(*bufs, pair, there, there).wait_recv()

    row_bufs = (send_rows, got_rows, row_send, row_recv)
    id_bufs = (send_ids, got_ids, id_send, id_recv)
    ret_bufs = (ret, got_ret, ret_send, ret_recv)
    order = list(range(1, groups)) + [0]

    barrier = pltpu.get_barrier_semaphore()
    for dg in order:
        every(
            dg,
            lambda dr, dg=dg: pl.semaphore_signal(
                barrier, inc=1, device_id=peer(dg, dr), device_id_type=MESH
            ),
        )

    ids = ids_ref[...]
    edges = bounds_ref[...]
    reached = ones_at(edges <= ids, F32)
    owner = jnp.sum(reached, axis=0, keepdims=True).astype(jnp.int32) - 1
    owned = iota((owners, rows), 0) == owner
    owned_f = ones_at(owned, F32)
    first = jnp.sum(owned_f * edges.astype(F32), axis=0, keepdims=True)
    local = ids.astype(F32) - first
    earlier = ones_at(iota((rows, rows), 0) < iota((rows, rows), 1), BF16)
    prefix = jnp.dot(owned_f.astype(BF16), earlier, preferred_element_type=F32)
    rank = jnp.sum(owned_f * prefix, axis=0, keepdims=True).astype(jnp.int32)
    target = jnp.where(rank < direct, owner * direct + rank, -1)
    spot = rank
    if extra:
        late = ones_at(rank >= direct, F32)
        queue = jnp.dot(
            jnp.broadcast_to(late, (8, rows)).astype(BF16), earlier, preferred_element_type=F32
        )[0:1, :].astype(jnp.int32)
        spot = jnp.where(rank < direct, rank, direct + queue)
    place = ones_at(iota((LANES, rows), 0) == spot, BF16)

    values = emb_ref[...].astype(F32)
    unit[...] = (
        values * lax.rsqrt(jnp.sum(values * values, axis=1, keepdims=True) + epsilon)
    ).astype(BF16)

    def pack(dg):
        tg = lax.rem(my_group + dg, groups)
        pick = ones_at(iota((sent, rows), 0) + tg * sent == target, BF16)
        packed = jnp.dot(pick, unit[...], preferred_element_type=F32).astype(BF16)
        send_rows[pl.ds(tg * replicas, replicas)] = packed.reshape(replicas, direct, width)

    def near_copy(pair, owner_at, dr):
        ref = got_rows.at[owner_at, pl.ds(direct, extra)]
        return pltpu.make_async_remote_copy(
            src_ref=ref, dst_ref=ref, send_sem=near_send.at[dr], recv_sem=near_recv.at[dr],
            device_id=pair, device_id_type=MESH,
        )

    def far_copy(group_at, to_group, dg):
        ref = got_rows.at[pl.ds(group_at * replicas, replicas), pl.ds(direct, extra)]
        return pltpu.make_async_remote_copy(
            src_ref=ref, dst_ref=ref, send_sem=far_send.at[dg], recv_sem=far_recv.at[dg],
            device_id=(to_group, my_replica), device_id_type=MESH,
        )

    if extra:
        pick = ones_at(iota((extra, rows), 0) + direct == spot, BF16)
        got_rows[me, direct:slots] = jnp.dot(
            pick, unit[...], preferred_element_type=F32
        ).astype(BF16)
    pack(order[0])
    pl.semaphore_wait(barrier, owners - 1)
    if extra:
        every(0, lambda dr: near_copy(peer(0, dr), me, dr).start())
    every(order[0], lambda dr: start(row_bufs, order[0], dr))

    high = jnp.floor(local * (1.0 / 32.0))
    low = local - 32.0 * high
    owned_d = jnp.where(rank < direct, owned_f, 0.0)
    upper = lax.dot_general((owned_d * high).astype(BF16), place, NT, preferred_element_type=F32)
    lower = lax.dot_general((owned_d * low).astype(BF16), place, NT, preferred_element_type=F32)
    filled = lax.dot_general(owned_d.astype(BF16), place, NT, preferred_element_type=F32)
    id_table = 32.0 * upper + lower + filled - 1.0
    count = jnp.zeros((1, 1), F32)
    if extra:
        named = jnp.broadcast_to(late * (ids.astype(F32) + 1.0), (8, rows))
        others = lax.dot_general(
            named, place.astype(F32), NT, precision=EXACT, preferred_element_type=F32
        )
        id_table = id_table + others[0:1, :]
        count = jnp.sum(late, axis=1, keepdims=True)
    top = iota((8, LANES), 0) == 0
    for o in range(owners):
        send_ids[o] = jnp.where(top, id_table[o : o + 1, :], count)
    got_ids[me] = send_ids[me]

    for dg in order:
        every(dg, lambda dr, dg=dg: start(id_bufs, dg, dr))
    for dg in order[1:]:
        pack(dg)
        every(dg, lambda dr, dg=dg: start(row_bufs, dg, dr))
    got_rows[me, 0:direct] = send_rows[me]
    if extra:
        def near_wait(dr):
            pair = source(0, dr)
            near_copy(pair, pair[0] * replicas + pair[1], dr).wait_recv()

        every(0, near_wait)
        for dg in order[:-1]:
            far_copy(my_group, lax.rem(my_group + dg, groups), dg).start()

    for dg in order:
        every(dg, lambda dr, dg=dg: wait_recv(id_bufs, dg, dr))
    worst = jnp.max(got_ids[:, 1, :], axis=0, keepdims=True)
    over_ref[...] = jnp.where(worst > extra, 1, 0)
    begin = jnp.sum(
        jnp.where(iota((owners, 1), 0) == me, edges, 0), axis=0, keepdims=True
    ).astype(F32)
    ending = jnp.sum(
        jnp.where(iota((owners, 1), 0) == me + 1, edges, 0), axis=0, keepdims=True
    ).astype(F32) + jnp.where(me == owners - 1, float(CL_DEV * owners), 0.0)

    lane = iota((1, block), 1)
    quotient = jnp.zeros((1, block), jnp.int32)
    for s in range(1, replicas):
        quotient = quotient + jnp.where(lane >= s * slots, 1, 0)
    remainder = lane - quotient * slots
    spread = iota((LANES, block), 0) == remainder
    spread_b, spread_f = ones_at(spread, BF16), ones_at(spread, F32)
    from_source = ones_at(iota((replicas, block), 0) == quotient, F32)
    before = ones_at(iota((block, block), 0) < iota((block, block), 1), BF16)
    cluster = iota((limit, block), 0)

    seen = jnp.zeros((limit, 1), F32)
    for sg in range(groups):
        table = got_ids[sg * replicas : (sg + 1) * replicas, 0, :]
        if extra:
            mine = jnp.where((table >= begin) & (table < ending), table - begin, -1.0)
            table = jnp.where(iota((replicas, LANES), 1) < direct, table, mine)
        flat = jnp.sum(from_source * digits_dot(table, spread_b), axis=0, keepdims=True)
        mask = ones_at(cluster == flat.astype(jnp.int32), F32)
        mask_b = mask.astype(BF16)
        member[sg] = mask_b
        ahead = jnp.dot(mask_b, before, preferred_element_type=F32) + seen
        slot = jnp.sum(mask * ahead, axis=0, keepdims=True)
        seen = seen + jnp.sum(mask, axis=1, keepdims=True)
        slot_mat[sg] = lax.dot_general(
            from_source * slot, spread_f, NT, precision=EXACT, preferred_element_type=F32
        )
    total[...] = jnp.zeros_like(total)
    for dg in order:
        sg = lax.rem(my_group + groups - dg, groups)
        every(dg, lambda dr, dg=dg: wait_recv(row_bufs, dg, dr))
        if extra and dg:
            far_copy(sg, sg, dg).wait_recv()
        block_rows = got_rows[pl.ds(sg * replicas, replicas)].reshape(block, width)
        total[...] += jnp.dot(member[sg], block_rows, preferred_element_type=F32)

    centroid = total[...] / jnp.maximum(seen, 1.0)
    norm = jnp.sqrt(jnp.sum(centroid * centroid, axis=1, keepdims=True))
    cent_ref[...] = (centroid / jnp.maximum(norm, norm_floor)).astype(BF16)

    for dg in order:
        sg = lax.rem(my_group + groups - dg, groups)
        tg = lax.rem(my_group + groups - dg, groups)
        block_rows = got_rows[pl.ds(sg * replicas, replicas)].reshape(block, width)
        score = lax.dot_general(cent_ref[...], block_rows, NT, preferred_element_type=F32)
        near = jnp.sum(member[sg].astype(F32) * score, axis=0, keepdims=True)
        dist_mat = lax.dot_general(
            from_source * (1.0 - near), spread_f, NT, precision=EXACT, preferred_element_type=F32
        )
        rank_mat = slot_mat[sg]
        for s in range(replicas):
            ret[tg * replicas + s] = jnp.where(top, dist_mat[s : s + 1, :], rank_mat[s : s + 1, :])
        back = (groups - dg) % groups
        every(back, lambda dr, back=back: start(ret_bufs, back, dr))
    got_ret[me] = ret[me]

    place_f = ones_at(iota((LANES, rows), 0) == spot, F32)
    for dg in order:
        every(dg, lambda dr, dg=dg: wait_recv(ret_bufs, dg, dr))
    dist_all = jnp.dot(got_ret[:, 0, :], place_f, precision=EXACT, preferred_element_type=F32)
    rank_all = jnp.dot(got_ret[:, 1, :], place_f, precision=EXACT, preferred_element_type=F32)
    dist_ref[...] = jnp.sum(owned_f * dist_all, axis=0, keepdims=True)
    rank_ref[...] = jnp.sum(owned_f * rank_all, axis=0, keepdims=True).astype(jnp.int32)
    for bufs in (id_bufs, row_bufs, ret_bufs):
        for dg in order:
            every(dg, lambda dr, dg=dg, bufs=bufs: wait_send(bufs, dg, dr))
    if extra:
        every(0, lambda dr: near_copy(peer(0, dr), me, dr).wait_send())
        for dg in order[:-1]:
            far_copy(my_group, lax.rem(my_group + dg, groups), dg).wait_send()


def fold(count, size):
    return jnp.floor((iota((1, count), 1).astype(F32) + 0.5) * (1.0 / size)).astype(jnp.int32)


def split(value):
    upper = value.astype(BF16)
    return upper, (value - upper.astype(F32)).astype(BF16)


def digits(value):
    upper = jnp.floor(value * (1.0 / 256.0))
    return upper.astype(BF16), (value - 256.0 * upper).astype(BF16)


def dot(left, right):
    return jnp.dot(left, right, preferred_element_type=F32)


def dot_nt(left, right):
    return lax.dot_general(left, right, NT, preferred_element_type=F32)


def fast_kernel(
    groups, replicas, direct, shared, spare,
    emb_ref, ids_ref, bounds_ref,
    cent_ref, dist_ref, rank_ref, over_ref,
    unit, send_d, send_q, got_d, got_q, got_e,
    send_ids, got_ids, send_rank, got_rank, send_dist, got_dist,
    mask_d, mask_q, mask_e, total, ranks, spread,
    d_send, d_recv, id_send, id_recv, rank_send, rank_recv, dist_send, dist_recv,
    q_send, q_recv, qf_send, qf_recv, e_send, e_recv, ef_send, ef_recv,
):
    my_group = lax.axis_index("grp")
    my_replica = lax.axis_index("rep")
    me = my_group * replicas + my_replica
    owners = groups * replicas
    rows, width = emb_ref.shape
    limit = cent_ref.shape[0]
    planes, sides = replicas // 2, groups // 2
    my_plane, my_col = lax.div(my_replica, 2), lax.rem(my_replica, 2)
    my_side, my_core = lax.div(my_group, 2), lax.rem(my_group, 2)

    def turn(at, step, size):
        return lax.rem(at + step, size)

    def back(at, step, size):
        return lax.rem(at + (size - step), size)

    to_group = [turn(my_group, s, groups) for s in range(groups)]
    to_replica = [turn(my_replica, s, replicas) for s in range(replicas)]
    from_group = [back(my_group, s, groups) for s in range(groups)]
    from_replica = [back(my_replica, s, replicas) for s in range(replicas)]
    steps = [
        (dg, dr) for dg in range(groups) for dr in range(replicas) if dg or dr
    ]

    barrier = pltpu.get_barrier_semaphore()
    for dg, dr in steps:
        pl.semaphore_signal(
            barrier, inc=1, device_id=(to_group[dg], to_replica[dr]), device_id_type=MESH
        )

    def remote(src, dst, ssem, rsem, pair):
        return pltpu.make_async_remote_copy(
            src_ref=src, dst_ref=dst, send_sem=ssem, recv_sem=rsem,
            device_id=pair, device_id_type=MESH,
        )

    def pair_out(bufs, dg, dr):
        src, dst, ssem, rsem = bufs
        pair = (to_group[dg], to_replica[dr])
        there = pair[0] * replicas + pair[1]
        return remote(src.at[there], dst.at[me], ssem.at[there], rsem.at[me], pair)

    def pair_in(bufs, dg, dr):
        src, dst, ssem, rsem = bufs
        pair = (from_group[dg], from_replica[dr])
        there = pair[0] * replicas + pair[1]
        return remote(src.at[there], dst.at[there], ssem.at[there], rsem.at[there], pair)

    d_bufs = (send_d, got_d, d_send, d_recv)
    id_bufs = (send_ids, got_ids, id_send, id_recv)
    rank_bufs = (send_rank, got_rank, rank_send, rank_recv)
    dist_bufs = (send_dist, got_dist, dist_send, dist_recv)

    def q_out(dr):
        there = to_replica[dr]
        return remote(
            send_q.at[there], got_q.at[my_group, my_replica],
            q_send.at[dr], q_recv.at[dr], (my_group, there),
        )

    def q_in(dr):
        there = from_replica[dr]
        return remote(
            send_q.at[there], got_q.at[my_group, there],
            q_send.at[dr], q_recv.at[dr], (my_group, there),
        )

    sibling = (my_side * 2 + (1 - my_core), my_replica)

    def side_pair(ds, inward):
        side = back(my_side, ds, sides) if inward else turn(my_side, ds, sides)
        return (side * 2 + my_core, my_replica)

    def qf_side(ds, inward):
        pair = side_pair(ds, inward)
        group = pair[0] if inward else my_group
        ref = got_q.at[group]
        return remote(ref, ref, qf_send.at[ds], qf_recv.at[ds], pair)

    def qf_core(ds, inward):
        group = side_pair(ds, True)[0]
        group = group + (1 - 2 * my_core) if inward else group
        ref = got_q.at[group]
        return remote(ref, ref, qf_send.at[sides + ds], qf_recv.at[sides + ds], sibling)

    def e_plane(dp, inward):
        plane = back(my_plane, dp, planes) if inward else turn(my_plane, dp, planes)
        ref = got_e.at[my_group, my_col, plane if inward else my_plane]
        return remote(
            ref, ref, e_send.at[dp], e_recv.at[dp], (my_group, plane * 2 + my_col)
        )

    def e_spot(ds, dc, inward):
        side = back(my_side, ds, sides) if inward else turn(my_side, ds, sides)
        col = lax.rem(my_col + dc, 2)
        return side * 2 + my_core, col

    def ef_side(ds, dc, inward):
        group, col = e_spot(ds, dc, inward)
        ref = got_e.at[group, col] if inward else got_e.at[my_group, my_col]
        at = ds * 2 + dc
        return remote(
            ref, ref, ef_send.at[at], ef_recv.at[at], (group, my_plane * 2 + col)
        )

    def ef_core(ds, dc, inward):
        group, col = e_spot(ds, dc, True)
        group = group + (1 - 2 * my_core) if inward else group
        ref = got_e.at[group, col]
        at = groups + ds * 2 + dc
        return remote(ref, ref, ef_send.at[at], ef_recv.at[at], sibling)

    ids = ids_ref[...]
    bounds = bounds_ref[...]
    diagonal = iota((owners, owners), 0) == iota((owners, owners), 1)
    edges = jnp.sum(jnp.where(diagonal, bounds, 0), axis=1, keepdims=True)
    owner = jnp.sum(ones_at(edges <= ids, F32), axis=0, keepdims=True).astype(jnp.int32) - 1
    owned = iota((owners, rows), 0) == owner
    owned_f = ones_at(owned, F32)
    earlier = ones_at(iota((rows, rows), 0) < iota((rows, rows), 1), BF16)
    prefix = dot(owned_f.astype(BF16), earlier)
    rank = jnp.sum(owned_f * prefix, axis=0, keepdims=True).astype(jnp.int32)
    column = lax.rem(owner, replicas)
    in_column = iota((replicas, rows), 0) == column
    late = rank >= direct
    column_f = ones_at(in_column, F32)
    late_f = jnp.where(late, column_f, 0.0)
    column_rank = jnp.sum(
        column_f * dot(late_f.astype(BF16), earlier), axis=0, keepdims=True
    ).astype(jnp.int32)
    in_direct = rank < direct
    in_shared = jnp.logical_and(late, column_rank < shared)
    in_spare = jnp.logical_and(late, column_rank >= shared)
    spare_f = ones_at(in_spare, F32)
    spare_rank = dot(
        jnp.broadcast_to(spare_f, (8, rows)).astype(BF16), earlier
    )[0:1, :].astype(jnp.int32)
    count = jnp.sum(spare_f, axis=1, keepdims=True)

    values = emb_ref[...].astype(F32)
    unit[...] = (
        values * lax.rsqrt(jnp.sum(values * values, axis=1, keepdims=True) + epsilon)
    ).astype(BF16)

    def picked(number, target):
        return dot(ones_at(iota((number, rows), 0) == target, BF16), unit[...]).astype(BF16)

    own_spare = picked(spare, jnp.where(in_spare, spare_rank, -1))
    got_e[my_group, my_col, my_plane] = own_spare
    packed = picked(replicas * shared, jnp.where(in_shared, column * shared + column_rank, -1))
    send_q[...] = packed.reshape(replicas, shared, width)
    got_q[my_group, my_replica] = send_q[my_replica]

    lane = jnp.where(
        in_direct, rank, jnp.where(in_shared, direct + column_rank, direct + shared + spare_rank)
    )
    place = ones_at(iota((LANES, rows), 0) == lane, BF16)
    near_f = jnp.concatenate([column_f] * groups, axis=0)
    chosen = jnp.where(in_direct, owned_f, jnp.where(in_shared, near_f, 1.0))
    id_high = jnp.floor(ids.astype(F32) * (1.0 / 256.0))
    id_low = ids.astype(F32) - 256.0 * id_high
    used = direct + shared + spare
    three = jnp.concatenate([chosen * id_high, chosen * id_low, chosen], axis=0).astype(BF16)
    table = dot_nt(three, place)
    table = 256.0 * table[0:owners] + table[owners : 2 * owners] + table[2 * owners :] - 1.0
    table = jnp.where(iota((owners, LANES), 1) < used, table, count)
    send_ids[...] = table.reshape(owners, 1, LANES)
    got_ids[me] = send_ids[me]

    pl.semaphore_wait(barrier, owners - 1)
    for dp in range(1, planes):
        e_plane(dp, False).start()
    for dr in range(1, replicas):
        q_out(dr).start()
    for dg, dr in steps:
        pair_out(id_bufs, dg, dr).start()

    target = jnp.where(in_direct, owner * direct + rank, -1)
    block = replicas * direct
    for dg in list(range(1, groups)) + [0]:
        tg = to_group[dg]
        packed = picked(block, target - tg * block)
        send_d[pl.ds(tg * replicas, replicas)] = packed.reshape(replicas, direct, width)
        for dr in range(replicas):
            if dg or dr:
                pair_out(d_bufs, dg, dr).start()
    got_d[me] = send_d[me]

    for dp in range(1, planes):
        e_plane(dp, True).wait_recv()
    others = [(ds, dc) for ds in range(sides) for dc in range(2) if ds or dc]
    for ds, dc in others:
        ef_side(ds, dc, False).start()
    ef_core(0, 0, False).start()
    for dr in range(1, replicas):
        q_in(dr).wait_recv()
    for ds in range(1, sides):
        qf_side(ds, False).start()
    qf_core(0, False).start()

    direct_row, shared_row, spare_row = groups * block, owners * shared, owners * spare
    d_lane, q_lane, e_lane = fold(block, direct), fold(block, shared), fold(replicas * spare, spare)
    e_col = fold(replicas * spare, spare * planes)
    e_source = (e_lane - e_col * planes) * 2 + e_col
    d_slot = iota((1, block), 1) - d_lane * direct
    q_slot = iota((1, block), 1) - q_lane * shared + direct
    e_slot = iota((1, replicas * spare), 1) - e_lane * spare + (direct + shared)
    lane_source = jnp.concatenate([d_lane, q_lane, e_source], axis=1)
    lane_slot = jnp.concatenate([d_slot, q_slot, e_slot], axis=1)
    span = lane_source.shape[1]
    expand = ones_at(iota((LANES, span), 0) == lane_slot, BF16)
    from_source = ones_at(iota((replicas, span), 0) == lane_source, F32)
    key = lane_source * used + lane_slot
    key_col = jnp.sum(
        jnp.where(iota((span, span), 0) == iota((span, span), 1), key, 0), axis=1, keepdims=True
    )
    before = ones_at(key_col < key, BF16)

    def spread_rows(size, offset):
        at = jnp.floor((iota((size, LANES), 0).astype(F32) + 0.5) * (1.0 / offset[0]))
        slot = iota((size, LANES), 0) - at.astype(jnp.int32) * offset[0] + offset[1]
        return ones_at(slot == iota((size, LANES), 1), BF16)

    spread[0:direct_row] = spread_rows(direct_row, (direct, 0))
    spread[direct_row : direct_row + shared_row] = spread_rows(shared_row, (shared, direct))
    spread[direct_row + shared_row :] = spread_rows(spare_row, (spare, direct + shared))

    d_all = fold(direct_row, direct)
    q_all = fold(shared_row, shared)
    e_all = fold(spare_row, spare)
    e_group = fold(spare_row, replicas * spare)
    e_inner = e_all - e_group * replicas
    e_side = fold(spare_row, planes * spare) - e_group * 2
    e_all = e_group * replicas + (e_inner - e_side * planes) * 2 + e_side
    all_source = jnp.concatenate([d_all, q_all, e_all], axis=1)

    def by_source(row, parts):
        held = jnp.where(iota((owners, row.shape[1]), 0) == all_source, row, 0.0)
        upper, lower = parts(held)
        both = dot(jnp.concatenate([upper, lower], axis=0), spread[...])
        return both[0:owners], both[owners:]

    for dg, dr in steps:
        pair_in(id_bufs, dg, dr).wait_recv()
    named = got_ids[...].reshape(owners, LANES)
    worst = jnp.max(named, axis=0, keepdims=True)
    over_ref[...] = jnp.where(worst > spare, 1, 0)
    begin = jnp.sum(jnp.where(iota((owners, 1), 0) == me, edges, 0), axis=0, keepdims=True)
    ending = jnp.sum(
        jnp.where(iota((owners, 1), 0) == me + 1, edges, 0), axis=0, keepdims=True
    ) + jnp.where(me == owners - 1, CL_DEV * owners, 0)
    begin, ending = begin.astype(F32), ending.astype(F32)
    mine = jnp.logical_and(named >= begin, named < ending)
    local = jnp.where(mine, named - begin + 1.0, 0.0)
    local_high, local_low = digits(local)
    flat_both = dot(jnp.concatenate([local_high, local_low], axis=0), expand)
    flat_all = 256.0 * flat_both[0:owners] + flat_both[owners:] - 1.0

    seen = jnp.zeros((limit, 1), F32)
    cluster = iota((limit, span), 0)
    wide = replicas * spare
    for sg in range(groups):
        flat = jnp.sum(
            from_source * flat_all[sg * replicas : (sg + 1) * replicas], axis=0, keepdims=True
        )
        mask = ones_at(cluster == flat.astype(jnp.int32), F32)
        mask_b = mask.astype(BF16)
        mask_d[:, sg * block : (sg + 1) * block] = mask_b[:, 0:block]
        mask_q[:, sg * block : (sg + 1) * block] = mask_b[:, block : 2 * block]
        mask_e[:, sg * wide : (sg + 1) * wide] = mask_b[:, 2 * block :]
        ahead = dot(mask_b, before) + seen
        slot = jnp.sum(mask * ahead, axis=0, keepdims=True)
        ranks[:, sg * block : (sg + 1) * block] = slot[:, 0:block]
        at = direct_row + sg * block
        ranks[:, at : at + block] = slot[:, block : 2 * block]
        at = direct_row + shared_row + sg * wide
        ranks[:, at : at + wide] = slot[:, 2 * block :]
        seen = seen + jnp.sum(mask, axis=1, keepdims=True)

    upper, lower = by_source(ranks[...], digits)
    send_rank[...] = (256.0 * upper + lower).reshape(owners, 1, LANES)
    got_rank[me] = send_rank[me]
    for dg, dr in steps:
        pair_out(rank_bufs, dg, dr).start()

    for ds in range(1, sides):
        qf_side(ds, True).wait_recv()
        qf_core(ds, False).start()
    for ds, dc in others:
        ef_side(ds, dc, True).wait_recv()
        ef_core(ds, dc, False).start()

    for ds in range(sides):
        qf_core(ds, True).wait_recv()
    rows_q = got_q[...].reshape(shared_row, width)
    total[...] = dot(mask_q[...], rows_q)
    for ds in range(sides):
        for dc in range(2):
            ef_core(ds, dc, True).wait_recv()
    rows_e = got_e[...].reshape(spare_row, width)
    total[...] += dot(mask_e[...], rows_e)

    for dg, dr in steps:
        pair_in(rank_bufs, dg, dr).wait_recv()

    def collect(ref, parts, scale):
        upper, lower = parts(ref[...].reshape(owners, LANES))
        both = dot(jnp.concatenate([upper, lower], axis=0), place)
        return jnp.sum(
            owned_f * (scale * both[0:owners] + both[owners:]), axis=0, keepdims=True
        )

    rank_ref[...] = collect(got_rank, digits, 256.0).astype(jnp.int32)

    for dg, dr in steps:
        pair_in(d_bufs, dg, dr).wait_recv()
    rows_d = got_d[...].reshape(direct_row, width)
    sums = total[...] + dot(mask_d[...], rows_d)
    share = 1.0 / jnp.maximum(seen, 1.0)
    norm = share * jnp.sqrt(jnp.sum(sums * sums, axis=1, keepdims=True))
    cent_ref[...] = (sums * (share / jnp.maximum(norm, norm_floor))).astype(BF16)

    def near(mask_ref, begin_at, end_at, block_rows):
        score = dot_nt(cent_ref[...], block_rows)
        return jnp.sum(
            mask_ref[:, begin_at:end_at].astype(F32) * score, axis=0, keepdims=True
        )

    half = spare_row // 2
    nears = jnp.concatenate([
        near(mask_d, 0, direct_row, got_d[...].reshape(direct_row, width)),
        near(mask_q, 0, shared_row, got_q[...].reshape(shared_row, width)),
        near(mask_e, 0, half, got_e[0 : groups // 2].reshape(half, width)),
        near(mask_e, half, spare_row, got_e[groups // 2 :].reshape(half, width)),
    ], axis=1)
    upper, lower = by_source(nears, split)
    send_dist[...] = (upper + lower).reshape(owners, 1, LANES)
    got_dist[me] = send_dist[me]
    for dg, dr in steps:
        pair_out(dist_bufs, dg, dr).start()

    for bufs in (id_bufs, d_bufs, rank_bufs):
        for dg, dr in steps:
            pair_out(bufs, dg, dr).wait_send()
    for dp in range(1, planes):
        e_plane(dp, False).wait_send()
    for dr in range(1, replicas):
        q_out(dr).wait_send()
    for ds, dc in others:
        ef_side(ds, dc, False).wait_send()
    for ds in range(1, sides):
        qf_side(ds, False).wait_send()
    for ds in range(sides):
        qf_core(ds, False).wait_send()
        for dc in range(2):
            ef_core(ds, dc, False).wait_send()

    for dg, dr in steps:
        pair_in(dist_bufs, dg, dr).wait_recv()
    dist_ref[...] = 1.0 - collect(got_dist, split, 1.0)
    for dg, dr in steps:
        pair_out(dist_bufs, dg, dr).wait_send()


def solution(mesh):
    groups, replicas = mesh.shape["grp"], mesh.shape["rep"]
    owners = groups * replicas

    def shards(embeddings, cluster_ids, owner_bounds):
        rows, width = embeddings.shape
        limit = CL_DEV + CL_DEV // 2
        most = -(-(3 * rows // owners) // 16) * 16
        direct, shared, spare = 16, 16, 32
        vmem = pl.BlockSpec(memory_space=pltpu.VMEM)
        each = pltpu.SemaphoreType.DMA((owners,))
        ids_row = cluster_ids.reshape(1, rows)
        outs = (
            jax.ShapeDtypeStruct((limit, width), BF16),
            jax.ShapeDtypeStruct((1, rows), F32),
            jax.ShapeDtypeStruct((1, rows), jnp.int32),
            jax.ShapeDtypeStruct((1, LANES), jnp.int32),
        )

        def run(number):
            small = pltpu.VMEM((owners, 8, LANES), F32)
            near = pltpu.SemaphoreType.DMA((replicas,))
            far = pltpu.SemaphoreType.DMA((groups,))
            return pl.pallas_call(
                functools.partial(kernel, groups, replicas, most, 0),
                out_shape=outs,
                in_specs=[vmem] * 3,
                out_specs=(vmem,) * 4,
                scratch_shapes=[
                    pltpu.VMEM((rows, width), BF16),
                    pltpu.VMEM((owners, most, width), BF16),
                    pltpu.VMEM((owners, most, width), BF16),
                    small,
                    small,
                    pltpu.VMEM((groups, limit, replicas * most), BF16),
                    pltpu.VMEM((limit, width), F32),
                    small,
                    small,
                    pltpu.VMEM((groups, replicas, LANES), F32),
                    each, each, each, each, each, each, near, near, far, far,
                ],
                compiler_params=pltpu.CompilerParams(
                    collective_id=number,
                    has_side_effects=True,
                    vmem_limit_bytes=48 * 1024 * 1024,
                ),
            )(embeddings, ids_row, owner_bounds.reshape(owners, 1))

        def run_fast(number):
            small = pltpu.VMEM((owners, 1, LANES), F32)
            slots = owners * (direct + shared + spare)
            return pl.pallas_call(
                functools.partial(fast_kernel, groups, replicas, direct, shared, spare),
                out_shape=outs,
                in_specs=[vmem] * 3,
                out_specs=(vmem,) * 4,
                scratch_shapes=[
                    pltpu.VMEM((rows, width), BF16),
                    pltpu.VMEM((owners, direct, width), BF16),
                    pltpu.VMEM((replicas, shared, width), BF16),
                    pltpu.VMEM((owners, direct, width), BF16),
                    pltpu.VMEM((groups, replicas, shared, width), BF16),
                    pltpu.VMEM((groups, 2, replicas // 2, spare, width), BF16),
                    small, small, small, small, small, small,
                    pltpu.VMEM((limit, owners * direct), BF16),
                    pltpu.VMEM((limit, owners * shared), BF16),
                    pltpu.VMEM((limit, owners * spare), BF16),
                    pltpu.VMEM((limit, width), F32),
                    pltpu.VMEM((1, slots), F32),
                    pltpu.VMEM((slots, LANES), BF16),
                    each, each, each, each, each, each, each, each,
                    pltpu.SemaphoreType.DMA((replicas,)),
                    pltpu.SemaphoreType.DMA((replicas,)),
                    pltpu.SemaphoreType.DMA((groups,)),
                    pltpu.SemaphoreType.DMA((groups,)),
                    pltpu.SemaphoreType.DMA((replicas // 2,)),
                    pltpu.SemaphoreType.DMA((replicas // 2,)),
                    pltpu.SemaphoreType.DMA((2 * groups,)),
                    pltpu.SemaphoreType.DMA((2 * groups,)),
                ],
                compiler_params=pltpu.CompilerParams(
                    collective_id=number,
                    has_side_effects=True,
                    vmem_limit_bytes=48 * 1024 * 1024,
                ),
            )(embeddings, ids_row, owner_bounds.reshape(1, owners))

        whole = groups % 2 == 0 and replicas * direct == LANES and rows // owners <= direct
        if most > 2 * direct and whole:
            first = run_fast(0)
            centroids, distance, rank = lax.cond(
                first[3][0, LANES - 1] > 0, lambda: run(1)[:3], lambda: first[:3]
            )
        else:
            centroids, distance, rank, _ = run(0)
        return distance.reshape(rows), rank.reshape(rows), centroids[None]

    placed = (P(("grp", "rep"), None), P(("grp", "rep")), P())
    return jax.shard_map(
        shards,
        mesh=mesh,
        in_specs=placed,
        out_specs=(P(("grp", "rep")), P(("grp", "rep")), P(("grp", "rep"), None, None)),
        check_vma=False,
    )
```

```python
import functools

import jax
import jax.numpy as jnp
from jax import lax
from jax.experimental import pallas as pl
from jax.experimental.pallas import tpu as pltpu
from jax.sharding import PartitionSpec as P

CL_DEV = 384
LANES = 128

epsilon = 1e-06
norm_floor = 0.25
MESH = pl.DeviceIdType.MESH
F32 = jnp.float32
BF16 = jnp.bfloat16
EXACT = lax.Precision.HIGHEST
NT = (((1,), (1,)), ((), ()))


def iota(shape, dim):
    return lax.broadcasted_iota(jnp.int32, shape, dim)


def ones_at(mask, kind):
    return jnp.where(mask, 1.0, 0.0).astype(kind)


def digits_dot(table, place):
    high = jnp.floor(table * (1.0 / 32.0))
    low = table - 32.0 * high
    upper = jnp.dot(high.astype(BF16), place, preferred_element_type=F32)
    lower = jnp.dot(low.astype(BF16), place, preferred_element_type=F32)
    return 32.0 * upper + lower


def kernel(
    groups, replicas, direct, extra,
    emb_in, ids_in, bounds_in,
    cent_ref, dist_ref, rank_ref, over_ref,
    emb_ref, ids_ref, bounds_ref, in_sems,
    unit, send_rows, got_rows, send_ids, got_ids, member, total, ret, got_ret, slot_mat,
    row_send, row_recv, id_send, id_recv, ret_send, ret_recv,
    near_send, near_recv, far_send, far_recv,
):
    my_group = lax.axis_index("grp")
    my_replica = lax.axis_index("rep")
    me = my_group * replicas + my_replica
    owners = groups * replicas
    rows, width = emb_ref.shape
    limit = cent_ref.shape[0]
    slots = direct + extra
    block = replicas * slots
    sent = replicas * direct

    def peer(dg, dr):
        return lax.rem(my_group + dg, groups), lax.rem(my_replica + dr, replicas)

    def source(dg, dr):
        return (
            lax.rem(my_group + groups - dg, groups),
            lax.rem(my_replica + replicas - dr, replicas),
        )

    def every(dg, act):
        def one(dr, carry):
            act(dr)
            return carry

        lax.fori_loop(1 if dg == 0 else 0, replicas, one, 0)

    def copy(src, dst, ssem, rsem, pair, here, there):
        return pltpu.make_async_remote_copy(
            src_ref=src.at[there],
            dst_ref=dst.at[here, pl.ds(0, direct)] if dst is got_rows else dst.at[here],
            send_sem=ssem.at[there],
            recv_sem=rsem.at[here],
            device_id=pair,
            device_id_type=MESH,
        )

    def start(bufs, dg, dr):
        pair = peer(dg, dr)
        copy(*bufs, pair, me, pair[0] * replicas + pair[1]).start()

    def wait_send(bufs, dg, dr):
        pair = peer(dg, dr)
        copy(*bufs, pair, me, pair[0] * replicas + pair[1]).wait_send()

    def wait_recv(bufs, dg, dr):
        pair = source(dg, dr)
        there = pair[0] * replicas + pair[1]
        copy(*bufs, pair, there, there).wait_recv()

    row_bufs = (send_rows, got_rows, row_send, row_recv)
    id_bufs = (send_ids, got_ids, id_send, id_recv)
    ret_bufs = (ret, got_ret, ret_send, ret_recv)
    order = list(range(1, groups)) + [0]

    barrier = pltpu.get_barrier_semaphore()
    for dg in order:
        every(
            dg,
            lambda dr, dg=dg: pl.semaphore_signal(
                barrier, inc=1, device_id=peer(dg, dr), device_id_type=MESH
            ),
        )

    loads = [
        pltpu.make_async_copy(emb_in, emb_ref, in_sems.at[0]),
        pltpu.make_async_copy(ids_in, ids_ref, in_sems.at[1]),
        pltpu.make_async_copy(bounds_in, bounds_ref, in_sems.at[2]),
    ]
    for load in loads:
        load.start()
    for load in loads:
        load.wait()
    ids = ids_ref[...]
    diagonal = iota((owners, owners), 0) == iota((owners, owners), 1)
    edges = jnp.sum(jnp.where(diagonal, bounds_ref[...], 0), axis=1, keepdims=True)
    reached = ones_at(edges <= ids, F32)
    owner = jnp.sum(reached, axis=0, keepdims=True).astype(jnp.int32) - 1
    owned = iota((owners, rows), 0) == owner
    owned_f = ones_at(owned, F32)
    first = jnp.sum(owned_f * edges.astype(F32), axis=0, keepdims=True)
    local = ids.astype(F32) - first
    earlier = ones_at(iota((rows, rows), 0) < iota((rows, rows), 1), BF16)
    prefix = jnp.dot(owned_f.astype(BF16), earlier, preferred_element_type=F32)
    rank = jnp.sum(owned_f * prefix, axis=0, keepdims=True).astype(jnp.int32)
    target = jnp.where(rank < direct, owner * direct + rank, -1)
    spot = rank
    if extra:
        late = ones_at(rank >= direct, F32)
        queue = jnp.dot(
            jnp.broadcast_to(late, (8, rows)).astype(BF16), earlier, preferred_element_type=F32
        )[0:1, :].astype(jnp.int32)
        spot = jnp.where(rank < direct, rank, direct + queue)
    place = ones_at(iota((LANES, rows), 0) == spot, BF16)

    values = emb_ref[...].astype(F32)
    unit[...] = (
        values * lax.rsqrt(jnp.sum(values * values, axis=1, keepdims=True) + epsilon)
    ).astype(BF16)

    def pack(dg):
        tg = lax.rem(my_group + dg, groups)
        pick = ones_at(iota((sent, rows), 0) + tg * sent == target, BF16)
        packed = jnp.dot(pick, unit[...], preferred_element_type=F32).astype(BF16)
        send_rows[pl.ds(tg * replicas, replicas)] = packed.reshape(replicas, direct, width)

    def near_copy(pair, owner_at, dr):
        ref = got_rows.at[owner_at, pl.ds(direct, extra)]
        return pltpu.make_async_remote_copy(
            src_ref=ref, dst_ref=ref, send_sem=near_send.at[dr], recv_sem=near_recv.at[dr],
            device_id=pair, device_id_type=MESH,
        )

    def far_copy(group_at, to_group, dg):
        ref = got_rows.at[pl.ds(group_at * replicas, replicas), pl.ds(direct, extra)]
        return pltpu.make_async_remote_copy(
            src_ref=ref, dst_ref=ref, send_sem=far_send.at[dg], recv_sem=far_recv.at[dg],
            device_id=(to_group, my_replica), device_id_type=MESH,
        )

    if extra:
        pick = ones_at(iota((extra, rows), 0) + direct == spot, BF16)
        got_rows[me, direct:slots] = jnp.dot(
            pick, unit[...], preferred_element_type=F32
        ).astype(BF16)
    pack(order[0])
    pl.semaphore_wait(barrier, owners - 1)
    if extra:
        every(0, lambda dr: near_copy(peer(0, dr), me, dr).start())
    every(order[0], lambda dr: start(row_bufs, order[0], dr))

    high = jnp.floor(local * (1.0 / 32.0))
    low = local - 32.0 * high
    owned_d = jnp.where(rank < direct, owned_f, 0.0)
    upper = lax.dot_general((owned_d * high).astype(BF16), place, NT, preferred_element_type=F32)
    lower = lax.dot_general((owned_d * low).astype(BF16), place, NT, preferred_element_type=F32)
    filled = lax.dot_general(owned_d.astype(BF16), place, NT, preferred_element_type=F32)
    id_table = 32.0 * upper + lower + filled - 1.0
    count = jnp.zeros((1, 1), F32)
    if extra:
        named = jnp.broadcast_to(late * (ids.astype(F32) + 1.0), (8, rows))
        others = lax.dot_general(
            named, place.astype(F32), NT, precision=EXACT, preferred_element_type=F32
        )
        id_table = id_table + others[0:1, :]
        count = jnp.sum(late, axis=1, keepdims=True)
    top = iota((8, LANES), 0) == 0
    for o in range(owners):
        send_ids[o] = jnp.where(top, id_table[o : o + 1, :], count)
    got_ids[me] = send_ids[me]

    for dg in order:
        every(dg, lambda dr, dg=dg: start(id_bufs, dg, dr))
    for dg in order[1:]:
        pack(dg)
        every(dg, lambda dr, dg=dg: start(row_bufs, dg, dr))
    got_rows[me, 0:direct] = send_rows[me]
    if extra:
        def near_wait(dr):
            pair = source(0, dr)
            near_copy(pair, pair[0] * replicas + pair[1], dr).wait_recv()

        every(0, near_wait)
        for dg in order[:-1]:
            far_copy(my_group, lax.rem(my_group + dg, groups), dg).start()

    for dg in order:
        every(dg, lambda dr, dg=dg: wait_recv(id_bufs, dg, dr))
    worst = jnp.max(got_ids[:, 1, :], axis=0, keepdims=True)
    over_ref[0, 0] = jnp.where(jnp.max(worst) > extra, 1, 0)
    begin = jnp.sum(
        jnp.where(iota((owners, 1), 0) == me, edges, 0), axis=0, keepdims=True
    ).astype(F32)
    ending = jnp.sum(
        jnp.where(iota((owners, 1), 0) == me + 1, edges, 0), axis=0, keepdims=True
    ).astype(F32) + jnp.where(me == owners - 1, float(CL_DEV * owners), 0.0)

    lane = iota((1, block), 1)
    quotient = jnp.zeros((1, block), jnp.int32)
    for s in range(1, replicas):
        quotient = quotient + jnp.where(lane >= s * slots, 1, 0)
    remainder = lane - quotient * slots
    spread = iota((LANES, block), 0) == remainder
    spread_b, spread_f = ones_at(spread, BF16), ones_at(spread, F32)
    from_source = ones_at(iota((replicas, block), 0) == quotient, F32)
    before = ones_at(iota((block, block), 0) < iota((block, block), 1), BF16)
    cluster = iota((limit, block), 0)

    seen = jnp.zeros((limit, 1), F32)
    for sg in range(groups):
        table = got_ids[sg * replicas : (sg + 1) * replicas, 0, :]
        if extra:
            mine = jnp.where((table >= begin) & (table < ending), table - begin, -1.0)
            table = jnp.where(iota((replicas, LANES), 1) < direct, table, mine)
        flat = jnp.sum(from_source * digits_dot(table, spread_b), axis=0, keepdims=True)
        mask = ones_at(cluster == flat.astype(jnp.int32), F32)
        mask_b = mask.astype(BF16)
        member[sg] = mask_b
        ahead = jnp.dot(mask_b, before, preferred_element_type=F32) + seen
        slot = jnp.sum(mask * ahead, axis=0, keepdims=True)
        seen = seen + jnp.sum(mask, axis=1, keepdims=True)
        slot_mat[sg] = lax.dot_general(
            from_source * slot, spread_f, NT, precision=EXACT, preferred_element_type=F32
        )
    total[...] = jnp.zeros_like(total)
    for dg in order:
        sg = lax.rem(my_group + groups - dg, groups)
        every(dg, lambda dr, dg=dg: wait_recv(row_bufs, dg, dr))
        if extra and dg:
            far_copy(sg, sg, dg).wait_recv()
        block_rows = got_rows[pl.ds(sg * replicas, replicas)].reshape(block, width)
        total[...] += jnp.dot(member[sg], block_rows, preferred_element_type=F32)

    centroid = total[...] / jnp.maximum(seen, 1.0)
    norm = jnp.sqrt(jnp.sum(centroid * centroid, axis=1, keepdims=True))
    cent_ref[...] = (centroid / jnp.maximum(norm, norm_floor)).astype(BF16)

    for dg in order:
        sg = lax.rem(my_group + groups - dg, groups)
        tg = lax.rem(my_group + groups - dg, groups)
        block_rows = got_rows[pl.ds(sg * replicas, replicas)].reshape(block, width)
        score = lax.dot_general(cent_ref[...], block_rows, NT, preferred_element_type=F32)
        near = jnp.sum(member[sg].astype(F32) * score, axis=0, keepdims=True)
        dist_mat = lax.dot_general(
            from_source * (1.0 - near), spread_f, NT, precision=EXACT, preferred_element_type=F32
        )
        rank_mat = slot_mat[sg]
        for s in range(replicas):
            ret[tg * replicas + s] = jnp.where(top, dist_mat[s : s + 1, :], rank_mat[s : s + 1, :])
        back = (groups - dg) % groups
        every(back, lambda dr, back=back: start(ret_bufs, back, dr))
    got_ret[me] = ret[me]

    place_f = ones_at(iota((LANES, rows), 0) == spot, F32)
    for dg in order:
        every(dg, lambda dr, dg=dg: wait_recv(ret_bufs, dg, dr))
    dist_all = jnp.dot(got_ret[:, 0, :], place_f, precision=EXACT, preferred_element_type=F32)
    rank_all = jnp.dot(got_ret[:, 1, :], place_f, precision=EXACT, preferred_element_type=F32)
    dist_ref[...] = jnp.sum(owned_f * dist_all, axis=0, keepdims=True)
    rank_ref[...] = jnp.sum(owned_f * rank_all, axis=0, keepdims=True).astype(jnp.int32)
    for bufs in (id_bufs, row_bufs, ret_bufs):
        for dg in order:
            every(dg, lambda dr, dg=dg, bufs=bufs: wait_send(bufs, dg, dr))
    if extra:
        every(0, lambda dr: near_copy(peer(0, dr), me, dr).wait_send())
        for dg in order[:-1]:
            far_copy(my_group, lax.rem(my_group + dg, groups), dg).wait_send()


def fold(count, size):
    return jnp.floor((iota((1, count), 1).astype(F32) + 0.5) * (1.0 / size)).astype(jnp.int32)


def split(value):
    upper = value.astype(BF16)
    return upper, (value - upper.astype(F32)).astype(BF16)


def digits(value):
    upper = jnp.floor(value * (1.0 / 256.0))
    return upper.astype(BF16), (value - 256.0 * upper).astype(BF16)


def dot(left, right):
    return jnp.dot(left, right, preferred_element_type=F32)


def dot_nt(left, right):
    return lax.dot_general(left, right, NT, preferred_element_type=F32)


def fast_kernel(
    groups, replicas, direct, shared, spare,
    emb_in, ids_in, bounds_in,
    cent_ref, dist_ref, rank_ref, over_ref, ids_ref, bounds_ref,
    emb_ref, in_sems,
    unit, send_d, send_q, got_d, got_q, got_e,
    send_ids, got_ids, send_rank, got_rank, send_dist, got_dist,
    mask_d, mask_q, mask_e, total, ranks, spread,
    d_send, d_recv, id_send, id_recv, rank_send, rank_recv, dist_send, dist_recv,
    q_send, q_recv, qf_send, qf_recv, e_send, e_recv, ef_send, ef_recv,
):
    my_group = lax.axis_index("grp")
    my_replica = lax.axis_index("rep")
    me = my_group * replicas + my_replica
    owners = groups * replicas
    rows, width = emb_ref.shape
    limit = cent_ref.shape[0]
    planes, sides = replicas // 2, groups // 2
    my_plane, my_col = lax.div(my_replica, 2), lax.rem(my_replica, 2)
    my_side, my_core = lax.div(my_group, 2), lax.rem(my_group, 2)

    def turn(at, step, size):
        return lax.rem(at + step, size)

    def back(at, step, size):
        return lax.rem(at + (size - step), size)

    to_group = [turn(my_group, s, groups) for s in range(groups)]
    to_replica = [turn(my_replica, s, replicas) for s in range(replicas)]
    from_group = [back(my_group, s, groups) for s in range(groups)]
    from_replica = [back(my_replica, s, replicas) for s in range(replicas)]
    steps = [
        (dg, dr) for dg in range(groups) for dr in range(replicas) if dg or dr
    ]

    barrier = pltpu.get_barrier_semaphore()
    for dg, dr in steps:
        pl.semaphore_signal(
            barrier, inc=1, device_id=(to_group[dg], to_replica[dr]), device_id_type=MESH
        )

    def remote(src, dst, ssem, rsem, pair):
        return pltpu.make_async_remote_copy(
            src_ref=src, dst_ref=dst, send_sem=ssem, recv_sem=rsem,
            device_id=pair, device_id_type=MESH,
        )

    def pair_out(bufs, dg, dr):
        src, dst, ssem, rsem = bufs
        pair = (to_group[dg], to_replica[dr])
        there = pair[0] * replicas + pair[1]
        return remote(src.at[there], dst.at[me], ssem.at[there], rsem.at[me], pair)

    def pair_in(bufs, dg, dr):
        src, dst, ssem, rsem = bufs
        pair = (from_group[dg], from_replica[dr])
        there = pair[0] * replicas + pair[1]
        return remote(src.at[there], dst.at[there], ssem.at[there], rsem.at[there], pair)

    d_bufs = (send_d, got_d, d_send, d_recv)
    id_bufs = (send_ids, got_ids, id_send, id_recv)
    rank_bufs = (send_rank, got_rank, rank_send, rank_recv)
    dist_bufs = (send_dist, got_dist, dist_send, dist_recv)

    def q_out(dr):
        there = to_replica[dr]
        return remote(
            send_q.at[there], got_q.at[my_group, my_replica],
            q_send.at[dr], q_recv.at[dr], (my_group, there),
        )

    def q_in(dr):
        there = from_replica[dr]
        return remote(
            send_q.at[there], got_q.at[my_group, there],
            q_send.at[dr], q_recv.at[dr], (my_group, there),
        )

    sibling = (my_side * 2 + (1 - my_core), my_replica)

    def side_pair(ds, inward):
        side = back(my_side, ds, sides) if inward else turn(my_side, ds, sides)
        return (side * 2 + my_core, my_replica)

    def qf_side(ds, inward):
        pair = side_pair(ds, inward)
        group = pair[0] if inward else my_group
        ref = got_q.at[group]
        return remote(ref, ref, qf_send.at[ds], qf_recv.at[ds], pair)

    def qf_core(ds, inward):
        group = side_pair(ds, True)[0]
        group = group + (1 - 2 * my_core) if inward else group
        ref = got_q.at[group]
        return remote(ref, ref, qf_send.at[sides + ds], qf_recv.at[sides + ds], sibling)

    def e_plane(dp, inward):
        plane = back(my_plane, dp, planes) if inward else turn(my_plane, dp, planes)
        ref = got_e.at[my_group, my_col, plane if inward else my_plane]
        return remote(
            ref, ref, e_send.at[dp], e_recv.at[dp], (my_group, plane * 2 + my_col)
        )

    def e_spot(ds, dc, inward):
        side = back(my_side, ds, sides) if inward else turn(my_side, ds, sides)
        col = lax.rem(my_col + dc, 2)
        return side * 2 + my_core, col

    def ef_side(ds, dc, inward):
        group, col = e_spot(ds, dc, inward)
        ref = got_e.at[group, col] if inward else got_e.at[my_group, my_col]
        at = ds * 2 + dc
        return remote(
            ref, ref, ef_send.at[at], ef_recv.at[at], (group, my_plane * 2 + col)
        )

    def ef_core(ds, dc, inward):
        group, col = e_spot(ds, dc, True)
        group = group + (1 - 2 * my_core) if inward else group
        ref = got_e.at[group, col]
        at = groups + ds * 2 + dc
        return remote(ref, ref, ef_send.at[at], ef_recv.at[at], sibling)

    loads = [
        pltpu.make_async_copy(ids_in, ids_ref, in_sems.at[0]),
        pltpu.make_async_copy(bounds_in, bounds_ref, in_sems.at[1]),
        pltpu.make_async_copy(emb_in, emb_ref, in_sems.at[2]),
    ]
    for load in loads:
        load.start()
    loads[0].wait()
    loads[1].wait()
    ids = ids_ref[...]
    bounds = bounds_ref[...]
    diagonal = iota((owners, owners), 0) == iota((owners, owners), 1)
    edges = jnp.sum(jnp.where(diagonal, bounds, 0), axis=1, keepdims=True)
    owner = jnp.sum(ones_at(edges <= ids, F32), axis=0, keepdims=True).astype(jnp.int32) - 1
    owned = iota((owners, rows), 0) == owner
    owned_f = ones_at(owned, F32)
    earlier = ones_at(iota((rows, rows), 0) < iota((rows, rows), 1), BF16)
    prefix = dot(owned_f.astype(BF16), earlier)
    rank = jnp.sum(owned_f * prefix, axis=0, keepdims=True).astype(jnp.int32)
    column = lax.rem(owner, replicas)
    in_column = iota((replicas, rows), 0) == column
    late = rank >= direct
    column_f = ones_at(in_column, F32)
    late_f = jnp.where(late, column_f, 0.0)
    column_rank = jnp.sum(
        column_f * dot(late_f.astype(BF16), earlier), axis=0, keepdims=True
    ).astype(jnp.int32)
    in_direct = rank < direct
    in_shared = jnp.logical_and(late, column_rank < shared)
    in_spare = jnp.logical_and(late, column_rank >= shared)
    spare_f = ones_at(in_spare, F32)
    spare_rank = dot(
        jnp.broadcast_to(spare_f, (8, rows)).astype(BF16), earlier
    )[0:1, :].astype(jnp.int32)
    count = jnp.sum(spare_f, axis=1, keepdims=True)

    loads[2].wait()
    values = emb_ref[...].astype(F32)
    unit[...] = (
        values * lax.rsqrt(jnp.sum(values * values, axis=1, keepdims=True) + epsilon)
    ).astype(BF16)

    def picked(number, target):
        return dot(ones_at(iota((number, rows), 0) == target, BF16), unit[...]).astype(BF16)

    own_spare = picked(spare, jnp.where(in_spare, spare_rank, -1))
    got_e[my_group, my_col, my_plane] = own_spare
    packed = picked(replicas * shared, jnp.where(in_shared, column * shared + column_rank, -1))
    send_q[...] = packed.reshape(replicas, shared, width)
    got_q[my_group, my_replica] = send_q[my_replica]

    lane = jnp.where(
        in_direct, rank, jnp.where(in_shared, direct + column_rank, direct + shared + spare_rank)
    )
    place = ones_at(iota((LANES, rows), 0) == lane, BF16)
    near_f = jnp.concatenate([column_f] * groups, axis=0)
    chosen = jnp.where(in_direct, owned_f, jnp.where(in_shared, near_f, 1.0))
    id_high = jnp.floor(ids.astype(F32) * (1.0 / 256.0))
    id_low = ids.astype(F32) - 256.0 * id_high
    used = direct + shared + spare
    three = jnp.concatenate([chosen * id_high, chosen * id_low, chosen], axis=0).astype(BF16)
    table = dot_nt(three, place)
    table = 256.0 * table[0:owners] + table[owners : 2 * owners] + table[2 * owners :] - 1.0
    table = jnp.where(iota((owners, LANES), 1) < used, table, count)
    send_ids[...] = table.reshape(owners, 1, LANES)
    got_ids[me] = send_ids[me]

    pl.semaphore_wait(barrier, owners - 1)
    for dp in range(1, planes):
        e_plane(dp, False).start()
    for dr in range(1, replicas):
        q_out(dr).start()
    for dg, dr in steps:
        pair_out(id_bufs, dg, dr).start()

    target = jnp.where(in_direct, owner * direct + rank, -1)
    block = replicas * direct
    for dg in list(range(1, groups)) + [0]:
        tg = to_group[dg]
        packed = picked(block, target - tg * block)
        send_d[pl.ds(tg * replicas, replicas)] = packed.reshape(replicas, direct, width)
        for dr in range(replicas):
            if dg or dr:
                pair_out(d_bufs, dg, dr).start()
    got_d[me] = send_d[me]

    for dp in range(1, planes):
        e_plane(dp, True).wait_recv()
    others = [(ds, dc) for ds in range(sides) for dc in range(2) if ds or dc]
    for ds, dc in others:
        ef_side(ds, dc, False).start()
    ef_core(0, 0, False).start()
    for dr in range(1, replicas):
        q_in(dr).wait_recv()
    for ds in range(1, sides):
        qf_side(ds, False).start()
    qf_core(0, False).start()

    direct_row, shared_row, spare_row = groups * block, owners * shared, owners * spare
    d_lane, q_lane, e_lane = fold(block, direct), fold(block, shared), fold(replicas * spare, spare)
    e_col = fold(replicas * spare, spare * planes)
    e_source = (e_lane - e_col * planes) * 2 + e_col
    d_slot = iota((1, block), 1) - d_lane * direct
    q_slot = iota((1, block), 1) - q_lane * shared + direct
    e_slot = iota((1, replicas * spare), 1) - e_lane * spare + (direct + shared)
    lane_source = jnp.concatenate([d_lane, q_lane, e_source], axis=1)
    lane_slot = jnp.concatenate([d_slot, q_slot, e_slot], axis=1)
    span = lane_source.shape[1]
    expand = ones_at(iota((LANES, span), 0) == lane_slot, BF16)
    from_source = ones_at(iota((replicas, span), 0) == lane_source, F32)
    key = lane_source * used + lane_slot
    key_col = jnp.sum(
        jnp.where(iota((span, span), 0) == iota((span, span), 1), key, 0), axis=1, keepdims=True
    )
    before = ones_at(key_col < key, BF16)

    def spread_rows(size, offset):
        at = jnp.floor((iota((size, LANES), 0).astype(F32) + 0.5) * (1.0 / offset[0]))
        slot = iota((size, LANES), 0) - at.astype(jnp.int32) * offset[0] + offset[1]
        return ones_at(slot == iota((size, LANES), 1), BF16)

    spread[0:direct_row] = spread_rows(direct_row, (direct, 0))
    spread[direct_row : direct_row + shared_row] = spread_rows(shared_row, (shared, direct))
    spread[direct_row + shared_row :] = spread_rows(spare_row, (spare, direct + shared))

    d_all = fold(direct_row, direct)
    q_all = fold(shared_row, shared)
    e_all = fold(spare_row, spare)
    e_group = fold(spare_row, replicas * spare)
    e_inner = e_all - e_group * replicas
    e_side = fold(spare_row, planes * spare) - e_group * 2
    e_all = e_group * replicas + (e_inner - e_side * planes) * 2 + e_side
    all_source = jnp.concatenate([d_all, q_all, e_all], axis=1)

    def by_source(row, parts):
        held = jnp.where(iota((owners, row.shape[1]), 0) == all_source, row, 0.0)
        upper, lower = parts(held)
        both = dot(jnp.concatenate([upper, lower], axis=0), spread[...])
        return both[0:owners], both[owners:]

    for dg, dr in steps:
        pair_in(id_bufs, dg, dr).wait_recv()
    named = got_ids[...].reshape(owners, LANES)
    over_ref[0, 0] = jnp.where(jnp.max(named[:, used:]) > spare, 1, 0)
    begin = jnp.sum(jnp.where(iota((owners, 1), 0) == me, edges, 0), axis=0, keepdims=True)
    ending = jnp.sum(
        jnp.where(iota((owners, 1), 0) == me + 1, edges, 0), axis=0, keepdims=True
    ) + jnp.where(me == owners - 1, CL_DEV * owners, 0)
    begin, ending = begin.astype(F32), ending.astype(F32)
    mine = jnp.logical_and(named >= begin, named < ending)
    local = jnp.where(mine, named - begin + 1.0, 0.0)
    local_high, local_low = digits(local)
    flat_both = dot(jnp.concatenate([local_high, local_low], axis=0), expand)
    flat_all = 256.0 * flat_both[0:owners] + flat_both[owners:] - 1.0

    seen = jnp.zeros((limit, 1), F32)
    cluster = iota((limit, span), 0)
    wide = replicas * spare
    for sg in range(groups):
        flat = jnp.sum(
            from_source * flat_all[sg * replicas : (sg + 1) * replicas], axis=0, keepdims=True
        )
        mask = ones_at(cluster == flat.astype(jnp.int32), F32)
        mask_b = mask.astype(BF16)
        mask_d[:, sg * block : (sg + 1) * block] = mask_b[:, 0:block]
        mask_q[:, sg * block : (sg + 1) * block] = mask_b[:, block : 2 * block]
        mask_e[:, sg * wide : (sg + 1) * wide] = mask_b[:, 2 * block :]
        ahead = dot(mask_b, before) + seen
        slot = jnp.sum(mask * ahead, axis=0, keepdims=True)
        ranks[:, sg * block : (sg + 1) * block] = slot[:, 0:block]
        at = direct_row + sg * block
        ranks[:, at : at + block] = slot[:, block : 2 * block]
        at = direct_row + shared_row + sg * wide
        ranks[:, at : at + wide] = slot[:, 2 * block :]
        seen = seen + jnp.sum(mask, axis=1, keepdims=True)

    upper, lower = by_source(ranks[...], digits)
    send_rank[...] = (256.0 * upper + lower).reshape(owners, 1, LANES)
    got_rank[me] = send_rank[me]
    for dg, dr in steps:
        pair_out(rank_bufs, dg, dr).start()

    for ds in range(1, sides):
        qf_side(ds, True).wait_recv()
        qf_core(ds, False).start()
    for ds, dc in others:
        ef_side(ds, dc, True).wait_recv()
        ef_core(ds, dc, False).start()

    for ds in range(sides):
        qf_core(ds, True).wait_recv()
    rows_q = got_q[...].reshape(shared_row, width)
    total[...] = dot(mask_q[...], rows_q)
    for ds in range(sides):
        for dc in range(2):
            ef_core(ds, dc, True).wait_recv()
    rows_e = got_e[...].reshape(spare_row, width)
    total[...] += dot(mask_e[...], rows_e)

    for dg, dr in steps:
        pair_in(rank_bufs, dg, dr).wait_recv()

    def collect(ref, parts, scale):
        upper, lower = parts(ref[...].reshape(owners, LANES))
        both = dot(jnp.concatenate([upper, lower], axis=0), place)
        return jnp.sum(
            owned_f * (scale * both[0:owners] + both[owners:]), axis=0, keepdims=True
        )

    rank_ref[...] = collect(got_rank, digits, 256.0).astype(jnp.int32)

    for dg, dr in steps:
        pair_in(d_bufs, dg, dr).wait_recv()
    rows_d = got_d[...].reshape(direct_row, width)
    sums = total[...] + dot(mask_d[...], rows_d)
    share = 1.0 / jnp.maximum(seen, 1.0)
    norm = share * jnp.sqrt(jnp.sum(sums * sums, axis=1, keepdims=True))
    cent_ref[...] = (sums * (share / jnp.maximum(norm, norm_floor))).astype(BF16)

    def near(mask_ref, begin_at, end_at, block_rows):
        score = dot_nt(cent_ref[...], block_rows)
        return jnp.sum(
            mask_ref[:, begin_at:end_at].astype(F32) * score, axis=0, keepdims=True
        )

    half = spare_row // 2
    nears = jnp.concatenate([
        near(mask_d, 0, direct_row, got_d[...].reshape(direct_row, width)),
        near(mask_q, 0, shared_row, got_q[...].reshape(shared_row, width)),
        near(mask_e, 0, half, got_e[0 : groups // 2].reshape(half, width)),
        near(mask_e, half, spare_row, got_e[groups // 2 :].reshape(half, width)),
    ], axis=1)
    upper, lower = by_source(nears, split)
    send_dist[...] = (upper + lower).reshape(owners, 1, LANES)
    got_dist[me] = send_dist[me]
    for dg, dr in steps:
        pair_out(dist_bufs, dg, dr).start()

    for bufs in (id_bufs, d_bufs, rank_bufs):
        for dg, dr in steps:
            pair_out(bufs, dg, dr).wait_send()
    for dp in range(1, planes):
        e_plane(dp, False).wait_send()
    for dr in range(1, replicas):
        q_out(dr).wait_send()
    for ds, dc in others:
        ef_side(ds, dc, False).wait_send()
    for ds in range(1, sides):
        qf_side(ds, False).wait_send()
    for ds in range(sides):
        qf_core(ds, False).wait_send()
        for dc in range(2):
            ef_core(ds, dc, False).wait_send()

    for dg, dr in steps:
        pair_in(dist_bufs, dg, dr).wait_recv()
    dist_ref[...] = 1.0 - collect(got_dist, split, 1.0)
    for dg, dr in steps:
        pair_out(dist_bufs, dg, dr).wait_send()


def store_kernel(cent_ref, dist_ref, rank_ref, cent_out, dist_out, rank_out, sems):
    pieces = sems.shape[0] - 2
    size = cent_ref.shape[0] // pieces
    copies = [
        pltpu.make_async_copy(
            cent_ref.at[pl.ds(at * size, size)], cent_out.at[pl.ds(at * size, size)], sems.at[at]
        )
        for at in range(pieces)
    ]
    copies.append(pltpu.make_async_copy(dist_ref, dist_out, sems.at[pieces]))
    copies.append(pltpu.make_async_copy(rank_ref, rank_out, sems.at[pieces + 1]))
    for copy in copies:
        copy.start()
    for copy in copies:
        copy.wait()


def solution(mesh):
    groups, replicas = mesh.shape["grp"], mesh.shape["rep"]
    owners = groups * replicas

    def shards(embeddings, cluster_ids, owner_bounds):
        rows, width = embeddings.shape
        limit = CL_DEV + CL_DEV // 2
        most = -(-(3 * rows // owners) // 16) * 16
        direct, shared, spare = 16, 16, 32
        vmem = pl.BlockSpec(memory_space=pltpu.VMEM)
        scalar = pl.BlockSpec(memory_space=pltpu.SMEM)
        anywhere = pl.BlockSpec(memory_space=pl.ANY)
        outside = pl.BlockSpec(memory_space=pltpu.HBM)
        each = pltpu.SemaphoreType.DMA((owners,))
        ids_row = cluster_ids.reshape(1, rows)
        bounds_row = owner_bounds.reshape(1, owners)
        outs = (
            jax.ShapeDtypeStruct((limit, width), BF16),
            jax.ShapeDtypeStruct((1, rows), F32),
            jax.ShapeDtypeStruct((1, rows), jnp.int32),
            jax.ShapeDtypeStruct((1, 1), jnp.int32),
        )

        def run(number, ids_in, bounds_in):
            small = pltpu.VMEM((owners, 8, LANES), F32)
            near = pltpu.SemaphoreType.DMA((replicas,))
            far = pltpu.SemaphoreType.DMA((groups,))
            return pl.pallas_call(
                functools.partial(kernel, groups, replicas, most, 0),
                out_shape=outs,
                in_specs=[anywhere] * 3,
                out_specs=(vmem, vmem, vmem, scalar),
                scratch_shapes=[
                    pltpu.VMEM((rows, width), BF16),
                    pltpu.VMEM((1, rows), jnp.int32),
                    pltpu.VMEM((1, owners), jnp.int32),
                    pltpu.SemaphoreType.DMA((3,)),
                    pltpu.VMEM((rows, width), BF16),
                    pltpu.VMEM((owners, most, width), BF16),
                    pltpu.VMEM((owners, most, width), BF16),
                    small,
                    small,
                    pltpu.VMEM((groups, limit, replicas * most), BF16),
                    pltpu.VMEM((limit, width), F32),
                    small,
                    small,
                    pltpu.VMEM((groups, replicas, LANES), F32),
                    each, each, each, each, each, each, near, near, far, far,
                ],
                compiler_params=pltpu.CompilerParams(
                    collective_id=number,
                    has_side_effects=True,
                    vmem_limit_bytes=48 * 1024 * 1024,
                ),
            )(embeddings, ids_in, bounds_in)

        def run_fast(number):
            small = pltpu.VMEM((owners, 1, LANES), F32)
            slots = owners * (direct + shared + spare)
            return pl.pallas_call(
                functools.partial(fast_kernel, groups, replicas, direct, shared, spare),
                out_shape=outs + (
                    jax.ShapeDtypeStruct((1, rows), jnp.int32),
                    jax.ShapeDtypeStruct((1, owners), jnp.int32),
                ),
                in_specs=[outside] * 3,
                out_specs=(vmem, vmem, vmem, scalar, vmem, vmem),
                scratch_shapes=[
                    pltpu.VMEM((rows, width), BF16),
                    pltpu.SemaphoreType.DMA((3,)),
                    pltpu.VMEM((rows, width), BF16),
                    pltpu.VMEM((owners, direct, width), BF16),
                    pltpu.VMEM((replicas, shared, width), BF16),
                    pltpu.VMEM((owners, direct, width), BF16),
                    pltpu.VMEM((groups, replicas, shared, width), BF16),
                    pltpu.VMEM((groups, 2, replicas // 2, spare, width), BF16),
                    small, small, small, small, small, small,
                    pltpu.VMEM((limit, owners * direct), BF16),
                    pltpu.VMEM((limit, owners * shared), BF16),
                    pltpu.VMEM((limit, owners * spare), BF16),
                    pltpu.VMEM((limit, width), F32),
                    pltpu.VMEM((1, slots), F32),
                    pltpu.VMEM((slots, LANES), BF16),
                    each, each, each, each, each, each, each, each,
                    pltpu.SemaphoreType.DMA((replicas,)),
                    pltpu.SemaphoreType.DMA((replicas,)),
                    pltpu.SemaphoreType.DMA((groups,)),
                    pltpu.SemaphoreType.DMA((groups,)),
                    pltpu.SemaphoreType.DMA((replicas // 2,)),
                    pltpu.SemaphoreType.DMA((replicas // 2,)),
                    pltpu.SemaphoreType.DMA((2 * groups,)),
                    pltpu.SemaphoreType.DMA((2 * groups,)),
                ],
                compiler_params=pltpu.CompilerParams(
                    collective_id=number,
                    has_side_effects=True,
                    vmem_limit_bytes=48 * 1024 * 1024,
                ),
            )(*(pltpu.with_memory_space_constraint(x, pltpu.HBM) for x in (embeddings, ids_row, bounds_row)))

        whole = groups % 2 == 0 and replicas * direct == LANES and rows // owners <= direct
        if most > 2 * direct and whole:
            first = run_fast(0)
            centroids, distance, rank = lax.cond(
                first[3][0, 0] > 0, lambda: run(1, first[4], first[5])[:3], lambda: first[:3]
            )
        else:
            centroids, distance, rank, _ = run(0, ids_row, bounds_row)
        centroids, distance, rank = pl.pallas_call(
            store_kernel,
            out_shape=outs[:3],
            in_specs=[vmem] * 3,
            out_specs=(anywhere,) * 3,
            scratch_shapes=[pltpu.SemaphoreType.DMA((6,))],
        )(centroids, distance, rank)
        return distance.reshape(rows), rank.reshape(rows), centroids[None]

    placed = (P(("grp", "rep"), None), P(("grp", "rep")), P())
    return jax.shard_map(
        shards,
        mesh=mesh,
        in_specs=placed,
        out_specs=(P(("grp", "rep")), P(("grp", "rep")), P(("grp", "rep"), None, None)),
        check_vma=False,
    )
```

```python
import functools

import jax
import jax.numpy as jnp
from jax import lax
from jax.experimental import pallas as pl
from jax.experimental.pallas import tpu as pltpu
from jax.sharding import PartitionSpec as P

CL_DEV = 384
LANES = 128

epsilon = 1e-06
norm_floor = 0.25
MESH = pl.DeviceIdType.MESH
F32 = jnp.float32
BF16 = jnp.bfloat16
EXACT = lax.Precision.HIGHEST
NT = (((1,), (1,)), ((), ()))


def iota(shape, dim):
    return lax.broadcasted_iota(jnp.int32, shape, dim)


def ones_at(mask, kind):
    return jnp.where(mask, 1.0, 0.0).astype(kind)


def digits_dot(table, place):
    high = jnp.floor(table * (1.0 / 32.0))
    low = table - 32.0 * high
    upper = jnp.dot(high.astype(BF16), place, preferred_element_type=F32)
    lower = jnp.dot(low.astype(BF16), place, preferred_element_type=F32)
    return 32.0 * upper + lower


def kernel(
    groups, replicas, direct, extra,
    emb_in, ids_in, bounds_in,
    cent_ref, dist_ref, rank_ref, over_ref,
    emb_ref, ids_ref, bounds_ref, in_sems,
    unit, send_rows, got_rows, send_ids, got_ids, member, total, ret, got_ret, slot_mat,
    row_send, row_recv, id_send, id_recv, ret_send, ret_recv,
    near_send, near_recv, far_send, far_recv,
):
    my_group = lax.axis_index("grp")
    my_replica = lax.axis_index("rep")
    me = my_group * replicas + my_replica
    owners = groups * replicas
    rows, width = emb_ref.shape
    limit = cent_ref.shape[0]
    slots = direct + extra
    block = replicas * slots
    sent = replicas * direct

    def peer(dg, dr):
        return lax.rem(my_group + dg, groups), lax.rem(my_replica + dr, replicas)

    def source(dg, dr):
        return (
            lax.rem(my_group + groups - dg, groups),
            lax.rem(my_replica + replicas - dr, replicas),
        )

    def every(dg, act):
        def one(dr, carry):
            act(dr)
            return carry

        lax.fori_loop(1 if dg == 0 else 0, replicas, one, 0)

    def copy(src, dst, ssem, rsem, pair, here, there):
        return pltpu.make_async_remote_copy(
            src_ref=src.at[there],
            dst_ref=dst.at[here, pl.ds(0, direct)] if dst is got_rows else dst.at[here],
            send_sem=ssem.at[there],
            recv_sem=rsem.at[here],
            device_id=pair,
            device_id_type=MESH,
        )

    def start(bufs, dg, dr):
        pair = peer(dg, dr)
        copy(*bufs, pair, me, pair[0] * replicas + pair[1]).start()

    def wait_send(bufs, dg, dr):
        pair = peer(dg, dr)
        copy(*bufs, pair, me, pair[0] * replicas + pair[1]).wait_send()

    def wait_recv(bufs, dg, dr):
        pair = source(dg, dr)
        there = pair[0] * replicas + pair[1]
        copy(*bufs, pair, there, there).wait_recv()

    row_bufs = (send_rows, got_rows, row_send, row_recv)
    id_bufs = (send_ids, got_ids, id_send, id_recv)
    ret_bufs = (ret, got_ret, ret_send, ret_recv)
    order = list(range(1, groups)) + [0]

    barrier = pltpu.get_barrier_semaphore()
    for dg in order:
        every(
            dg,
            lambda dr, dg=dg: pl.semaphore_signal(
                barrier, inc=1, device_id=peer(dg, dr), device_id_type=MESH
            ),
        )

    loads = [
        pltpu.make_async_copy(emb_in, emb_ref, in_sems.at[0]),
        pltpu.make_async_copy(ids_in, ids_ref, in_sems.at[1]),
        pltpu.make_async_copy(bounds_in, bounds_ref, in_sems.at[2]),
    ]
    for load in loads:
        load.start()
    for load in loads:
        load.wait()
    ids = ids_ref[...]
    diagonal = iota((owners, owners), 0) == iota((owners, owners), 1)
    edges = jnp.sum(jnp.where(diagonal, bounds_ref[...], 0), axis=1, keepdims=True)
    reached = ones_at(edges <= ids, F32)
    owner = jnp.sum(reached, axis=0, keepdims=True).astype(jnp.int32) - 1
    owned = iota((owners, rows), 0) == owner
    owned_f = ones_at(owned, F32)
    first = jnp.sum(owned_f * edges.astype(F32), axis=0, keepdims=True)
    local = ids.astype(F32) - first
    earlier = ones_at(iota((rows, rows), 0) < iota((rows, rows), 1), BF16)
    prefix = jnp.dot(owned_f.astype(BF16), earlier, preferred_element_type=F32)
    rank = jnp.sum(owned_f * prefix, axis=0, keepdims=True).astype(jnp.int32)
    target = jnp.where(rank < direct, owner * direct + rank, -1)
    spot = rank
    if extra:
        late = ones_at(rank >= direct, F32)
        queue = jnp.dot(
            jnp.broadcast_to(late, (8, rows)).astype(BF16), earlier, preferred_element_type=F32
        )[0:1, :].astype(jnp.int32)
        spot = jnp.where(rank < direct, rank, direct + queue)
    place = ones_at(iota((LANES, rows), 0) == spot, BF16)

    values = emb_ref[...].astype(F32)
    unit[...] = (
        values * lax.rsqrt(jnp.sum(values * values, axis=1, keepdims=True) + epsilon)
    ).astype(BF16)

    def pack(dg):
        tg = lax.rem(my_group + dg, groups)
        pick = ones_at(iota((sent, rows), 0) + tg * sent == target, BF16)
        packed = jnp.dot(pick, unit[...], preferred_element_type=F32).astype(BF16)
        send_rows[pl.ds(tg * replicas, replicas)] = packed.reshape(replicas, direct, width)

    def near_copy(pair, owner_at, dr):
        ref = got_rows.at[owner_at, pl.ds(direct, extra)]
        return pltpu.make_async_remote_copy(
            src_ref=ref, dst_ref=ref, send_sem=near_send.at[dr], recv_sem=near_recv.at[dr],
            device_id=pair, device_id_type=MESH,
        )

    def far_copy(group_at, to_group, dg):
        ref = got_rows.at[pl.ds(group_at * replicas, replicas), pl.ds(direct, extra)]
        return pltpu.make_async_remote_copy(
            src_ref=ref, dst_ref=ref, send_sem=far_send.at[dg], recv_sem=far_recv.at[dg],
            device_id=(to_group, my_replica), device_id_type=MESH,
        )

    if extra:
        pick = ones_at(iota((extra, rows), 0) + direct == spot, BF16)
        got_rows[me, direct:slots] = jnp.dot(
            pick, unit[...], preferred_element_type=F32
        ).astype(BF16)
    pack(order[0])
    pl.semaphore_wait(barrier, owners - 1)
    if extra:
        every(0, lambda dr: near_copy(peer(0, dr), me, dr).start())
    every(order[0], lambda dr: start(row_bufs, order[0], dr))

    high = jnp.floor(local * (1.0 / 32.0))
    low = local - 32.0 * high
    owned_d = jnp.where(rank < direct, owned_f, 0.0)
    upper = lax.dot_general((owned_d * high).astype(BF16), place, NT, preferred_element_type=F32)
    lower = lax.dot_general((owned_d * low).astype(BF16), place, NT, preferred_element_type=F32)
    filled = lax.dot_general(owned_d.astype(BF16), place, NT, preferred_element_type=F32)
    id_table = 32.0 * upper + lower + filled - 1.0
    count = jnp.zeros((1, 1), F32)
    if extra:
        named = jnp.broadcast_to(late * (ids.astype(F32) + 1.0), (8, rows))
        others = lax.dot_general(
            named, place.astype(F32), NT, precision=EXACT, preferred_element_type=F32
        )
        id_table = id_table + others[0:1, :]
        count = jnp.sum(late, axis=1, keepdims=True)
    top = iota((8, LANES), 0) == 0
    for o in range(owners):
        send_ids[o] = jnp.where(top, id_table[o : o + 1, :], count)
    got_ids[me] = send_ids[me]

    for dg in order:
        every(dg, lambda dr, dg=dg: start(id_bufs, dg, dr))
    for dg in order[1:]:
        pack(dg)
        every(dg, lambda dr, dg=dg: start(row_bufs, dg, dr))
    got_rows[me, 0:direct] = send_rows[me]
    if extra:
        def near_wait(dr):
            pair = source(0, dr)
            near_copy(pair, pair[0] * replicas + pair[1], dr).wait_recv()

        every(0, near_wait)
        for dg in order[:-1]:
            far_copy(my_group, lax.rem(my_group + dg, groups), dg).start()

    for dg in order:
        every(dg, lambda dr, dg=dg: wait_recv(id_bufs, dg, dr))
    worst = jnp.max(got_ids[:, 1, :], axis=0, keepdims=True)
    over_ref[0, 0] = jnp.where(jnp.max(worst) > extra, 1, 0)
    begin = jnp.sum(
        jnp.where(iota((owners, 1), 0) == me, edges, 0), axis=0, keepdims=True
    ).astype(F32)
    ending = jnp.sum(
        jnp.where(iota((owners, 1), 0) == me + 1, edges, 0), axis=0, keepdims=True
    ).astype(F32) + jnp.where(me == owners - 1, float(CL_DEV * owners), 0.0)

    lane = iota((1, block), 1)
    quotient = jnp.zeros((1, block), jnp.int32)
    for s in range(1, replicas):
        quotient = quotient + jnp.where(lane >= s * slots, 1, 0)
    remainder = lane - quotient * slots
    spread = iota((LANES, block), 0) == remainder
    spread_b, spread_f = ones_at(spread, BF16), ones_at(spread, F32)
    from_source = ones_at(iota((replicas, block), 0) == quotient, F32)
    before = ones_at(iota((block, block), 0) < iota((block, block), 1), BF16)
    cluster = iota((limit, block), 0)

    seen = jnp.zeros((limit, 1), F32)
    for sg in range(groups):
        table = got_ids[sg * replicas : (sg + 1) * replicas, 0, :]
        if extra:
            mine = jnp.where((table >= begin) & (table < ending), table - begin, -1.0)
            table = jnp.where(iota((replicas, LANES), 1) < direct, table, mine)
        flat = jnp.sum(from_source * digits_dot(table, spread_b), axis=0, keepdims=True)
        mask = ones_at(cluster == flat.astype(jnp.int32), F32)
        mask_b = mask.astype(BF16)
        member[sg] = mask_b
        ahead = jnp.dot(mask_b, before, preferred_element_type=F32) + seen
        slot = jnp.sum(mask * ahead, axis=0, keepdims=True)
        seen = seen + jnp.sum(mask, axis=1, keepdims=True)
        slot_mat[sg] = lax.dot_general(
            from_source * slot, spread_f, NT, precision=EXACT, preferred_element_type=F32
        )
    total[...] = jnp.zeros_like(total)
    for dg in order:
        sg = lax.rem(my_group + groups - dg, groups)
        every(dg, lambda dr, dg=dg: wait_recv(row_bufs, dg, dr))
        if extra and dg:
            far_copy(sg, sg, dg).wait_recv()
        block_rows = got_rows[pl.ds(sg * replicas, replicas)].reshape(block, width)
        total[...] += jnp.dot(member[sg], block_rows, preferred_element_type=F32)

    centroid = total[...] / jnp.maximum(seen, 1.0)
    norm = jnp.sqrt(jnp.sum(centroid * centroid, axis=1, keepdims=True))
    cent_ref[...] = (centroid / jnp.maximum(norm, norm_floor)).astype(BF16)

    for dg in order:
        sg = lax.rem(my_group + groups - dg, groups)
        tg = lax.rem(my_group + groups - dg, groups)
        block_rows = got_rows[pl.ds(sg * replicas, replicas)].reshape(block, width)
        score = lax.dot_general(cent_ref[...], block_rows, NT, preferred_element_type=F32)
        near = jnp.sum(member[sg].astype(F32) * score, axis=0, keepdims=True)
        dist_mat = lax.dot_general(
            from_source * (1.0 - near), spread_f, NT, precision=EXACT, preferred_element_type=F32
        )
        rank_mat = slot_mat[sg]
        for s in range(replicas):
            ret[tg * replicas + s] = jnp.where(top, dist_mat[s : s + 1, :], rank_mat[s : s + 1, :])
        back = (groups - dg) % groups
        every(back, lambda dr, back=back: start(ret_bufs, back, dr))
    got_ret[me] = ret[me]

    place_f = ones_at(iota((LANES, rows), 0) == spot, F32)
    for dg in order:
        every(dg, lambda dr, dg=dg: wait_recv(ret_bufs, dg, dr))
    dist_all = jnp.dot(got_ret[:, 0, :], place_f, precision=EXACT, preferred_element_type=F32)
    rank_all = jnp.dot(got_ret[:, 1, :], place_f, precision=EXACT, preferred_element_type=F32)
    dist_ref[...] = jnp.sum(owned_f * dist_all, axis=0, keepdims=True)
    rank_ref[...] = jnp.sum(owned_f * rank_all, axis=0, keepdims=True).astype(jnp.int32)
    for bufs in (id_bufs, row_bufs, ret_bufs):
        for dg in order:
            every(dg, lambda dr, dg=dg, bufs=bufs: wait_send(bufs, dg, dr))
    if extra:
        every(0, lambda dr: near_copy(peer(0, dr), me, dr).wait_send())
        for dg in order[:-1]:
            far_copy(my_group, lax.rem(my_group + dg, groups), dg).wait_send()


def fold(count, size):
    return jnp.floor((iota((1, count), 1).astype(F32) + 0.5) * (1.0 / size)).astype(jnp.int32)


def split(value):
    upper = value.astype(BF16)
    return upper, (value - upper.astype(F32)).astype(BF16)


def digits(value):
    upper = jnp.floor(value * (1.0 / 256.0))
    return upper.astype(BF16), (value - 256.0 * upper).astype(BF16)


def dot(left, right):
    return jnp.dot(left, right, preferred_element_type=F32)


def dot_nt(left, right):
    return lax.dot_general(left, right, NT, preferred_element_type=F32)


def fast_kernel(
    groups, replicas, direct, shared, spare,
    emb_in, ids_in, bounds_in,
    cent_ref, dist_ref, rank_ref, over_ref, ids_ref, bounds_ref,
    emb_ref, in_sems,
    unit, send_d, send_q, got_d, got_q, got_e,
    send_ids, got_ids, send_rank, got_rank, send_dist, got_dist,
    mask_d, mask_q, mask_e, total, ranks, spread,
    d_send, d_recv, id_send, id_recv, rank_send, rank_recv, dist_send, dist_recv,
    q_send, q_recv, qf_send, qf_recv, e_send, e_recv, ef_send, ef_recv,
):
    my_group = lax.axis_index("grp")
    my_replica = lax.axis_index("rep")
    me = my_group * replicas + my_replica
    owners = groups * replicas
    rows, width = emb_ref.shape
    limit = cent_ref.shape[0]
    planes, sides = replicas // 2, groups // 2
    my_plane, my_col = lax.div(my_replica, 2), lax.rem(my_replica, 2)
    my_side, my_core = lax.div(my_group, 2), lax.rem(my_group, 2)

    def turn(at, step, size):
        return lax.rem(at + step, size)

    def back(at, step, size):
        return lax.rem(at + (size - step), size)

    to_group = [turn(my_group, s, groups) for s in range(groups)]
    to_replica = [turn(my_replica, s, replicas) for s in range(replicas)]
    from_group = [back(my_group, s, groups) for s in range(groups)]
    from_replica = [back(my_replica, s, replicas) for s in range(replicas)]
    steps = [
        (dg, dr) for dg in range(groups) for dr in range(replicas) if dg or dr
    ]

    barrier = pltpu.get_barrier_semaphore()
    for dg, dr in steps:
        pl.semaphore_signal(
            barrier, inc=1, device_id=(to_group[dg], to_replica[dr]), device_id_type=MESH
        )

    def remote(src, dst, ssem, rsem, pair):
        return pltpu.make_async_remote_copy(
            src_ref=src, dst_ref=dst, send_sem=ssem, recv_sem=rsem,
            device_id=pair, device_id_type=MESH,
        )

    def pair_out(bufs, dg, dr):
        src, dst, ssem, rsem = bufs
        pair = (to_group[dg], to_replica[dr])
        there = pair[0] * replicas + pair[1]
        return remote(src.at[there], dst.at[me], ssem.at[there], rsem.at[me], pair)

    def pair_in(bufs, dg, dr):
        src, dst, ssem, rsem = bufs
        pair = (from_group[dg], from_replica[dr])
        there = pair[0] * replicas + pair[1]
        return remote(src.at[there], dst.at[there], ssem.at[there], rsem.at[there], pair)

    d_bufs = (send_d, got_d, d_send, d_recv)
    id_bufs = (send_ids, got_ids, id_send, id_recv)
    rank_bufs = (send_rank, got_rank, rank_send, rank_recv)
    dist_bufs = (send_dist, got_dist, dist_send, dist_recv)

    def q_out(dr):
        there = to_replica[dr]
        return remote(
            send_q.at[there], got_q.at[my_group, my_replica],
            q_send.at[dr], q_recv.at[dr], (my_group, there),
        )

    def q_in(dr):
        there = from_replica[dr]
        return remote(
            send_q.at[there], got_q.at[my_group, there],
            q_send.at[dr], q_recv.at[dr], (my_group, there),
        )

    sibling = (my_side * 2 + (1 - my_core), my_replica)

    def side_pair(ds, inward):
        side = back(my_side, ds, sides) if inward else turn(my_side, ds, sides)
        return (side * 2 + my_core, my_replica)

    def qf_side(ds, inward):
        pair = side_pair(ds, inward)
        group = pair[0] if inward else my_group
        ref = got_q.at[group]
        return remote(ref, ref, qf_send.at[ds], qf_recv.at[ds], pair)

    def qf_core(ds, inward):
        group = side_pair(ds, True)[0]
        group = group + (1 - 2 * my_core) if inward else group
        ref = got_q.at[group]
        return remote(ref, ref, qf_send.at[sides + ds], qf_recv.at[sides + ds], sibling)

    def e_plane(dp, inward):
        plane = back(my_plane, dp, planes) if inward else turn(my_plane, dp, planes)
        ref = got_e.at[my_group, my_col, plane if inward else my_plane]
        return remote(
            ref, ref, e_send.at[dp], e_recv.at[dp], (my_group, plane * 2 + my_col)
        )

    def e_spot(ds, dc, inward):
        side = back(my_side, ds, sides) if inward else turn(my_side, ds, sides)
        col = lax.rem(my_col + dc, 2)
        return side * 2 + my_core, col

    def ef_side(ds, inward):
        group = e_spot(ds, 0, inward)[0]
        ref = got_e.at[group if inward else my_group, my_col]
        return remote(
            ref, ref, ef_send.at[2 * ds], ef_recv.at[2 * ds], (group, my_replica)
        )

    def ef_col(ds, inward):
        group = e_spot(ds, 0, True)[0]
        ref = got_e.at[group, 1 - my_col if inward else my_col]
        at = 2 * ds + 1
        return remote(
            ref, ref, ef_send.at[at], ef_recv.at[at],
            (my_group, my_plane * 2 + (1 - my_col)),
        )

    def ef_core(ds, dc, inward):
        group, col = e_spot(ds, dc, True)
        group = group + (1 - 2 * my_core) if inward else group
        ref = got_e.at[group, col]
        at = groups + ds * 2 + dc
        return remote(ref, ref, ef_send.at[at], ef_recv.at[at], sibling)

    loads = [
        pltpu.make_async_copy(ids_in, ids_ref, in_sems.at[0]),
        pltpu.make_async_copy(bounds_in, bounds_ref, in_sems.at[1]),
        pltpu.make_async_copy(emb_in, emb_ref, in_sems.at[2]),
    ]
    for load in loads:
        load.start()
    loads[0].wait()
    loads[1].wait()
    ids = ids_ref[...]
    bounds = bounds_ref[...]
    diagonal = iota((owners, owners), 0) == iota((owners, owners), 1)
    edges = jnp.sum(jnp.where(diagonal, bounds, 0), axis=1, keepdims=True)
    owner = jnp.sum(ones_at(edges <= ids, F32), axis=0, keepdims=True).astype(jnp.int32) - 1
    owned = iota((owners, rows), 0) == owner
    owned_f = ones_at(owned, F32)
    earlier = ones_at(iota((rows, rows), 0) < iota((rows, rows), 1), BF16)
    prefix = dot(owned_f.astype(BF16), earlier)
    rank = jnp.sum(owned_f * prefix, axis=0, keepdims=True).astype(jnp.int32)
    column = lax.rem(owner, replicas)
    in_column = iota((replicas, rows), 0) == column
    late = rank >= direct
    column_f = ones_at(in_column, F32)
    late_f = jnp.where(late, column_f, 0.0)
    column_rank = jnp.sum(
        column_f * dot(late_f.astype(BF16), earlier), axis=0, keepdims=True
    ).astype(jnp.int32)
    in_direct = rank < direct
    in_shared = jnp.logical_and(late, column_rank < shared)
    in_spare = jnp.logical_and(late, column_rank >= shared)
    spare_f = ones_at(in_spare, F32)
    spare_rank = dot(
        jnp.broadcast_to(spare_f, (8, rows)).astype(BF16), earlier
    )[0:1, :].astype(jnp.int32)
    count = jnp.sum(spare_f, axis=1, keepdims=True)

    loads[2].wait()
    values = emb_ref[...].astype(F32)
    unit[...] = (
        values * lax.rsqrt(jnp.sum(values * values, axis=1, keepdims=True) + epsilon)
    ).astype(BF16)

    def picked(number, target):
        return dot(ones_at(iota((number, rows), 0) == target, BF16), unit[...]).astype(BF16)

    own_spare = picked(spare, jnp.where(in_spare, spare_rank, -1))
    got_e[my_group, my_col, my_plane] = own_spare
    packed = picked(replicas * shared, jnp.where(in_shared, column * shared + column_rank, -1))
    send_q[...] = packed.reshape(replicas, shared, width)
    got_q[my_group, my_replica] = send_q[my_replica]

    lane = jnp.where(
        in_direct, rank, jnp.where(in_shared, direct + column_rank, direct + shared + spare_rank)
    )
    place = ones_at(iota((LANES, rows), 0) == lane, BF16)
    near_f = jnp.concatenate([column_f] * groups, axis=0)
    chosen = jnp.where(in_direct, owned_f, jnp.where(in_shared, near_f, 1.0))
    id_high = jnp.floor(ids.astype(F32) * (1.0 / 256.0))
    id_low = ids.astype(F32) - 256.0 * id_high
    used = direct + shared + spare
    three = jnp.concatenate([chosen * id_high, chosen * id_low, chosen], axis=0).astype(BF16)
    table = dot_nt(three, place)
    table = 256.0 * table[0:owners] + table[owners : 2 * owners] + table[2 * owners :] - 1.0
    table = jnp.where(iota((owners, LANES), 1) < used, table, count)
    send_ids[...] = table.reshape(owners, 1, LANES)
    got_ids[me] = send_ids[me]

    pl.semaphore_wait(barrier, owners - 1)
    for dp in range(1, planes):
        e_plane(dp, False).start()
    for dr in range(1, replicas):
        q_out(dr).start()
    for dg, dr in steps:
        pair_out(id_bufs, dg, dr).start()

    target = jnp.where(in_direct, owner * direct + rank, -1)
    block = replicas * direct
    for dg in list(range(1, groups)) + [0]:
        tg = to_group[dg]
        packed = picked(block, target - tg * block)
        send_d[pl.ds(tg * replicas, replicas)] = packed.reshape(replicas, direct, width)
        for dr in range(replicas):
            if dg or dr:
                pair_out(d_bufs, dg, dr).start()
    got_d[me] = send_d[me]

    for dp in range(1, planes):
        e_plane(dp, True).wait_recv()
    for ds in range(1, sides):
        ef_side(ds, False).start()
    ef_col(0, False).start()
    ef_core(0, 0, False).start()
    for dr in range(1, replicas):
        q_in(dr).wait_recv()
    for ds in range(1, sides):
        qf_side(ds, False).start()
    qf_core(0, False).start()

    def forward_sides():
        for ds in range(1, sides):
            ef_side(ds, True).wait_recv()
            ef_col(ds, False).start()
            ef_core(ds, 0, False).start()
        for ds in range(1, sides):
            qf_side(ds, True).wait_recv()
            qf_core(ds, False).start()

    def forward_col(ds):
        ef_col(ds, True).wait_recv()
        ef_core(ds, 1, False).start()

    direct_row, shared_row, spare_row = groups * block, owners * shared, owners * spare
    d_lane, q_lane, e_lane = fold(block, direct), fold(block, shared), fold(replicas * spare, spare)
    e_col = fold(replicas * spare, spare * planes)
    e_source = (e_lane - e_col * planes) * 2 + e_col
    d_slot = iota((1, block), 1) - d_lane * direct
    q_slot = iota((1, block), 1) - q_lane * shared + direct
    e_slot = iota((1, replicas * spare), 1) - e_lane * spare + (direct + shared)
    lane_source = jnp.concatenate([d_lane, q_lane, e_source], axis=1)
    lane_slot = jnp.concatenate([d_slot, q_slot, e_slot], axis=1)
    span = lane_source.shape[1]
    expand = ones_at(iota((LANES, span), 0) == lane_slot, BF16)
    from_source = ones_at(iota((replicas, span), 0) == lane_source, F32)
    key = lane_source * used + lane_slot
    key_col = jnp.sum(
        jnp.where(iota((span, span), 0) == iota((span, span), 1), key, 0), axis=1, keepdims=True
    )
    before = ones_at(key_col < key, BF16)

    def spread_rows(size, offset):
        at = jnp.floor((iota((size, LANES), 0).astype(F32) + 0.5) * (1.0 / offset[0]))
        slot = iota((size, LANES), 0) - at.astype(jnp.int32) * offset[0] + offset[1]
        return ones_at(slot == iota((size, LANES), 1), BF16)

    spread[0:direct_row] = spread_rows(direct_row, (direct, 0))
    spread[direct_row : direct_row + shared_row] = spread_rows(shared_row, (shared, direct))
    spread[direct_row + shared_row :] = spread_rows(spare_row, (spare, direct + shared))

    d_all = fold(direct_row, direct)
    q_all = fold(shared_row, shared)
    e_all = fold(spare_row, spare)
    e_group = fold(spare_row, replicas * spare)
    e_inner = e_all - e_group * replicas
    e_side = fold(spare_row, planes * spare) - e_group * 2
    e_all = e_group * replicas + (e_inner - e_side * planes) * 2 + e_side
    all_source = jnp.concatenate([d_all, q_all, e_all], axis=1)

    def by_source(row, parts):
        held = jnp.where(iota((owners, row.shape[1]), 0) == all_source, row, 0.0)
        upper, lower = parts(held)
        both = dot(jnp.concatenate([upper, lower], axis=0), spread[...])
        return both[0:owners], both[owners:]

    for dg, dr in steps:
        pair_in(id_bufs, dg, dr).wait_recv()
    named = got_ids[...].reshape(owners, LANES)
    over_ref[0, 0] = jnp.where(jnp.max(named[:, used:]) > spare, 1, 0)
    begin = jnp.sum(jnp.where(iota((owners, 1), 0) == me, edges, 0), axis=0, keepdims=True)
    ending = jnp.sum(
        jnp.where(iota((owners, 1), 0) == me + 1, edges, 0), axis=0, keepdims=True
    ) + jnp.where(me == owners - 1, CL_DEV * owners, 0)
    begin, ending = begin.astype(F32), ending.astype(F32)
    mine = jnp.logical_and(named >= begin, named < ending)
    local = jnp.where(mine, named - begin + 1.0, 0.0)
    local_high, local_low = digits(local)
    flat_both = dot(jnp.concatenate([local_high, local_low], axis=0), expand)
    flat_all = 256.0 * flat_both[0:owners] + flat_both[owners:] - 1.0

    seen = jnp.zeros((limit, 1), F32)
    cluster = iota((limit, span), 0)
    wide = replicas * spare
    for sg in range(groups):
        flat = jnp.sum(
            from_source * flat_all[sg * replicas : (sg + 1) * replicas], axis=0, keepdims=True
        )
        mask = ones_at(cluster == flat.astype(jnp.int32), F32)
        mask_b = mask.astype(BF16)
        mask_d[:, sg * block : (sg + 1) * block] = mask_b[:, 0:block]
        mask_q[:, sg * block : (sg + 1) * block] = mask_b[:, block : 2 * block]
        mask_e[:, sg * wide : (sg + 1) * wide] = mask_b[:, 2 * block :]
        ahead = dot(mask_b, before) + seen
        slot = jnp.sum(mask * ahead, axis=0, keepdims=True)
        ranks[:, sg * block : (sg + 1) * block] = slot[:, 0:block]
        at = direct_row + sg * block
        ranks[:, at : at + block] = slot[:, block : 2 * block]
        at = direct_row + shared_row + sg * wide
        ranks[:, at : at + wide] = slot[:, 2 * block :]
        seen = seen + jnp.sum(mask, axis=1, keepdims=True)
        if sg == 1:
            forward_sides()

    upper, lower = by_source(ranks[...], digits)
    send_rank[...] = (256.0 * upper + lower).reshape(owners, 1, LANES)
    got_rank[me] = send_rank[me]
    for dg, dr in steps:
        pair_out(rank_bufs, dg, dr).start()

    for ds in range(sides):
        forward_col(ds)

    for ds in range(sides):
        qf_core(ds, True).wait_recv()
    rows_q = got_q[...].reshape(shared_row, width)
    total[...] = dot(mask_q[...], rows_q)
    for ds in range(sides):
        for dc in range(2):
            ef_core(ds, dc, True).wait_recv()
    rows_e = got_e[...].reshape(spare_row, width)
    total[...] += dot(mask_e[...], rows_e)


    def collect(ref, parts, scale):
        upper, lower = parts(ref[...].reshape(owners, LANES))
        both = dot(jnp.concatenate([upper, lower], axis=0), place)
        return jnp.sum(
            owned_f * (scale * both[0:owners] + both[owners:]), axis=0, keepdims=True
        )


    for dg, dr in steps:
        pair_in(d_bufs, dg, dr).wait_recv()
    rows_d = got_d[...].reshape(direct_row, width)
    sums = total[...] + dot(mask_d[...], rows_d)
    share = 1.0 / jnp.maximum(seen, 1.0)
    norm = share * jnp.sqrt(jnp.sum(sums * sums, axis=1, keepdims=True))
    cent_ref[...] = (sums * (share / jnp.maximum(norm, norm_floor))).astype(BF16)

    def near(mask_ref, begin_at, end_at, block_rows):
        score = dot_nt(cent_ref[...], block_rows)
        return jnp.sum(
            mask_ref[:, begin_at:end_at].astype(F32) * score, axis=0, keepdims=True
        )

    half = spare_row // 2
    nears = jnp.concatenate([
        near(mask_d, 0, direct_row, got_d[...].reshape(direct_row, width)),
        near(mask_q, 0, shared_row, got_q[...].reshape(shared_row, width)),
        near(mask_e, 0, half, got_e[0 : groups // 2].reshape(half, width)),
        near(mask_e, half, spare_row, got_e[groups // 2 :].reshape(half, width)),
    ], axis=1)
    upper, lower = by_source(nears, split)
    send_dist[...] = (upper + lower).reshape(owners, 1, LANES)
    got_dist[me] = send_dist[me]
    for dg, dr in steps:
        pair_out(dist_bufs, dg, dr).start()

    for dg, dr in steps:
        pair_in(rank_bufs, dg, dr).wait_recv()
    rank_ref[...] = collect(got_rank, digits, 256.0).astype(jnp.int32)
    for bufs in (id_bufs, d_bufs, rank_bufs):
        for dg, dr in steps:
            pair_out(bufs, dg, dr).wait_send()
    for dp in range(1, planes):
        e_plane(dp, False).wait_send()
    for dr in range(1, replicas):
        q_out(dr).wait_send()
    for ds in range(1, sides):
        ef_side(ds, False).wait_send()
    for ds in range(1, sides):
        qf_side(ds, False).wait_send()
    for ds in range(sides):
        qf_core(ds, False).wait_send()
        ef_col(ds, False).wait_send()
        for dc in range(2):
            ef_core(ds, dc, False).wait_send()

    for dg, dr in steps:
        pair_in(dist_bufs, dg, dr).wait_recv()
    dist_ref[...] = 1.0 - collect(got_dist, split, 1.0)
    for dg, dr in steps:
        pair_out(dist_bufs, dg, dr).wait_send()


def store_kernel(cent_ref, dist_ref, rank_ref, cent_out, dist_out, rank_out, sems):
    pieces = sems.shape[0] - 2
    size = cent_ref.shape[0] // pieces
    copies = [
        pltpu.make_async_copy(
            cent_ref.at[pl.ds(at * size, size)], cent_out.at[pl.ds(at * size, size)], sems.at[at]
        )
        for at in range(pieces)
    ]
    copies.append(pltpu.make_async_copy(dist_ref, dist_out, sems.at[pieces]))
    copies.append(pltpu.make_async_copy(rank_ref, rank_out, sems.at[pieces + 1]))
    for copy in copies:
        copy.start()
    for copy in copies:
        copy.wait()


def solution(mesh):
    groups, replicas = mesh.shape["grp"], mesh.shape["rep"]
    owners = groups * replicas

    def shards(embeddings, cluster_ids, owner_bounds):
        rows, width = embeddings.shape
        limit = CL_DEV + CL_DEV // 2
        most = -(-(3 * rows // owners) // 16) * 16
        direct, shared, spare = 16, 16, 32
        vmem = pl.BlockSpec(memory_space=pltpu.VMEM)
        scalar = pl.BlockSpec(memory_space=pltpu.SMEM)
        anywhere = pl.BlockSpec(memory_space=pl.ANY)
        outside = pl.BlockSpec(memory_space=pltpu.HBM)
        each = pltpu.SemaphoreType.DMA((owners,))
        ids_row = cluster_ids.reshape(1, rows)
        bounds_row = owner_bounds.reshape(1, owners)
        outs = (
            jax.ShapeDtypeStruct((limit, width), BF16),
            jax.ShapeDtypeStruct((1, rows), F32),
            jax.ShapeDtypeStruct((1, rows), jnp.int32),
            jax.ShapeDtypeStruct((1, 1), jnp.int32),
        )

        def run(number, ids_in, bounds_in):
            small = pltpu.VMEM((owners, 8, LANES), F32)
            near = pltpu.SemaphoreType.DMA((replicas,))
            far = pltpu.SemaphoreType.DMA((groups,))
            return pl.pallas_call(
                functools.partial(kernel, groups, replicas, most, 0),
                out_shape=outs,
                in_specs=[anywhere] * 3,
                out_specs=(vmem, vmem, vmem, scalar),
                scratch_shapes=[
                    pltpu.VMEM((rows, width), BF16),
                    pltpu.VMEM((1, rows), jnp.int32),
                    pltpu.VMEM((1, owners), jnp.int32),
                    pltpu.SemaphoreType.DMA((3,)),
                    pltpu.VMEM((rows, width), BF16),
                    pltpu.VMEM((owners, most, width), BF16),
                    pltpu.VMEM((owners, most, width), BF16),
                    small,
                    small,
                    pltpu.VMEM((groups, limit, replicas * most), BF16),
                    pltpu.VMEM((limit, width), F32),
                    small,
                    small,
                    pltpu.VMEM((groups, replicas, LANES), F32),
                    each, each, each, each, each, each, near, near, far, far,
                ],
                compiler_params=pltpu.CompilerParams(
                    collective_id=number,
                    has_side_effects=True,
                    vmem_limit_bytes=48 * 1024 * 1024,
                ),
            )(embeddings, ids_in, bounds_in)

        def run_fast(number):
            small = pltpu.VMEM((owners, 1, LANES), F32)
            slots = owners * (direct + shared + spare)
            return pl.pallas_call(
                functools.partial(fast_kernel, groups, replicas, direct, shared, spare),
                out_shape=outs + (
                    jax.ShapeDtypeStruct((1, rows), jnp.int32),
                    jax.ShapeDtypeStruct((1, owners), jnp.int32),
                ),
                in_specs=[outside] * 3,
                out_specs=(vmem, vmem, vmem, scalar, vmem, vmem),
                scratch_shapes=[
                    pltpu.VMEM((rows, width), BF16),
                    pltpu.SemaphoreType.DMA((3,)),
                    pltpu.VMEM((rows, width), BF16),
                    pltpu.VMEM((owners, direct, width), BF16),
                    pltpu.VMEM((replicas, shared, width), BF16),
                    pltpu.VMEM((owners, direct, width), BF16),
                    pltpu.VMEM((groups, replicas, shared, width), BF16),
                    pltpu.VMEM((groups, 2, replicas // 2, spare, width), BF16),
                    small, small, small, small, small, small,
                    pltpu.VMEM((limit, owners * direct), BF16),
                    pltpu.VMEM((limit, owners * shared), BF16),
                    pltpu.VMEM((limit, owners * spare), BF16),
                    pltpu.VMEM((limit, width), F32),
                    pltpu.VMEM((1, slots), F32),
                    pltpu.VMEM((slots, LANES), BF16),
                    each, each, each, each, each, each, each, each,
                    pltpu.SemaphoreType.DMA((replicas,)),
                    pltpu.SemaphoreType.DMA((replicas,)),
                    pltpu.SemaphoreType.DMA((groups,)),
                    pltpu.SemaphoreType.DMA((groups,)),
                    pltpu.SemaphoreType.DMA((replicas // 2,)),
                    pltpu.SemaphoreType.DMA((replicas // 2,)),
                    pltpu.SemaphoreType.DMA((2 * groups,)),
                    pltpu.SemaphoreType.DMA((2 * groups,)),
                ],
                compiler_params=pltpu.CompilerParams(
                    collective_id=number,
                    has_side_effects=True,
                    vmem_limit_bytes=48 * 1024 * 1024,
                ),
            )(*(pltpu.with_memory_space_constraint(x, pltpu.HBM) for x in (embeddings, ids_row, bounds_row)))

        whole = groups % 2 == 0 and replicas * direct == LANES and rows // owners <= direct
        if most > 2 * direct and whole:
            first = run_fast(0)
            centroids, distance, rank = lax.cond(
                first[3][0, 0] > 0, lambda: run(1, first[4], first[5])[:3], lambda: first[:3]
            )
        else:
            centroids, distance, rank, _ = run(0, ids_row, bounds_row)
        centroids, distance, rank = pl.pallas_call(
            store_kernel,
            out_shape=outs[:3],
            in_specs=[vmem] * 3,
            out_specs=(anywhere,) * 3,
            scratch_shapes=[pltpu.SemaphoreType.DMA((6,))],
        )(centroids, distance, rank)
        return distance.reshape(rows), rank.reshape(rows), centroids[None]

    placed = (P(("grp", "rep"), None), P(("grp", "rep")), P())
    return jax.shard_map(
        shards,
        mesh=mesh,
        in_specs=placed,
        out_specs=(P(("grp", "rep")), P(("grp", "rep")), P(("grp", "rep"), None, None)),
        check_vma=False,
    )
```

```python
import functools

import jax
import jax.numpy as jnp
from jax import lax
from jax.experimental import pallas as pl
from jax.experimental.pallas import tpu as pltpu
from jax.sharding import PartitionSpec as P

CL_DEV = 384
LANES = 128

epsilon = 1e-06
norm_floor = 0.25
MESH = pl.DeviceIdType.MESH
F32 = jnp.float32
BF16 = jnp.bfloat16
EXACT = lax.Precision.HIGHEST
NT = (((1,), (1,)), ((), ()))


def iota(shape, dim):
    return lax.broadcasted_iota(jnp.int32, shape, dim)


def ones_at(mask, kind):
    return jnp.where(mask, 1.0, 0.0).astype(kind)


def digits_dot(table, place):
    high = jnp.floor(table * (1.0 / 32.0))
    low = table - 32.0 * high
    upper = jnp.dot(high.astype(BF16), place, preferred_element_type=F32)
    lower = jnp.dot(low.astype(BF16), place, preferred_element_type=F32)
    return 32.0 * upper + lower


def kernel(
    groups, replicas, direct, extra,
    emb_in, ids_in, bounds_in,
    cent_ref, dist_ref, rank_ref, over_ref,
    emb_ref, ids_ref, bounds_ref, in_sems,
    unit, send_rows, got_rows, send_ids, got_ids, member, total, ret, got_ret, slot_mat,
    row_send, row_recv, id_send, id_recv, ret_send, ret_recv,
    near_send, near_recv, far_send, far_recv,
):
    my_group = lax.axis_index("grp")
    my_replica = lax.axis_index("rep")
    me = my_group * replicas + my_replica
    owners = groups * replicas
    rows, width = emb_ref.shape
    limit = cent_ref.shape[0]
    slots = direct + extra
    block = replicas * slots
    sent = replicas * direct

    def peer(dg, dr):
        return lax.rem(my_group + dg, groups), lax.rem(my_replica + dr, replicas)

    def source(dg, dr):
        return (
            lax.rem(my_group + groups - dg, groups),
            lax.rem(my_replica + replicas - dr, replicas),
        )

    def every(dg, act):
        def one(dr, carry):
            act(dr)
            return carry

        lax.fori_loop(1 if dg == 0 else 0, replicas, one, 0)

    def copy(src, dst, ssem, rsem, pair, here, there):
        return pltpu.make_async_remote_copy(
            src_ref=src.at[there],
            dst_ref=dst.at[here, pl.ds(0, direct)] if dst is got_rows else dst.at[here],
            send_sem=ssem.at[there],
            recv_sem=rsem.at[here],
            device_id=pair,
            device_id_type=MESH,
        )

    def start(bufs, dg, dr):
        pair = peer(dg, dr)
        copy(*bufs, pair, me, pair[0] * replicas + pair[1]).start()

    def wait_send(bufs, dg, dr):
        pair = peer(dg, dr)
        copy(*bufs, pair, me, pair[0] * replicas + pair[1]).wait_send()

    def wait_recv(bufs, dg, dr):
        pair = source(dg, dr)
        there = pair[0] * replicas + pair[1]
        copy(*bufs, pair, there, there).wait_recv()

    row_bufs = (send_rows, got_rows, row_send, row_recv)
    id_bufs = (send_ids, got_ids, id_send, id_recv)
    ret_bufs = (ret, got_ret, ret_send, ret_recv)
    order = list(range(1, groups)) + [0]

    barrier = pltpu.get_barrier_semaphore()
    for dg in order:
        every(
            dg,
            lambda dr, dg=dg: pl.semaphore_signal(
                barrier, inc=1, device_id=peer(dg, dr), device_id_type=MESH
            ),
        )

    loads = [
        pltpu.make_async_copy(emb_in, emb_ref, in_sems.at[0]),
        pltpu.make_async_copy(ids_in, ids_ref, in_sems.at[1]),
        pltpu.make_async_copy(bounds_in, bounds_ref, in_sems.at[2]),
    ]
    for load in loads:
        load.start()
    for load in loads:
        load.wait()
    ids = ids_ref[...]
    diagonal = iota((owners, owners), 0) == iota((owners, owners), 1)
    edges = jnp.sum(jnp.where(diagonal, bounds_ref[...], 0), axis=1, keepdims=True)
    reached = ones_at(edges <= ids, F32)
    owner = jnp.sum(reached, axis=0, keepdims=True).astype(jnp.int32) - 1
    owned = iota((owners, rows), 0) == owner
    owned_f = ones_at(owned, F32)
    first = jnp.sum(owned_f * edges.astype(F32), axis=0, keepdims=True)
    local = ids.astype(F32) - first
    earlier = ones_at(iota((rows, rows), 0) < iota((rows, rows), 1), BF16)
    prefix = jnp.dot(owned_f.astype(BF16), earlier, preferred_element_type=F32)
    rank = jnp.sum(owned_f * prefix, axis=0, keepdims=True).astype(jnp.int32)
    target = jnp.where(rank < direct, owner * direct + rank, -1)
    spot = rank
    if extra:
        late = ones_at(rank >= direct, F32)
        queue = jnp.dot(
            jnp.broadcast_to(late, (8, rows)).astype(BF16), earlier, preferred_element_type=F32
        )[0:1, :].astype(jnp.int32)
        spot = jnp.where(rank < direct, rank, direct + queue)
    place = ones_at(iota((LANES, rows), 0) == spot, BF16)

    values = emb_ref[...].astype(F32)
    unit[...] = (
        values * lax.rsqrt(jnp.sum(values * values, axis=1, keepdims=True) + epsilon)
    ).astype(BF16)

    def pack(dg):
        tg = lax.rem(my_group + dg, groups)
        pick = ones_at(iota((sent, rows), 0) + tg * sent == target, BF16)
        packed = jnp.dot(pick, unit[...], preferred_element_type=F32).astype(BF16)
        send_rows[pl.ds(tg * replicas, replicas)] = packed.reshape(replicas, direct, width)

    def near_copy(pair, owner_at, dr):
        ref = got_rows.at[owner_at, pl.ds(direct, extra)]
        return pltpu.make_async_remote_copy(
            src_ref=ref, dst_ref=ref, send_sem=near_send.at[dr], recv_sem=near_recv.at[dr],
            device_id=pair, device_id_type=MESH,
        )

    def far_copy(group_at, to_group, dg):
        ref = got_rows.at[pl.ds(group_at * replicas, replicas), pl.ds(direct, extra)]
        return pltpu.make_async_remote_copy(
            src_ref=ref, dst_ref=ref, send_sem=far_send.at[dg], recv_sem=far_recv.at[dg],
            device_id=(to_group, my_replica), device_id_type=MESH,
        )

    if extra:
        pick = ones_at(iota((extra, rows), 0) + direct == spot, BF16)
        got_rows[me, direct:slots] = jnp.dot(
            pick, unit[...], preferred_element_type=F32
        ).astype(BF16)
    pack(order[0])
    pl.semaphore_wait(barrier, owners - 1)
    if extra:
        every(0, lambda dr: near_copy(peer(0, dr), me, dr).start())
    every(order[0], lambda dr: start(row_bufs, order[0], dr))

    high = jnp.floor(local * (1.0 / 32.0))
    low = local - 32.0 * high
    owned_d = jnp.where(rank < direct, owned_f, 0.0)
    upper = lax.dot_general((owned_d * high).astype(BF16), place, NT, preferred_element_type=F32)
    lower = lax.dot_general((owned_d * low).astype(BF16), place, NT, preferred_element_type=F32)
    filled = lax.dot_general(owned_d.astype(BF16), place, NT, preferred_element_type=F32)
    id_table = 32.0 * upper + lower + filled - 1.0
    count = jnp.zeros((1, 1), F32)
    if extra:
        named = jnp.broadcast_to(late * (ids.astype(F32) + 1.0), (8, rows))
        others = lax.dot_general(
            named, place.astype(F32), NT, precision=EXACT, preferred_element_type=F32
        )
        id_table = id_table + others[0:1, :]
        count = jnp.sum(late, axis=1, keepdims=True)
    top = iota((8, LANES), 0) == 0
    for o in range(owners):
        send_ids[o] = jnp.where(top, id_table[o : o + 1, :], count)
    got_ids[me] = send_ids[me]

    for dg in order:
        every(dg, lambda dr, dg=dg: start(id_bufs, dg, dr))
    for dg in order[1:]:
        pack(dg)
        every(dg, lambda dr, dg=dg: start(row_bufs, dg, dr))
    got_rows[me, 0:direct] = send_rows[me]
    if extra:
        def near_wait(dr):
            pair = source(0, dr)
            near_copy(pair, pair[0] * replicas + pair[1], dr).wait_recv()

        every(0, near_wait)
        for dg in order[:-1]:
            far_copy(my_group, lax.rem(my_group + dg, groups), dg).start()

    for dg in order:
        every(dg, lambda dr, dg=dg: wait_recv(id_bufs, dg, dr))
    worst = jnp.max(got_ids[:, 1, :], axis=0, keepdims=True)
    over_ref[0, 0] = jnp.where(jnp.max(worst) > extra, 1, 0)
    begin = jnp.sum(
        jnp.where(iota((owners, 1), 0) == me, edges, 0), axis=0, keepdims=True
    ).astype(F32)
    ending = jnp.sum(
        jnp.where(iota((owners, 1), 0) == me + 1, edges, 0), axis=0, keepdims=True
    ).astype(F32) + jnp.where(me == owners - 1, float(CL_DEV * owners), 0.0)

    lane = iota((1, block), 1)
    quotient = jnp.zeros((1, block), jnp.int32)
    for s in range(1, replicas):
        quotient = quotient + jnp.where(lane >= s * slots, 1, 0)
    remainder = lane - quotient * slots
    spread = iota((LANES, block), 0) == remainder
    spread_b, spread_f = ones_at(spread, BF16), ones_at(spread, F32)
    from_source = ones_at(iota((replicas, block), 0) == quotient, F32)
    before = ones_at(iota((block, block), 0) < iota((block, block), 1), BF16)
    cluster = iota((limit, block), 0)

    seen = jnp.zeros((limit, 1), F32)
    for sg in range(groups):
        table = got_ids[sg * replicas : (sg + 1) * replicas, 0, :]
        if extra:
            mine = jnp.where((table >= begin) & (table < ending), table - begin, -1.0)
            table = jnp.where(iota((replicas, LANES), 1) < direct, table, mine)
        flat = jnp.sum(from_source * digits_dot(table, spread_b), axis=0, keepdims=True)
        mask = ones_at(cluster == flat.astype(jnp.int32), F32)
        mask_b = mask.astype(BF16)
        member[sg] = mask_b
        ahead = jnp.dot(mask_b, before, preferred_element_type=F32) + seen
        slot = jnp.sum(mask * ahead, axis=0, keepdims=True)
        seen = seen + jnp.sum(mask, axis=1, keepdims=True)
        slot_mat[sg] = lax.dot_general(
            from_source * slot, spread_f, NT, precision=EXACT, preferred_element_type=F32
        )
    total[...] = jnp.zeros_like(total)
    for dg in order:
        sg = lax.rem(my_group + groups - dg, groups)
        every(dg, lambda dr, dg=dg: wait_recv(row_bufs, dg, dr))
        if extra and dg:
            far_copy(sg, sg, dg).wait_recv()
        block_rows = got_rows[pl.ds(sg * replicas, replicas)].reshape(block, width)
        total[...] += jnp.dot(member[sg], block_rows, preferred_element_type=F32)

    centroid = total[...] / jnp.maximum(seen, 1.0)
    norm = jnp.sqrt(jnp.sum(centroid * centroid, axis=1, keepdims=True))
    cent_ref[...] = (centroid / jnp.maximum(norm, norm_floor)).astype(BF16)

    for dg in order:
        sg = lax.rem(my_group + groups - dg, groups)
        tg = lax.rem(my_group + groups - dg, groups)
        block_rows = got_rows[pl.ds(sg * replicas, replicas)].reshape(block, width)
        score = lax.dot_general(cent_ref[...], block_rows, NT, preferred_element_type=F32)
        near = jnp.sum(member[sg].astype(F32) * score, axis=0, keepdims=True)
        dist_mat = lax.dot_general(
            from_source * (1.0 - near), spread_f, NT, precision=EXACT, preferred_element_type=F32
        )
        rank_mat = slot_mat[sg]
        for s in range(replicas):
            ret[tg * replicas + s] = jnp.where(top, dist_mat[s : s + 1, :], rank_mat[s : s + 1, :])
        back = (groups - dg) % groups
        every(back, lambda dr, back=back: start(ret_bufs, back, dr))
    got_ret[me] = ret[me]

    place_f = ones_at(iota((LANES, rows), 0) == spot, F32)
    for dg in order:
        every(dg, lambda dr, dg=dg: wait_recv(ret_bufs, dg, dr))
    dist_all = jnp.dot(got_ret[:, 0, :], place_f, precision=EXACT, preferred_element_type=F32)
    rank_all = jnp.dot(got_ret[:, 1, :], place_f, precision=EXACT, preferred_element_type=F32)
    dist_ref[...] = jnp.sum(owned_f * dist_all, axis=0, keepdims=True)
    rank_ref[...] = jnp.sum(owned_f * rank_all, axis=0, keepdims=True).astype(jnp.int32)
    for bufs in (id_bufs, row_bufs, ret_bufs):
        for dg in order:
            every(dg, lambda dr, dg=dg, bufs=bufs: wait_send(bufs, dg, dr))
    if extra:
        every(0, lambda dr: near_copy(peer(0, dr), me, dr).wait_send())
        for dg in order[:-1]:
            far_copy(my_group, lax.rem(my_group + dg, groups), dg).wait_send()


def fold(count, size):
    return jnp.floor((iota((1, count), 1).astype(F32) + 0.5) * (1.0 / size)).astype(jnp.int32)


def split(value):
    upper = value.astype(BF16)
    return upper, (value - upper.astype(F32)).astype(BF16)


def digits(value):
    upper = jnp.floor(value * (1.0 / 256.0))
    return upper.astype(BF16), (value - 256.0 * upper).astype(BF16)


def dot(left, right):
    return jnp.dot(left, right, preferred_element_type=F32)


def dot_nt(left, right):
    return lax.dot_general(left, right, NT, preferred_element_type=F32)


def fast_kernel(
    groups, replicas, direct, shared, spare,
    emb_in, ids_in, bounds_in,
    cent_ref, dist_ref, rank_ref, over_ref, ids_ref, bounds_ref,
    emb_ref, in_sems, over,
    unit, send_d, send_q, got_d, got_q, got_e,
    send_ids, got_ids, send_rank, got_rank, send_dist, got_dist,
    mask_d, mask_q, mask_e, total, ranks, spread,
    d_send, d_recv, id_send, id_recv, rank_send, rank_recv, dist_send, dist_recv,
    q_send, q_recv, qf_send, qf_recv, e_send, e_recv, ef_send, ef_recv,
):
    my_group = lax.axis_index("grp")
    my_replica = lax.axis_index("rep")
    me = my_group * replicas + my_replica
    owners = groups * replicas
    rows, width = emb_ref.shape
    limit = cent_ref.shape[0]
    planes, sides = replicas // 2, groups // 2
    my_plane, my_col = lax.div(my_replica, 2), lax.rem(my_replica, 2)
    my_side, my_core = lax.div(my_group, 2), lax.rem(my_group, 2)

    def turn(at, step, size):
        return lax.rem(at + step, size)

    def back(at, step, size):
        return lax.rem(at + (size - step), size)

    to_group = [turn(my_group, s, groups) for s in range(groups)]
    to_replica = [turn(my_replica, s, replicas) for s in range(replicas)]
    from_group = [back(my_group, s, groups) for s in range(groups)]
    from_replica = [back(my_replica, s, replicas) for s in range(replicas)]
    steps = [
        (dg, dr) for dg in range(groups) for dr in range(replicas) if dg or dr
    ]

    barrier = pltpu.get_barrier_semaphore()
    for dg, dr in steps:
        pl.semaphore_signal(
            barrier, inc=1, device_id=(to_group[dg], to_replica[dr]), device_id_type=MESH
        )

    def remote(src, dst, ssem, rsem, pair):
        return pltpu.make_async_remote_copy(
            src_ref=src, dst_ref=dst, send_sem=ssem, recv_sem=rsem,
            device_id=pair, device_id_type=MESH,
        )

    def pair_out(bufs, dg, dr):
        src, dst, ssem, rsem = bufs
        pair = (to_group[dg], to_replica[dr])
        there = pair[0] * replicas + pair[1]
        return remote(src.at[there], dst.at[me], ssem.at[there], rsem.at[me], pair)

    def pair_in(bufs, dg, dr):
        src, dst, ssem, rsem = bufs
        pair = (from_group[dg], from_replica[dr])
        there = pair[0] * replicas + pair[1]
        return remote(src.at[there], dst.at[there], ssem.at[there], rsem.at[there], pair)

    d_bufs = (send_d, got_d, d_send, d_recv)
    id_bufs = (send_ids, got_ids, id_send, id_recv)
    rank_bufs = (send_rank, got_rank, rank_send, rank_recv)
    dist_bufs = (send_dist, got_dist, dist_send, dist_recv)

    low, half = lax.rem(my_plane, 2), lax.div(my_plane, 2)
    plane_order = [
        my_plane, half * 2 + (1 - low), (1 - half) * 2 + low, (1 - half) * 2 + (1 - low)
    ]

    def d_out(plane, dg, dc):
        pair = (to_group[dg], plane * 2 + lax.rem(my_col + dc, 2))
        there = pair[0] * replicas + pair[1]
        return remote(send_d.at[there], got_d.at[me], d_send.at[there], d_recv.at[me], pair)

    def q_out(dr):
        there = to_replica[dr]
        return remote(
            send_q.at[there], got_q.at[my_group, my_replica],
            q_send.at[dr], q_recv.at[dr], (my_group, there),
        )

    def q_in(dr):
        there = from_replica[dr]
        return remote(
            send_q.at[there], got_q.at[my_group, there],
            q_send.at[dr], q_recv.at[dr], (my_group, there),
        )

    sibling = (my_side * 2 + (1 - my_core), my_replica)

    def side_pair(ds, inward):
        side = back(my_side, ds, sides) if inward else turn(my_side, ds, sides)
        return (side * 2 + my_core, my_replica)

    def qf_side(ds, inward):
        pair = side_pair(ds, inward)
        group = pair[0] if inward else my_group
        ref = got_q.at[group]
        return remote(ref, ref, qf_send.at[ds], qf_recv.at[ds], pair)

    def qf_core(ds, inward):
        group = side_pair(ds, True)[0]
        group = group + (1 - 2 * my_core) if inward else group
        ref = got_q.at[group]
        return remote(ref, ref, qf_send.at[sides + ds], qf_recv.at[sides + ds], sibling)

    def e_plane(dp, inward):
        plane = back(my_plane, dp, planes) if inward else turn(my_plane, dp, planes)
        ref = got_e.at[my_group, my_col, plane if inward else my_plane]
        return remote(
            ref, ref, e_send.at[dp], e_recv.at[dp], (my_group, plane * 2 + my_col)
        )

    def e_spot(ds, dc, inward):
        side = back(my_side, ds, sides) if inward else turn(my_side, ds, sides)
        col = lax.rem(my_col + dc, 2)
        return side * 2 + my_core, col

    def ef_side(ds, inward):
        group = e_spot(ds, 0, inward)[0]
        ref = got_e.at[group if inward else my_group, my_col]
        return remote(
            ref, ref, ef_send.at[2 * ds], ef_recv.at[2 * ds], (group, my_replica)
        )

    def ef_col(ds, inward):
        group = e_spot(ds, 0, True)[0]
        ref = got_e.at[group, 1 - my_col if inward else my_col]
        at = 2 * ds + 1
        return remote(
            ref, ref, ef_send.at[at], ef_recv.at[at],
            (my_group, my_plane * 2 + (1 - my_col)),
        )

    def ef_core(ds, dc, inward):
        group, col = e_spot(ds, dc, True)
        group = group + (1 - 2 * my_core) if inward else group
        ref = got_e.at[group, col]
        at = groups + ds * 2 + dc
        return remote(ref, ref, ef_send.at[at], ef_recv.at[at], sibling)

    loads = [
        pltpu.make_async_copy(ids_in, ids_ref, in_sems.at[0]),
        pltpu.make_async_copy(bounds_in, bounds_ref, in_sems.at[1]),
        pltpu.make_async_copy(emb_in, emb_ref, in_sems.at[2]),
    ]
    for load in loads:
        load.start()
    loads[0].wait()
    loads[1].wait()
    ids = ids_ref[...]
    bounds = bounds_ref[...]
    diagonal = iota((owners, owners), 0) == iota((owners, owners), 1)
    edges = jnp.sum(jnp.where(diagonal, bounds, 0), axis=1, keepdims=True)
    owner = jnp.sum(ones_at(edges <= ids, F32), axis=0, keepdims=True).astype(jnp.int32) - 1
    owned = iota((owners, rows), 0) == owner
    owned_f = ones_at(owned, F32)
    earlier = ones_at(iota((rows, rows), 0) < iota((rows, rows), 1), BF16)
    prefix = dot(owned_f.astype(BF16), earlier)
    rank = jnp.sum(owned_f * prefix, axis=0, keepdims=True).astype(jnp.int32)
    column = lax.rem(owner, replicas)
    in_column = iota((replicas, rows), 0) == column
    late = rank >= direct
    column_f = ones_at(in_column, F32)
    late_f = jnp.where(late, column_f, 0.0)
    column_rank = jnp.sum(
        column_f * dot(late_f.astype(BF16), earlier), axis=0, keepdims=True
    ).astype(jnp.int32)
    in_direct = rank < direct
    in_shared = jnp.logical_and(late, column_rank < shared)
    in_spare = jnp.logical_and(late, column_rank >= shared)
    spare_f = ones_at(in_spare, F32)
    spare_rank = dot(
        jnp.broadcast_to(spare_f, (8, rows)).astype(BF16), earlier
    )[0:1, :].astype(jnp.int32)
    count = jnp.sum(spare_f, axis=1, keepdims=True)

    loads[2].wait()
    values = emb_ref[...].astype(F32)
    unit[...] = (
        values * lax.rsqrt(jnp.sum(values * values, axis=1, keepdims=True) + epsilon)
    ).astype(BF16)

    def picked(number, target):
        return dot(ones_at(iota((number, rows), 0) == target, BF16), unit[...]).astype(BF16)

    own_spare = picked(spare, jnp.where(in_spare, spare_rank, -1))
    got_e[my_group, my_col, my_plane] = own_spare
    packed = picked(replicas * shared, jnp.where(in_shared, column * shared + column_rank, -1))
    send_q[...] = packed.reshape(replicas, shared, width)
    got_q[my_group, my_replica] = send_q[my_replica]

    lane = jnp.where(
        in_direct, rank, jnp.where(in_shared, direct + column_rank, direct + shared + spare_rank)
    )
    place = ones_at(iota((LANES, rows), 0) == lane, BF16)
    near_f = jnp.concatenate([column_f] * groups, axis=0)
    chosen = jnp.where(in_direct, owned_f, jnp.where(in_shared, near_f, 1.0))
    id_high = jnp.floor(ids.astype(F32) * (1.0 / 256.0))
    id_low = ids.astype(F32) - 256.0 * id_high
    used = direct + shared + spare
    three = jnp.concatenate([chosen * id_high, chosen * id_low, chosen], axis=0).astype(BF16)
    table = dot_nt(three, place)
    table = 256.0 * table[0:owners] + table[owners : 2 * owners] + table[2 * owners :] - 1.0
    table = jnp.where(iota((owners, LANES), 1) < used, table, count)
    send_ids[...] = table.reshape(owners, 1, LANES)
    got_ids[me] = send_ids[me]

    target = jnp.where(in_direct, owner * direct + rank, -1)
    block = replicas * direct
    for tg in range(groups):
        packed = picked(block, target - tg * block)
        send_d[tg * replicas : (tg + 1) * replicas] = packed.reshape(replicas, direct, width)
    got_d[me] = send_d[me]

    pl.semaphore_wait(barrier, owners - 1)
    for dp in range(1, planes):
        e_plane(dp, False).start()
    for dr in range(1, replicas):
        q_out(dr).start()
    for dg, dr in steps:
        pair_out(id_bufs, dg, dr).start()

    for plane in plane_order:
        for dg in range(groups):
            for dc in range(2):
                if dg or dc or plane is not my_plane:
                    d_out(plane, dg, dc).start()

    for dp in range(1, planes):
        e_plane(dp, True).wait_recv()
    for ds in range(1, sides):
        ef_side(ds, False).start()
    ef_col(0, False).start()
    ef_core(0, 0, False).start()
    for dr in range(1, replicas):
        q_in(dr).wait_recv()
    for ds in range(1, sides):
        qf_side(ds, False).start()
    qf_core(0, False).start()

    def forward_sides():
        for ds in range(1, sides):
            ef_side(ds, True).wait_recv()
            ef_col(ds, False).start()
            ef_core(ds, 0, False).start()
        for ds in range(1, sides):
            qf_side(ds, True).wait_recv()
            qf_core(ds, False).start()

    def forward_col(ds):
        ef_col(ds, True).wait_recv()
        ef_core(ds, 1, False).start()

    direct_row, shared_row, spare_row = groups * block, owners * shared, owners * spare
    d_lane, q_lane, e_lane = fold(block, direct), fold(block, shared), fold(replicas * spare, spare)
    e_col = fold(replicas * spare, spare * planes)
    e_source = (e_lane - e_col * planes) * 2 + e_col
    d_slot = iota((1, block), 1) - d_lane * direct
    q_slot = iota((1, block), 1) - q_lane * shared + direct
    e_slot = iota((1, replicas * spare), 1) - e_lane * spare + (direct + shared)
    lane_source = jnp.concatenate([d_lane, q_lane, e_source], axis=1)
    lane_slot = jnp.concatenate([d_slot, q_slot, e_slot], axis=1)
    span = lane_source.shape[1]
    expand = ones_at(iota((LANES, span), 0) == lane_slot, BF16)
    from_source = ones_at(iota((replicas, span), 0) == lane_source, F32)
    key = lane_source * used + lane_slot
    key_col = jnp.sum(
        jnp.where(iota((span, span), 0) == iota((span, span), 1), key, 0), axis=1, keepdims=True
    )
    before = ones_at(key_col < key, BF16)

    def spread_rows(size, offset):
        at = jnp.floor((iota((size, LANES), 0).astype(F32) + 0.5) * (1.0 / offset[0]))
        slot = iota((size, LANES), 0) - at.astype(jnp.int32) * offset[0] + offset[1]
        return ones_at(slot == iota((size, LANES), 1), BF16)

    spread[0:direct_row] = spread_rows(direct_row, (direct, 0))
    spread[direct_row : direct_row + shared_row] = spread_rows(shared_row, (shared, direct))
    spread[direct_row + shared_row :] = spread_rows(spare_row, (spare, direct + shared))

    d_all = fold(direct_row, direct)
    q_all = fold(shared_row, shared)
    e_all = fold(spare_row, spare)
    e_group = fold(spare_row, replicas * spare)
    e_inner = e_all - e_group * replicas
    e_side = fold(spare_row, planes * spare) - e_group * 2
    e_all = e_group * replicas + (e_inner - e_side * planes) * 2 + e_side
    all_source = jnp.concatenate([d_all, q_all, e_all], axis=1)

    def by_source(row, parts):
        held = jnp.where(iota((owners, row.shape[1]), 0) == all_source, row, 0.0)
        upper, lower = parts(held)
        both = dot(jnp.concatenate([upper, lower], axis=0), spread[...])
        return both[0:owners], both[owners:]

    for dg, dr in steps:
        pair_in(id_bufs, dg, dr).wait_recv()
    named = got_ids[...].reshape(owners, LANES)
    over[0, 0] = jnp.where(jnp.max(named[:, used:]) > spare, 1, 0)
    flag = pltpu.make_async_copy(over, over_ref, in_sems.at[3])
    flag.start()
    begin = jnp.sum(jnp.where(iota((owners, 1), 0) == me, edges, 0), axis=0, keepdims=True)
    ending = jnp.sum(
        jnp.where(iota((owners, 1), 0) == me + 1, edges, 0), axis=0, keepdims=True
    ) + jnp.where(me == owners - 1, CL_DEV * owners, 0)
    begin, ending = begin.astype(F32), ending.astype(F32)
    mine = jnp.logical_and(named >= begin, named < ending)
    local = jnp.where(mine, named - begin + 1.0, 0.0)
    local_high, local_low = digits(local)
    flat_both = dot(jnp.concatenate([local_high, local_low], axis=0), expand)
    flat_all = 256.0 * flat_both[0:owners] + flat_both[owners:] - 1.0

    seen = jnp.zeros((limit, 1), F32)
    cluster = iota((limit, span), 0)
    wide = replicas * spare
    for sg in range(groups):
        flat = jnp.sum(
            from_source * flat_all[sg * replicas : (sg + 1) * replicas], axis=0, keepdims=True
        )
        mask = ones_at(cluster == flat.astype(jnp.int32), F32)
        mask_b = mask.astype(BF16)
        mask_d[:, sg * block : (sg + 1) * block] = mask_b[:, 0:block]
        mask_q[:, sg * block : (sg + 1) * block] = mask_b[:, block : 2 * block]
        mask_e[:, sg * wide : (sg + 1) * wide] = mask_b[:, 2 * block :]
        ahead = dot(mask_b, before) + seen
        slot = jnp.sum(mask * ahead, axis=0, keepdims=True)
        ranks[:, sg * block : (sg + 1) * block] = slot[:, 0:block]
        at = direct_row + sg * block
        ranks[:, at : at + block] = slot[:, block : 2 * block]
        at = direct_row + shared_row + sg * wide
        ranks[:, at : at + wide] = slot[:, 2 * block :]
        seen = seen + jnp.sum(mask, axis=1, keepdims=True)
        if sg == 1:
            forward_sides()

    upper, lower = by_source(ranks[...], digits)
    send_rank[...] = (256.0 * upper + lower).reshape(owners, 1, LANES)
    got_rank[me] = send_rank[me]
    for dg, dr in steps:
        pair_out(rank_bufs, dg, dr).start()

    for ds in range(sides):
        forward_col(ds)

    for ds in range(sides):
        qf_core(ds, True).wait_recv()
    rows_q = got_q[...].reshape(shared_row, width)
    total[...] = dot(mask_q[...], rows_q)
    for ds in range(sides):
        for dc in range(2):
            ef_core(ds, dc, True).wait_recv()
    rows_e = got_e[...].reshape(spare_row, width)
    total[...] += dot(mask_e[...], rows_e)


    def collect(ref, parts, scale):
        upper, lower = parts(ref[...].reshape(owners, LANES))
        both = dot(jnp.concatenate([upper, lower], axis=0), place)
        return jnp.sum(
            owned_f * (scale * both[0:owners] + both[owners:]), axis=0, keepdims=True
        )


    for dg, dr in steps:
        pair_in(d_bufs, dg, dr).wait_recv()
    rows_d = got_d[...].reshape(direct_row, width)
    sums = total[...] + dot(mask_d[...], rows_d)
    share = 1.0 / jnp.maximum(seen, 1.0)
    norm = share * jnp.sqrt(jnp.sum(sums * sums, axis=1, keepdims=True))
    cent_ref[...] = (sums * (share / jnp.maximum(norm, norm_floor))).astype(BF16)

    def near(mask_ref, begin_at, end_at, block_rows):
        score = dot_nt(cent_ref[...], block_rows)
        return jnp.sum(
            mask_ref[:, begin_at:end_at].astype(F32) * score, axis=0, keepdims=True
        )

    half = spare_row // 2
    nears = jnp.concatenate([
        near(mask_d, 0, direct_row, got_d[...].reshape(direct_row, width)),
        near(mask_q, 0, shared_row, got_q[...].reshape(shared_row, width)),
        near(mask_e, 0, half, got_e[0 : groups // 2].reshape(half, width)),
        near(mask_e, half, spare_row, got_e[groups // 2 :].reshape(half, width)),
    ], axis=1)
    upper, lower = by_source(nears, split)
    send_dist[...] = (upper + lower).reshape(owners, 1, LANES)
    got_dist[me] = send_dist[me]
    for dg, dr in steps:
        pair_out(dist_bufs, dg, dr).start()

    for dg, dr in steps:
        pair_in(rank_bufs, dg, dr).wait_recv()
    rank_ref[...] = collect(got_rank, digits, 256.0).astype(jnp.int32)
    for bufs in (id_bufs, d_bufs, rank_bufs):
        for dg, dr in steps:
            pair_out(bufs, dg, dr).wait_send()
    for dp in range(1, planes):
        e_plane(dp, False).wait_send()
    for dr in range(1, replicas):
        q_out(dr).wait_send()
    for ds in range(1, sides):
        ef_side(ds, False).wait_send()
    for ds in range(1, sides):
        qf_side(ds, False).wait_send()
    for ds in range(sides):
        qf_core(ds, False).wait_send()
        ef_col(ds, False).wait_send()
        for dc in range(2):
            ef_core(ds, dc, False).wait_send()

    for dg, dr in steps:
        pair_in(dist_bufs, dg, dr).wait_recv()
    flag.wait()
    dist_ref[...] = 1.0 - collect(got_dist, split, 1.0)
    for dg, dr in steps:
        pair_out(dist_bufs, dg, dr).wait_send()


def store_kernel(cent_ref, dist_ref, rank_ref, cent_out, dist_out, rank_out, sems):
    pieces = sems.shape[0] - 2
    size = cent_ref.shape[0] // pieces
    copies = [
        pltpu.make_async_copy(
            cent_ref.at[pl.ds(at * size, size)], cent_out.at[pl.ds(at * size, size)], sems.at[at]
        )
        for at in range(pieces)
    ]
    copies.append(pltpu.make_async_copy(dist_ref, dist_out, sems.at[pieces]))
    copies.append(pltpu.make_async_copy(rank_ref, rank_out, sems.at[pieces + 1]))
    for copy in copies:
        copy.start()
    for copy in copies:
        copy.wait()


def solution(mesh):
    groups, replicas = mesh.shape["grp"], mesh.shape["rep"]
    owners = groups * replicas

    def shards(embeddings, cluster_ids, owner_bounds):
        rows, width = embeddings.shape
        limit = CL_DEV + CL_DEV // 2
        most = -(-(3 * rows // owners) // 16) * 16
        direct, shared, spare = 16, 16, 32
        vmem = pl.BlockSpec(memory_space=pltpu.VMEM)
        scalar = pl.BlockSpec(memory_space=pltpu.SMEM)
        anywhere = pl.BlockSpec(memory_space=pl.ANY)
        outside = pl.BlockSpec(memory_space=pltpu.HBM)
        each = pltpu.SemaphoreType.DMA((owners,))
        ids_row = cluster_ids.reshape(1, rows)
        bounds_row = owner_bounds.reshape(1, owners)
        outs = (
            jax.ShapeDtypeStruct((limit, width), BF16),
            jax.ShapeDtypeStruct((1, rows), F32),
            jax.ShapeDtypeStruct((1, rows), jnp.int32),
            jax.ShapeDtypeStruct((1, 1), jnp.int32),
        )

        def run(number, ids_in, bounds_in):
            small = pltpu.VMEM((owners, 8, LANES), F32)
            near = pltpu.SemaphoreType.DMA((replicas,))
            far = pltpu.SemaphoreType.DMA((groups,))
            return pl.pallas_call(
                functools.partial(kernel, groups, replicas, most, 0),
                out_shape=outs,
                in_specs=[anywhere] * 3,
                out_specs=(vmem, vmem, vmem, scalar),
                scratch_shapes=[
                    pltpu.VMEM((rows, width), BF16),
                    pltpu.VMEM((1, rows), jnp.int32),
                    pltpu.VMEM((1, owners), jnp.int32),
                    pltpu.SemaphoreType.DMA((3,)),
                    pltpu.VMEM((rows, width), BF16),
                    pltpu.VMEM((owners, most, width), BF16),
                    pltpu.VMEM((owners, most, width), BF16),
                    small,
                    small,
                    pltpu.VMEM((groups, limit, replicas * most), BF16),
                    pltpu.VMEM((limit, width), F32),
                    small,
                    small,
                    pltpu.VMEM((groups, replicas, LANES), F32),
                    each, each, each, each, each, each, near, near, far, far,
                ],
                compiler_params=pltpu.CompilerParams(
                    collective_id=number,
                    has_side_effects=True,
                    vmem_limit_bytes=48 * 1024 * 1024,
                ),
            )(embeddings, ids_in, bounds_in)

        def run_fast(number):
            small = pltpu.VMEM((owners, 1, LANES), F32)
            slots = owners * (direct + shared + spare)
            return pl.pallas_call(
                functools.partial(fast_kernel, groups, replicas, direct, shared, spare),
                out_shape=outs + (
                    jax.ShapeDtypeStruct((1, rows), jnp.int32),
                    jax.ShapeDtypeStruct((1, owners), jnp.int32),
                ),
                in_specs=[outside] * 3,
                out_specs=(vmem, vmem, vmem, outside, vmem, vmem),
                scratch_shapes=[
                    pltpu.VMEM((rows, width), BF16),
                    pltpu.SemaphoreType.DMA((4,)),
                    pltpu.SMEM((1, 1), jnp.int32),
                    pltpu.VMEM((rows, width), BF16),
                    pltpu.VMEM((owners, direct, width), BF16),
                    pltpu.VMEM((replicas, shared, width), BF16),
                    pltpu.VMEM((owners, direct, width), BF16),
                    pltpu.VMEM((groups, replicas, shared, width), BF16),
                    pltpu.VMEM((groups, 2, replicas // 2, spare, width), BF16),
                    small, small, small, small, small, small,
                    pltpu.VMEM((limit, owners * direct), BF16),
                    pltpu.VMEM((limit, owners * shared), BF16),
                    pltpu.VMEM((limit, owners * spare), BF16),
                    pltpu.VMEM((limit, width), F32),
                    pltpu.VMEM((1, slots), F32),
                    pltpu.VMEM((slots, LANES), BF16),
                    each, each, each, each, each, each, each, each,
                    pltpu.SemaphoreType.DMA((replicas,)),
                    pltpu.SemaphoreType.DMA((replicas,)),
                    pltpu.SemaphoreType.DMA((groups,)),
                    pltpu.SemaphoreType.DMA((groups,)),
                    pltpu.SemaphoreType.DMA((replicas // 2,)),
                    pltpu.SemaphoreType.DMA((replicas // 2,)),
                    pltpu.SemaphoreType.DMA((2 * groups,)),
                    pltpu.SemaphoreType.DMA((2 * groups,)),
                ],
                compiler_params=pltpu.CompilerParams(
                    collective_id=number,
                    has_side_effects=True,
                    vmem_limit_bytes=48 * 1024 * 1024,
                ),
            )(*(pltpu.with_memory_space_constraint(x, pltpu.HBM) for x in (embeddings, ids_row, bounds_row)))

        def stored(results):
            return tuple(
                pl.pallas_call(
                    store_kernel,
                    out_shape=outs[:3],
                    in_specs=[vmem] * 3,
                    out_specs=(anywhere,) * 3,
                    scratch_shapes=[pltpu.SemaphoreType.DMA((6,))],
                    compiler_params=pltpu.CompilerParams(vmem_limit_bytes=4 * 1024 * 1024),
                )(*results[:3])
            )

        whole = groups == 4 and replicas * direct == LANES and rows // owners <= direct
        if most > 2 * direct and whole:
            first = run_fast(0)
            kept = stored(first)
            centroids, distance, rank = lax.cond(
                first[3][0, 0] > 0, lambda: stored(run(1, first[4], first[5])), lambda: kept
            )
        else:
            centroids, distance, rank, _ = run(0, ids_row, bounds_row)
        return distance.reshape(rows), rank.reshape(rows), centroids[None]

    placed = (P(("grp", "rep"), None), P(("grp", "rep")), P())
    return jax.shard_map(
        shards,
        mesh=mesh,
        in_specs=placed,
        out_specs=(P(("grp", "rep")), P(("grp", "rep")), P(("grp", "rep"), None, None)),
        check_vma=False,
    )
```

```python
import functools

import jax
import jax.numpy as jnp
from jax import lax
from jax.experimental import pallas as pl
from jax.experimental.pallas import tpu as pltpu
from jax.sharding import PartitionSpec as P

CL_DEV = 384
LANES = 128

epsilon = 1e-06
norm_floor = 0.25
MESH = pl.DeviceIdType.MESH
F32 = jnp.float32
BF16 = jnp.bfloat16
EXACT = lax.Precision.HIGHEST
NT = (((1,), (1,)), ((), ()))


def iota(shape, dim):
    return lax.broadcasted_iota(jnp.int32, shape, dim)


def ones_at(mask, kind):
    return jnp.where(mask, 1.0, 0.0).astype(kind)


def digits_dot(table, place):
    high = jnp.floor(table * (1.0 / 32.0))
    low = table - 32.0 * high
    upper = jnp.dot(high.astype(BF16), place, preferred_element_type=F32)
    lower = jnp.dot(low.astype(BF16), place, preferred_element_type=F32)
    return 32.0 * upper + lower


def kernel(
    groups, replicas, direct, extra,
    emb_in, ids_in, bounds_in,
    cent_ref, dist_ref, rank_ref, over_ref,
    emb_ref, ids_ref, bounds_ref, in_sems,
    unit, send_rows, got_rows, send_ids, got_ids, member, total, ret, got_ret, slot_mat,
    row_send, row_recv, id_send, id_recv, ret_send, ret_recv,
    near_send, near_recv, far_send, far_recv,
):
    my_group = lax.axis_index("grp")
    my_replica = lax.axis_index("rep")
    me = my_group * replicas + my_replica
    owners = groups * replicas
    rows, width = emb_ref.shape
    limit = cent_ref.shape[0]
    slots = direct + extra
    block = replicas * slots
    sent = replicas * direct

    def peer(dg, dr):
        return lax.rem(my_group + dg, groups), lax.rem(my_replica + dr, replicas)

    def source(dg, dr):
        return (
            lax.rem(my_group + groups - dg, groups),
            lax.rem(my_replica + replicas - dr, replicas),
        )

    def every(dg, act):
        def one(dr, carry):
            act(dr)
            return carry

        lax.fori_loop(1 if dg == 0 else 0, replicas, one, 0)

    def copy(src, dst, ssem, rsem, pair, here, there):
        return pltpu.make_async_remote_copy(
            src_ref=src.at[there],
            dst_ref=dst.at[here, pl.ds(0, direct)] if dst is got_rows else dst.at[here],
            send_sem=ssem.at[there],
            recv_sem=rsem.at[here],
            device_id=pair,
            device_id_type=MESH,
        )

    def start(bufs, dg, dr):
        pair = peer(dg, dr)
        copy(*bufs, pair, me, pair[0] * replicas + pair[1]).start()

    def wait_send(bufs, dg, dr):
        pair = peer(dg, dr)
        copy(*bufs, pair, me, pair[0] * replicas + pair[1]).wait_send()

    def wait_recv(bufs, dg, dr):
        pair = source(dg, dr)
        there = pair[0] * replicas + pair[1]
        copy(*bufs, pair, there, there).wait_recv()

    row_bufs = (send_rows, got_rows, row_send, row_recv)
    id_bufs = (send_ids, got_ids, id_send, id_recv)
    ret_bufs = (ret, got_ret, ret_send, ret_recv)
    order = list(range(1, groups)) + [0]

    barrier = pltpu.get_barrier_semaphore()
    for dg in order:
        every(
            dg,
            lambda dr, dg=dg: pl.semaphore_signal(
                barrier, inc=1, device_id=peer(dg, dr), device_id_type=MESH
            ),
        )

    loads = [
        pltpu.make_async_copy(emb_in, emb_ref, in_sems.at[0]),
        pltpu.make_async_copy(ids_in, ids_ref, in_sems.at[1]),
        pltpu.make_async_copy(bounds_in, bounds_ref, in_sems.at[2]),
    ]
    for load in loads:
        load.start()
    for load in loads:
        load.wait()
    ids = ids_ref[...]
    diagonal = iota((owners, owners), 0) == iota((owners, owners), 1)
    edges = jnp.sum(jnp.where(diagonal, bounds_ref[...], 0), axis=1, keepdims=True)
    reached = ones_at(edges <= ids, F32)
    owner = jnp.sum(reached, axis=0, keepdims=True).astype(jnp.int32) - 1
    owned = iota((owners, rows), 0) == owner
    owned_f = ones_at(owned, F32)
    first = jnp.sum(owned_f * edges.astype(F32), axis=0, keepdims=True)
    local = ids.astype(F32) - first
    earlier = ones_at(iota((rows, rows), 0) < iota((rows, rows), 1), BF16)
    prefix = jnp.dot(owned_f.astype(BF16), earlier, preferred_element_type=F32)
    rank = jnp.sum(owned_f * prefix, axis=0, keepdims=True).astype(jnp.int32)
    target = jnp.where(rank < direct, owner * direct + rank, -1)
    spot = rank
    if extra:
        late = ones_at(rank >= direct, F32)
        queue = jnp.dot(
            jnp.broadcast_to(late, (8, rows)).astype(BF16), earlier, preferred_element_type=F32
        )[0:1, :].astype(jnp.int32)
        spot = jnp.where(rank < direct, rank, direct + queue)
    place = ones_at(iota((LANES, rows), 0) == spot, BF16)

    values = emb_ref[...].astype(F32)
    unit[...] = (
        values * lax.rsqrt(jnp.sum(values * values, axis=1, keepdims=True) + epsilon)
    ).astype(BF16)

    def pack(dg):
        tg = lax.rem(my_group + dg, groups)
        pick = ones_at(iota((sent, rows), 0) + tg * sent == target, BF16)
        packed = jnp.dot(pick, unit[...], preferred_element_type=F32).astype(BF16)
        send_rows[pl.ds(tg * replicas, replicas)] = packed.reshape(replicas, direct, width)

    def near_copy(pair, owner_at, dr):
        ref = got_rows.at[owner_at, pl.ds(direct, extra)]
        return pltpu.make_async_remote_copy(
            src_ref=ref, dst_ref=ref, send_sem=near_send.at[dr], recv_sem=near_recv.at[dr],
            device_id=pair, device_id_type=MESH,
        )

    def far_copy(group_at, to_group, dg):
        ref = got_rows.at[pl.ds(group_at * replicas, replicas), pl.ds(direct, extra)]
        return pltpu.make_async_remote_copy(
            src_ref=ref, dst_ref=ref, send_sem=far_send.at[dg], recv_sem=far_recv.at[dg],
            device_id=(to_group, my_replica), device_id_type=MESH,
        )

    if extra:
        pick = ones_at(iota((extra, rows), 0) + direct == spot, BF16)
        got_rows[me, direct:slots] = jnp.dot(
            pick, unit[...], preferred_element_type=F32
        ).astype(BF16)
    pack(order[0])
    pl.semaphore_wait(barrier, owners - 1)
    if extra:
        every(0, lambda dr: near_copy(peer(0, dr), me, dr).start())
    every(order[0], lambda dr: start(row_bufs, order[0], dr))

    high = jnp.floor(local * (1.0 / 32.0))
    low = local - 32.0 * high
    owned_d = jnp.where(rank < direct, owned_f, 0.0)
    upper = lax.dot_general((owned_d * high).astype(BF16), place, NT, preferred_element_type=F32)
    lower = lax.dot_general((owned_d * low).astype(BF16), place, NT, preferred_element_type=F32)
    filled = lax.dot_general(owned_d.astype(BF16), place, NT, preferred_element_type=F32)
    id_table = 32.0 * upper + lower + filled - 1.0
    count = jnp.zeros((1, 1), F32)
    if extra:
        named = jnp.broadcast_to(late * (ids.astype(F32) + 1.0), (8, rows))
        others = lax.dot_general(
            named, place.astype(F32), NT, precision=EXACT, preferred_element_type=F32
        )
        id_table = id_table + others[0:1, :]
        count = jnp.sum(late, axis=1, keepdims=True)
    top = iota((8, LANES), 0) == 0
    for o in range(owners):
        send_ids[o] = jnp.where(top, id_table[o : o + 1, :], count)
    got_ids[me] = send_ids[me]

    for dg in order:
        every(dg, lambda dr, dg=dg: start(id_bufs, dg, dr))
    for dg in order[1:]:
        pack(dg)
        every(dg, lambda dr, dg=dg: start(row_bufs, dg, dr))
    got_rows[me, 0:direct] = send_rows[me]
    if extra:
        def near_wait(dr):
            pair = source(0, dr)
            near_copy(pair, pair[0] * replicas + pair[1], dr).wait_recv()

        every(0, near_wait)
        for dg in order[:-1]:
            far_copy(my_group, lax.rem(my_group + dg, groups), dg).start()

    for dg in order:
        every(dg, lambda dr, dg=dg: wait_recv(id_bufs, dg, dr))
    worst = jnp.max(got_ids[:, 1, :], axis=0, keepdims=True)
    over_ref[0, 0] = jnp.where(jnp.max(worst) > extra, 1, 0)
    begin = jnp.sum(
        jnp.where(iota((owners, 1), 0) == me, edges, 0), axis=0, keepdims=True
    ).astype(F32)
    ending = jnp.sum(
        jnp.where(iota((owners, 1), 0) == me + 1, edges, 0), axis=0, keepdims=True
    ).astype(F32) + jnp.where(me == owners - 1, float(CL_DEV * owners), 0.0)

    lane = iota((1, block), 1)
    quotient = jnp.zeros((1, block), jnp.int32)
    for s in range(1, replicas):
        quotient = quotient + jnp.where(lane >= s * slots, 1, 0)
    remainder = lane - quotient * slots
    spread = iota((LANES, block), 0) == remainder
    spread_b, spread_f = ones_at(spread, BF16), ones_at(spread, F32)
    from_source = ones_at(iota((replicas, block), 0) == quotient, F32)
    before = ones_at(iota((block, block), 0) < iota((block, block), 1), BF16)
    cluster = iota((limit, block), 0)

    seen = jnp.zeros((limit, 1), F32)
    for sg in range(groups):
        table = got_ids[sg * replicas : (sg + 1) * replicas, 0, :]
        if extra:
            mine = jnp.where((table >= begin) & (table < ending), table - begin, -1.0)
            table = jnp.where(iota((replicas, LANES), 1) < direct, table, mine)
        flat = jnp.sum(from_source * digits_dot(table, spread_b), axis=0, keepdims=True)
        mask = ones_at(cluster == flat.astype(jnp.int32), F32)
        mask_b = mask.astype(BF16)
        member[sg] = mask_b
        ahead = jnp.dot(mask_b, before, preferred_element_type=F32) + seen
        slot = jnp.sum(mask * ahead, axis=0, keepdims=True)
        seen = seen + jnp.sum(mask, axis=1, keepdims=True)
        slot_mat[sg] = lax.dot_general(
            from_source * slot, spread_f, NT, precision=EXACT, preferred_element_type=F32
        )
    total[...] = jnp.zeros_like(total)
    for dg in order:
        sg = lax.rem(my_group + groups - dg, groups)
        every(dg, lambda dr, dg=dg: wait_recv(row_bufs, dg, dr))
        if extra and dg:
            far_copy(sg, sg, dg).wait_recv()
        block_rows = got_rows[pl.ds(sg * replicas, replicas)].reshape(block, width)
        total[...] += jnp.dot(member[sg], block_rows, preferred_element_type=F32)

    centroid = total[...] / jnp.maximum(seen, 1.0)
    norm = jnp.sqrt(jnp.sum(centroid * centroid, axis=1, keepdims=True))
    cent_ref[...] = (centroid / jnp.maximum(norm, norm_floor)).astype(BF16)

    for dg in order:
        sg = lax.rem(my_group + groups - dg, groups)
        tg = lax.rem(my_group + groups - dg, groups)
        block_rows = got_rows[pl.ds(sg * replicas, replicas)].reshape(block, width)
        score = lax.dot_general(cent_ref[...], block_rows, NT, preferred_element_type=F32)
        near = jnp.sum(member[sg].astype(F32) * score, axis=0, keepdims=True)
        dist_mat = lax.dot_general(
            from_source * (1.0 - near), spread_f, NT, precision=EXACT, preferred_element_type=F32
        )
        rank_mat = slot_mat[sg]
        for s in range(replicas):
            ret[tg * replicas + s] = jnp.where(top, dist_mat[s : s + 1, :], rank_mat[s : s + 1, :])
        back = (groups - dg) % groups
        every(back, lambda dr, back=back: start(ret_bufs, back, dr))
    got_ret[me] = ret[me]

    place_f = ones_at(iota((LANES, rows), 0) == spot, F32)
    for dg in order:
        every(dg, lambda dr, dg=dg: wait_recv(ret_bufs, dg, dr))
    dist_all = jnp.dot(got_ret[:, 0, :], place_f, precision=EXACT, preferred_element_type=F32)
    rank_all = jnp.dot(got_ret[:, 1, :], place_f, precision=EXACT, preferred_element_type=F32)
    dist_ref[...] = jnp.sum(owned_f * dist_all, axis=0, keepdims=True)
    rank_ref[...] = jnp.sum(owned_f * rank_all, axis=0, keepdims=True).astype(jnp.int32)
    for bufs in (id_bufs, row_bufs, ret_bufs):
        for dg in order:
            every(dg, lambda dr, dg=dg, bufs=bufs: wait_send(bufs, dg, dr))
    if extra:
        every(0, lambda dr: near_copy(peer(0, dr), me, dr).wait_send())
        for dg in order[:-1]:
            far_copy(my_group, lax.rem(my_group + dg, groups), dg).wait_send()


def fold(count, size):
    return jnp.floor((iota((1, count), 1).astype(F32) + 0.5) * (1.0 / size)).astype(jnp.int32)


def split(value):
    upper = value.astype(BF16)
    return upper, (value - upper.astype(F32)).astype(BF16)


def digits(value):
    upper = jnp.floor(value * (1.0 / 256.0))
    return upper.astype(BF16), (value - 256.0 * upper).astype(BF16)


def dot(left, right):
    return jnp.dot(left, right, preferred_element_type=F32)


def dot_nt(left, right):
    return lax.dot_general(left, right, NT, preferred_element_type=F32)


def fast_kernel(
    groups, replicas, direct, shared, spare,
    emb_in, ids_in, bounds_in,
    cent_ref, dist_ref, rank_ref, over_ref, ids_ref, bounds_ref,
    emb_ref, in_sems, over,
    unit, send_d, send_q, got_d, got_q, got_e,
    send_ids, got_ids, send_rank, got_rank, send_dist, got_dist,
    masks, total, ranks, spread,
    d_send, d_recv, id_send, id_recv, rank_send, rank_recv, dist_send, dist_recv,
    q_send, q_recv, qf_send, qf_recv, e_send, e_recv, ef_send, ef_recv,
):
    my_group = lax.axis_index("grp")
    my_replica = lax.axis_index("rep")
    me = my_group * replicas + my_replica
    owners = groups * replicas
    rows, width = emb_ref.shape
    limit = cent_ref.shape[0]
    planes, sides = replicas // 2, groups // 2
    my_plane, my_col = lax.div(my_replica, 2), lax.rem(my_replica, 2)
    my_side, my_core = lax.div(my_group, 2), lax.rem(my_group, 2)

    def turn(at, step, size):
        return lax.rem(at + step, size)

    def back(at, step, size):
        return lax.rem(at + (size - step), size)

    to_group = [turn(my_group, s, groups) for s in range(groups)]
    to_replica = [turn(my_replica, s, replicas) for s in range(replicas)]
    from_group = [back(my_group, s, groups) for s in range(groups)]
    from_replica = [back(my_replica, s, replicas) for s in range(replicas)]
    steps = [
        (dg, dr) for dg in range(groups) for dr in range(replicas) if dg or dr
    ]

    barrier = pltpu.get_barrier_semaphore()
    for dg, dr in steps:
        pl.semaphore_signal(
            barrier, inc=1, device_id=(to_group[dg], to_replica[dr]), device_id_type=MESH
        )

    def remote(src, dst, ssem, rsem, pair):
        return pltpu.make_async_remote_copy(
            src_ref=src, dst_ref=dst, send_sem=ssem, recv_sem=rsem,
            device_id=pair, device_id_type=MESH,
        )

    def pair_out(bufs, dg, dr):
        src, dst, ssem, rsem = bufs
        pair = (to_group[dg], to_replica[dr])
        there = pair[0] * replicas + pair[1]
        return remote(src.at[there], dst.at[me], ssem.at[there], rsem.at[me], pair)

    def pair_in(bufs, dg, dr):
        src, dst, ssem, rsem = bufs
        pair = (from_group[dg], from_replica[dr])
        there = pair[0] * replicas + pair[1]
        return remote(src.at[there], dst.at[there], ssem.at[there], rsem.at[there], pair)

    id_bufs = (send_ids, got_ids, id_send, id_recv)
    rank_bufs = (send_rank, got_rank, rank_send, rank_recv)

    low, half = lax.rem(my_plane, 2), lax.div(my_plane, 2)
    plane_order = [
        my_plane, half * 2 + (1 - low), (1 - half) * 2 + low, (1 - half) * 2 + (1 - low)
    ]

    def at_plane(plane, dg, dc):
        return to_group[dg], plane * 2 + lax.rem(my_col + dc, 2)

    def d_out(plane, dg, dc):
        pair = at_plane(plane, dg, dc)
        there = pair[0] * replicas + pair[1]
        return remote(
            send_d.at[there], got_d.at[my_group, my_replica],
            d_send.at[there], d_recv.at[me], pair,
        )

    def d_in(dg, dr):
        pair = (from_group[dg], from_replica[dr])
        there = pair[0] * replicas + pair[1]
        return remote(
            send_d.at[there], got_d.at[pair], d_send.at[there], d_recv.at[there], pair
        )

    def dist_out(part, plane, dg, dc):
        pair = at_plane(plane, dg, dc)
        there = pair[0] * replicas + pair[1]
        return remote(
            send_dist.at[part, there], got_dist.at[me],
            dist_send.at[there], dist_recv.at[me], pair,
        )

    def dist_in(dg, dr):
        pair = (from_group[dg], from_replica[dr])
        there = pair[0] * replicas + pair[1]
        return remote(
            send_dist.at[0, there], got_dist.at[there],
            dist_send.at[there], dist_recv.at[there], pair,
        )

    spots = [
        (plane, dg, dc)
        for plane in plane_order
        for dg in range(groups)
        for dc in range(2)
        if dg or dc or plane is not my_plane
    ]

    def q_out(dr):
        there = to_replica[dr]
        return remote(
            send_q.at[there], got_q.at[my_group, my_replica],
            q_send.at[dr], q_recv.at[dr], (my_group, there),
        )

    def q_in(dr):
        there = from_replica[dr]
        return remote(
            send_q.at[there], got_q.at[my_group, there],
            q_send.at[dr], q_recv.at[dr], (my_group, there),
        )

    sibling = (my_side * 2 + (1 - my_core), my_replica)

    def side_pair(ds, inward):
        side = back(my_side, ds, sides) if inward else turn(my_side, ds, sides)
        return (side * 2 + my_core, my_replica)

    def qf_side(ds, inward):
        pair = side_pair(ds, inward)
        group = pair[0] if inward else my_group
        ref = got_q.at[group]
        return remote(ref, ref, qf_send.at[ds], qf_recv.at[ds], pair)

    def qf_core(ds, inward):
        group = side_pair(ds, True)[0]
        group = group + (1 - 2 * my_core) if inward else group
        ref = got_q.at[group]
        return remote(ref, ref, qf_send.at[sides + ds], qf_recv.at[sides + ds], sibling)

    def e_plane(dp, inward):
        plane = back(my_plane, dp, planes) if inward else turn(my_plane, dp, planes)
        ref = got_e.at[my_group, my_col, plane if inward else my_plane]
        return remote(
            ref, ref, e_send.at[dp], e_recv.at[dp], (my_group, plane * 2 + my_col)
        )

    def e_spot(ds, dc, inward):
        side = back(my_side, ds, sides) if inward else turn(my_side, ds, sides)
        col = lax.rem(my_col + dc, 2)
        return side * 2 + my_core, col

    def ef_side(ds, inward):
        group = e_spot(ds, 0, inward)[0]
        ref = got_e.at[group if inward else my_group, my_col]
        return remote(
            ref, ref, ef_send.at[2 * ds], ef_recv.at[2 * ds], (group, my_replica)
        )

    def ef_col(ds, inward):
        group = e_spot(ds, 0, True)[0]
        ref = got_e.at[group, 1 - my_col if inward else my_col]
        at = 2 * ds + 1
        return remote(
            ref, ref, ef_send.at[at], ef_recv.at[at],
            (my_group, my_plane * 2 + (1 - my_col)),
        )

    def ef_core(ds, dc, inward):
        group, col = e_spot(ds, dc, True)
        group = group + (1 - 2 * my_core) if inward else group
        ref = got_e.at[group, col]
        at = groups + ds * 2 + dc
        return remote(ref, ref, ef_send.at[at], ef_recv.at[at], sibling)

    loads = [
        pltpu.make_async_copy(ids_in, ids_ref, in_sems.at[0]),
        pltpu.make_async_copy(bounds_in, bounds_ref, in_sems.at[1]),
        pltpu.make_async_copy(emb_in, emb_ref, in_sems.at[2]),
    ]
    for load in loads:
        load.start()
    loads[0].wait()
    loads[1].wait()
    ids = ids_ref[...]
    bounds = bounds_ref[...]
    diagonal = iota((owners, owners), 0) == iota((owners, owners), 1)
    edges = jnp.sum(jnp.where(diagonal, bounds, 0), axis=1, keepdims=True)
    owner = jnp.sum(ones_at(edges <= ids, F32), axis=0, keepdims=True).astype(jnp.int32) - 1
    owned = iota((owners, rows), 0) == owner
    owned_f = ones_at(owned, F32)
    earlier = ones_at(iota((rows, rows), 0) < iota((rows, rows), 1), BF16)
    prefix = dot(owned_f.astype(BF16), earlier)
    rank = jnp.sum(owned_f * prefix, axis=0, keepdims=True).astype(jnp.int32)
    column = lax.rem(owner, replicas)
    in_column = iota((replicas, rows), 0) == column
    late = rank >= direct
    column_f = ones_at(in_column, F32)
    late_f = jnp.where(late, column_f, 0.0)
    column_rank = jnp.sum(
        column_f * dot(late_f.astype(BF16), earlier), axis=0, keepdims=True
    ).astype(jnp.int32)
    in_direct = rank < direct
    in_shared = jnp.logical_and(late, column_rank < shared)
    in_spare = jnp.logical_and(late, column_rank >= shared)
    spare_f = ones_at(in_spare, F32)
    spare_rank = dot(
        jnp.broadcast_to(spare_f, (8, rows)).astype(BF16), earlier
    )[0:1, :].astype(jnp.int32)
    count = jnp.sum(spare_f, axis=1, keepdims=True)

    loads[2].wait()
    values = emb_ref[...].astype(F32)
    unit[...] = (
        values * lax.rsqrt(jnp.sum(values * values, axis=1, keepdims=True) + epsilon)
    ).astype(BF16)

    def picked(number, target):
        return dot(ones_at(iota((number, rows), 0) == target, BF16), unit[...]).astype(BF16)

    own_spare = picked(spare, jnp.where(in_spare, spare_rank, -1))
    got_e[my_group, my_col, my_plane] = own_spare
    packed = picked(replicas * shared, jnp.where(in_shared, column * shared + column_rank, -1))
    send_q[...] = packed.reshape(replicas, shared, width)
    got_q[my_group, my_replica] = send_q[my_replica]

    lane = jnp.where(
        in_direct, rank, jnp.where(in_shared, direct + column_rank, direct + shared + spare_rank)
    )
    place = ones_at(iota((LANES, rows), 0) == lane, BF16)
    near_f = jnp.concatenate([column_f] * groups, axis=0)
    chosen = jnp.where(in_direct, owned_f, jnp.where(in_shared, near_f, 1.0))
    id_high = jnp.floor(ids.astype(F32) * (1.0 / 256.0))
    id_low = ids.astype(F32) - 256.0 * id_high
    used = direct + shared + spare
    three = jnp.concatenate([chosen * id_high, chosen * id_low, chosen], axis=0).astype(BF16)
    table = dot_nt(three, place)
    table = 256.0 * table[0:owners] + table[owners : 2 * owners] + table[2 * owners :] - 1.0
    table = jnp.where(iota((owners, LANES), 1) < used, table, count)
    send_ids[...] = table.reshape(owners, 1, LANES)
    got_ids[me] = send_ids[me]

    target = jnp.where(in_direct, owner * direct + rank, -1)
    block = replicas * direct
    for tg in range(groups):
        packed = picked(block, target - tg * block)
        send_d[tg * replicas : (tg + 1) * replicas] = packed.reshape(replicas, direct, width)
    got_d[my_group, my_replica] = send_d[me]

    pl.semaphore_wait(barrier, owners - 1)
    for dp in range(1, planes):
        e_plane(dp, False).start()
    for dr in range(1, replicas):
        q_out(dr).start()
    for dg, dr in steps:
        pair_out(id_bufs, dg, dr).start()

    for spot in spots:
        d_out(*spot).start()

    for dp in range(1, planes):
        e_plane(dp, True).wait_recv()
    for ds in range(1, sides):
        ef_side(ds, False).start()
    ef_col(0, False).start()
    ef_core(0, 0, False).start()
    for dr in range(1, replicas):
        q_in(dr).wait_recv()
    for ds in range(1, sides):
        qf_side(ds, False).start()
    qf_core(0, False).start()

    def forward_sides():
        for ds in range(1, sides):
            ef_side(ds, True).wait_recv()
            ef_col(ds, False).start()
            ef_core(ds, 0, False).start()
        for ds in range(1, sides):
            qf_side(ds, True).wait_recv()
            qf_core(ds, False).start()

    def forward_col(ds):
        ef_col(ds, True).wait_recv()
        ef_core(ds, 1, False).start()

    direct_row, shared_row, spare_row = groups * block, owners * shared, owners * spare
    d_lane, q_lane, e_lane = fold(block, direct), fold(block, shared), fold(replicas * spare, spare)
    e_col = fold(replicas * spare, spare * planes)
    e_source = (e_lane - e_col * planes) * 2 + e_col
    d_slot = iota((1, block), 1) - d_lane * direct
    q_slot = iota((1, block), 1) - q_lane * shared + direct
    e_slot = iota((1, replicas * spare), 1) - e_lane * spare + (direct + shared)
    lane_source = jnp.concatenate([d_lane, q_lane, e_source], axis=1)
    lane_slot = jnp.concatenate([d_slot, q_slot, e_slot], axis=1)
    span = lane_source.shape[1]
    expand = ones_at(iota((LANES, span), 0) == lane_slot, BF16)
    from_source = ones_at(iota((replicas, span), 0) == lane_source, F32)
    key = lane_source * used + lane_slot
    key_col = jnp.sum(
        jnp.where(iota((span, span), 0) == iota((span, span), 1), key, 0), axis=1, keepdims=True
    )
    before = ones_at(key_col < key, BF16)

    def spread_rows(size, offset):
        at = jnp.floor((iota((size, LANES), 0).astype(F32) + 0.5) * (1.0 / offset[0]))
        slot = iota((size, LANES), 0) - at.astype(jnp.int32) * offset[0] + offset[1]
        return ones_at(slot == iota((size, LANES), 1), BF16)

    spread[0:direct_row] = spread_rows(direct_row, (direct, 0))
    spread[direct_row : direct_row + shared_row] = spread_rows(shared_row, (shared, direct))
    spread[direct_row + shared_row :] = spread_rows(spare_row, (spare, direct + shared))

    d_all = fold(direct_row, direct)
    q_all = fold(shared_row, shared)
    e_all = fold(spare_row, spare)
    e_group = fold(spare_row, replicas * spare)
    e_inner = e_all - e_group * replicas
    e_side = fold(spare_row, planes * spare) - e_group * 2
    e_all = e_group * replicas + (e_inner - e_side * planes) * 2 + e_side
    all_source = jnp.concatenate([d_all, q_all, e_all], axis=1)

    def by_source(row, parts):
        held = jnp.where(iota((owners, row.shape[1]), 0) == all_source, row, 0.0)
        upper, lower = parts(held)
        both = dot(jnp.concatenate([upper, lower], axis=0), spread[...])
        return both[0:owners], both[owners:]

    for dg, dr in steps:
        pair_in(id_bufs, dg, dr).wait_recv()
    named = got_ids[...].reshape(owners, LANES)
    over[0, 0] = jnp.where(jnp.max(named[:, used:]) > spare, 1, 0)
    flag = pltpu.make_async_copy(over, over_ref, in_sems.at[3])
    flag.start()
    begin = jnp.sum(jnp.where(iota((owners, 1), 0) == me, edges, 0), axis=0, keepdims=True)
    ending = jnp.sum(
        jnp.where(iota((owners, 1), 0) == me + 1, edges, 0), axis=0, keepdims=True
    ) + jnp.where(me == owners - 1, CL_DEV * owners, 0)
    begin, ending = begin.astype(F32), ending.astype(F32)
    mine = jnp.logical_and(named >= begin, named < ending)
    local = jnp.where(mine, named - begin + 1.0, 0.0)
    local_high, local_low = digits(local)
    flat_both = dot(jnp.concatenate([local_high, local_low], axis=0), expand)
    flat_all = 256.0 * flat_both[0:owners] + flat_both[owners:] - 1.0

    each, width_h = replicas // 2, planes // 2
    half_d, half_q, half_e = direct_row // 2, shared_row // 2, spare_row // 2
    hd, hq, he = fold(half_d, direct), fold(half_q, shared), fold(half_e, spare)
    gd, gq = fold(half_d, direct * each), fold(half_q, shared * each)
    ge = fold(half_e, spare * each)
    xe = fold(half_e, spare * width_h)
    base_source = jnp.concatenate([
        gd * replicas + hd - gd * each,
        gq * replicas + hq - gq * each,
        ge * replicas + (he - xe * width_h) * 2 + xe - ge * 2,
    ], axis=1)
    half_slot = jnp.concatenate([
        iota((1, half_d), 1) - hd * direct,
        iota((1, half_q), 1) - hq * shared + direct,
        iota((1, half_e), 1) - he * spare + (direct + shared),
    ], axis=1)
    part_span = half_d + half_q + half_e
    half_expand = ones_at(iota((LANES, part_span), 0) == half_slot, BF16)
    half_both = dot(jnp.concatenate([local_high, local_low], axis=0), half_expand)
    half_flat = 256.0 * half_both[0:owners] + half_both[owners:] - 1.0
    part_half = [1 - half, half]
    part_source = [base_source + at * each for at in part_half]
    for part in range(2):
        chosen_source = iota((owners, part_span), 0) == part_source[part]
        flat = jnp.sum(jnp.where(chosen_source, half_flat, 0.0), axis=0, keepdims=True)
        masks[part] = ones_at(iota((limit, part_span), 0) == flat.astype(jnp.int32), BF16)

    def part_d(part):
        return got_d[:, pl.ds(part_half[part] * each, each)].reshape(half_d, width)

    def part_q(part):
        return got_q[:, pl.ds(part_half[part] * each, each)].reshape(half_q, width)

    def part_e(part):
        return got_e[:, :, pl.ds(part_half[part] * width_h, width_h)].reshape(half_e, width)

    in_d = slice(0, half_d)
    in_q = slice(half_d, half_d + half_q)
    in_e = slice(half_d + half_q, part_span)

    seen = jnp.zeros((limit, 1), F32)
    cluster = iota((limit, span), 0)
    wide = replicas * spare
    for sg in range(groups):
        flat = jnp.sum(
            from_source * flat_all[sg * replicas : (sg + 1) * replicas], axis=0, keepdims=True
        )
        mask = ones_at(cluster == flat.astype(jnp.int32), F32)
        mask_b = mask.astype(BF16)
        ahead = dot(mask_b, before) + seen
        slot = jnp.sum(mask * ahead, axis=0, keepdims=True)
        ranks[:, sg * block : (sg + 1) * block] = slot[:, 0:block]
        at = direct_row + sg * block
        ranks[:, at : at + block] = slot[:, block : 2 * block]
        at = direct_row + shared_row + sg * wide
        ranks[:, at : at + wide] = slot[:, 2 * block :]
        seen = seen + jnp.sum(mask, axis=1, keepdims=True)
        if sg == 1:
            forward_sides()

    upper, lower = by_source(ranks[...], digits)
    send_rank[...] = (256.0 * upper + lower).reshape(owners, 1, LANES)
    got_rank[me] = send_rank[me]
    for dg, dr in steps:
        pair_out(rank_bufs, dg, dr).start()

    for ds in range(sides):
        forward_col(ds)

    for ds in range(sides):
        qf_core(ds, True).wait_recv()
    total[...] = dot(masks[0, :, in_q], part_q(0)) + dot(masks[1, :, in_q], part_q(1))
    for ds in range(sides):
        for dc in range(2):
            ef_core(ds, dc, True).wait_recv()
    for part in range(2):
        total[...] += dot(masks[part, :, in_e], part_e(part))


    def collect(ref, parts, scale):
        upper, lower = parts(ref[...].reshape(owners, LANES))
        both = dot(jnp.concatenate([upper, lower], axis=0), place)
        return jnp.sum(
            owned_f * (scale * both[0:owners] + both[owners:]), axis=0, keepdims=True
        )


    for dg, dr in steps:
        d_in(dg, dr).wait_recv()
    sums = total[...] + dot(masks[0, :, in_d], part_d(0)) + dot(masks[1, :, in_d], part_d(1))
    share = 1.0 / jnp.maximum(seen, 1.0)
    norm = share * jnp.sqrt(jnp.sum(sums * sums, axis=1, keepdims=True))
    cent_ref[...] = (sums * (share / jnp.maximum(norm, norm_floor))).astype(BF16)

    def near(part, inside, block_rows):
        score = dot_nt(cent_ref[...], block_rows)
        return jnp.sum(
            masks[part, :, inside].astype(F32) * score, axis=0, keepdims=True
        )

    half_spread = jnp.concatenate([
        spread[0:half_d],
        spread[direct_row : direct_row + half_q],
        spread[direct_row + shared_row : direct_row + shared_row + half_e],
    ], axis=0)
    for part in range(2):
        nears = jnp.concatenate([
            near(part, in_d, part_d(part)),
            near(part, in_q, part_q(part)),
            near(part, in_e, part_e(part)),
        ], axis=1)
        held = jnp.where(iota((owners, part_span), 0) == part_source[part], nears, 0.0)
        upper, lower = split(held)
        both = dot(jnp.concatenate([upper, lower], axis=0), half_spread)
        send_dist[part] = (both[0:owners] + both[owners:]).reshape(owners, 1, LANES)
        for at, spot in enumerate(spots):
            if (at < len(spots) - 4 * groups) == (part == 1):
                dist_out(part, *spot).start()
    got_dist[me] = send_dist[1, me]

    for dg, dr in steps:
        pair_in(rank_bufs, dg, dr).wait_recv()
    rank_ref[...] = collect(got_rank, digits, 256.0).astype(jnp.int32)
    for bufs in (id_bufs, rank_bufs):
        for dg, dr in steps:
            pair_out(bufs, dg, dr).wait_send()
    for spot in spots:
        d_out(*spot).wait_send()
    for dp in range(1, planes):
        e_plane(dp, False).wait_send()
    for dr in range(1, replicas):
        q_out(dr).wait_send()
    for ds in range(1, sides):
        ef_side(ds, False).wait_send()
    for ds in range(1, sides):
        qf_side(ds, False).wait_send()
    for ds in range(sides):
        qf_core(ds, False).wait_send()
        ef_col(ds, False).wait_send()
        for dc in range(2):
            ef_core(ds, dc, False).wait_send()

    for dg, dr in steps:
        dist_in(dg, dr).wait_recv()
    flag.wait()
    dist_ref[...] = 1.0 - collect(got_dist, split, 1.0)
    for at, spot in enumerate(spots):
        dist_out(1 if at < len(spots) - 4 * groups else 0, *spot).wait_send()


def store_kernel(cent_ref, dist_ref, rank_ref, cent_out, dist_out, rank_out, sems):
    pieces = sems.shape[0] - 2
    size = cent_ref.shape[0] // pieces
    copies = [
        pltpu.make_async_copy(
            cent_ref.at[pl.ds(at * size, size)], cent_out.at[pl.ds(at * size, size)], sems.at[at]
        )
        for at in range(pieces)
    ]
    copies.append(pltpu.make_async_copy(dist_ref, dist_out, sems.at[pieces]))
    copies.append(pltpu.make_async_copy(rank_ref, rank_out, sems.at[pieces + 1]))
    for copy in copies:
        copy.start()
    for copy in copies:
        copy.wait()


def solution(mesh):
    groups, replicas = mesh.shape["grp"], mesh.shape["rep"]
    owners = groups * replicas

    def shards(embeddings, cluster_ids, owner_bounds):
        rows, width = embeddings.shape
        limit = CL_DEV + CL_DEV // 2
        most = -(-(3 * rows // owners) // 16) * 16
        direct, shared, spare = 16, 16, 32
        vmem = pl.BlockSpec(memory_space=pltpu.VMEM)
        scalar = pl.BlockSpec(memory_space=pltpu.SMEM)
        anywhere = pl.BlockSpec(memory_space=pl.ANY)
        outside = pl.BlockSpec(memory_space=pltpu.HBM)
        each = pltpu.SemaphoreType.DMA((owners,))
        ids_row = cluster_ids.reshape(1, rows)
        bounds_row = owner_bounds.reshape(1, owners)
        outs = (
            jax.ShapeDtypeStruct((limit, width), BF16),
            jax.ShapeDtypeStruct((1, rows), F32),
            jax.ShapeDtypeStruct((1, rows), jnp.int32),
            jax.ShapeDtypeStruct((1, 1), jnp.int32),
        )

        def run(number, ids_in, bounds_in):
            small = pltpu.VMEM((owners, 8, LANES), F32)
            near = pltpu.SemaphoreType.DMA((replicas,))
            far = pltpu.SemaphoreType.DMA((groups,))
            return pl.pallas_call(
                functools.partial(kernel, groups, replicas, most, 0),
                out_shape=outs,
                in_specs=[anywhere] * 3,
                out_specs=(vmem, vmem, vmem, scalar),
                scratch_shapes=[
                    pltpu.VMEM((rows, width), BF16),
                    pltpu.VMEM((1, rows), jnp.int32),
                    pltpu.VMEM((1, owners), jnp.int32),
                    pltpu.SemaphoreType.DMA((3,)),
                    pltpu.VMEM((rows, width), BF16),
                    pltpu.VMEM((owners, most, width), BF16),
                    pltpu.VMEM((owners, most, width), BF16),
                    small,
                    small,
                    pltpu.VMEM((groups, limit, replicas * most), BF16),
                    pltpu.VMEM((limit, width), F32),
                    small,
                    small,
                    pltpu.VMEM((groups, replicas, LANES), F32),
                    each, each, each, each, each, each, near, near, far, far,
                ],
                compiler_params=pltpu.CompilerParams(
                    collective_id=number,
                    has_side_effects=True,
                    vmem_limit_bytes=48 * 1024 * 1024,
                ),
            )(embeddings, ids_in, bounds_in)

        def run_fast(number):
            small = pltpu.VMEM((owners, 1, LANES), F32)
            slots = owners * (direct + shared + spare)
            return pl.pallas_call(
                functools.partial(fast_kernel, groups, replicas, direct, shared, spare),
                out_shape=outs + (
                    jax.ShapeDtypeStruct((1, rows), jnp.int32),
                    jax.ShapeDtypeStruct((1, owners), jnp.int32),
                ),
                in_specs=[outside] * 3,
                out_specs=(vmem, vmem, vmem, outside, vmem, vmem),
                scratch_shapes=[
                    pltpu.VMEM((rows, width), BF16),
                    pltpu.SemaphoreType.DMA((4,)),
                    pltpu.SMEM((1, 1), jnp.int32),
                    pltpu.VMEM((rows, width), BF16),
                    pltpu.VMEM((owners, direct, width), BF16),
                    pltpu.VMEM((replicas, shared, width), BF16),
                    pltpu.VMEM((groups, replicas, direct, width), BF16),
                    pltpu.VMEM((groups, replicas, shared, width), BF16),
                    pltpu.VMEM((groups, 2, replicas // 2, spare, width), BF16),
                    small, small, small, small,
                    pltpu.VMEM((2, owners, 1, LANES), F32), small,
                    pltpu.VMEM((2, limit, slots // 2), BF16),
                    pltpu.VMEM((limit, width), F32),
                    pltpu.VMEM((1, slots), F32),
                    pltpu.VMEM((slots, LANES), BF16),
                    each, each, each, each, each, each, each, each,
                    pltpu.SemaphoreType.DMA((replicas,)),
                    pltpu.SemaphoreType.DMA((replicas,)),
                    pltpu.SemaphoreType.DMA((groups,)),
                    pltpu.SemaphoreType.DMA((groups,)),
                    pltpu.SemaphoreType.DMA((replicas // 2,)),
                    pltpu.SemaphoreType.DMA((replicas // 2,)),
                    pltpu.SemaphoreType.DMA((2 * groups,)),
                    pltpu.SemaphoreType.DMA((2 * groups,)),
                ],
                compiler_params=pltpu.CompilerParams(
                    collective_id=number,
                    has_side_effects=True,
                    vmem_limit_bytes=48 * 1024 * 1024,
                ),
            )(*(pltpu.with_memory_space_constraint(x, pltpu.HBM) for x in (embeddings, ids_row, bounds_row)))

        def stored(results):
            return tuple(
                pl.pallas_call(
                    store_kernel,
                    out_shape=outs[:3],
                    in_specs=[vmem] * 3,
                    out_specs=(anywhere,) * 3,
                    scratch_shapes=[pltpu.SemaphoreType.DMA((6,))],
                    compiler_params=pltpu.CompilerParams(vmem_limit_bytes=4 * 1024 * 1024),
                )(*results[:3])
            )

        whole = groups == 4 and replicas * direct == LANES and rows // owners <= direct
        if most > 2 * direct and whole:
            first = run_fast(0)
            kept = stored(first)
            centroids, distance, rank = lax.cond(
                first[3][0, 0] > 0, lambda: stored(run(1, first[4], first[5])), lambda: kept
            )
        else:
            centroids, distance, rank, _ = run(0, ids_row, bounds_row)
        return distance.reshape(rows), rank.reshape(rows), centroids[None]

    placed = (P(("grp", "rep"), None), P(("grp", "rep")), P())
    return jax.shard_map(
        shards,
        mesh=mesh,
        in_specs=placed,
        out_specs=(P(("grp", "rep")), P(("grp", "rep")), P(("grp", "rep"), None, None)),
        check_vma=False,
    )
```

```python
import functools

import jax
import jax.numpy as jnp
from jax import lax
from jax.experimental import pallas as pl
from jax.experimental.pallas import tpu as pltpu
from jax.sharding import PartitionSpec as P

CL_DEV = 384
LANES = 128

epsilon = 1e-06
norm_floor = 0.25
MESH = pl.DeviceIdType.MESH
F32 = jnp.float32
BF16 = jnp.bfloat16
EXACT = lax.Precision.HIGHEST
NT = (((1,), (1,)), ((), ()))


def iota(shape, dim):
    return lax.broadcasted_iota(jnp.int32, shape, dim)


def ones_at(mask, kind):
    return jnp.where(mask, 1.0, 0.0).astype(kind)


def digits_dot(table, place):
    high = jnp.floor(table * (1.0 / 32.0))
    low = table - 32.0 * high
    upper = jnp.dot(high.astype(BF16), place, preferred_element_type=F32)
    lower = jnp.dot(low.astype(BF16), place, preferred_element_type=F32)
    return 32.0 * upper + lower


def kernel(
    groups, replicas, direct, extra,
    emb_in, ids_in, bounds_in,
    cent_ref, dist_ref, rank_ref, over_ref,
    emb_ref, ids_ref, bounds_ref, in_sems,
    unit, send_rows, got_rows, send_ids, got_ids, member, total, ret, got_ret, slot_mat,
    row_send, row_recv, id_send, id_recv, ret_send, ret_recv,
    near_send, near_recv, far_send, far_recv,
):
    my_group = lax.axis_index("grp")
    my_replica = lax.axis_index("rep")
    me = my_group * replicas + my_replica
    owners = groups * replicas
    rows, width = emb_ref.shape
    limit = cent_ref.shape[0]
    slots = direct + extra
    block = replicas * slots
    sent = replicas * direct

    def peer(dg, dr):
        return lax.rem(my_group + dg, groups), lax.rem(my_replica + dr, replicas)

    def source(dg, dr):
        return (
            lax.rem(my_group + groups - dg, groups),
            lax.rem(my_replica + replicas - dr, replicas),
        )

    def every(dg, act):
        def one(dr, carry):
            act(dr)
            return carry

        lax.fori_loop(1 if dg == 0 else 0, replicas, one, 0)

    def copy(src, dst, ssem, rsem, pair, here, there):
        return pltpu.make_async_remote_copy(
            src_ref=src.at[there],
            dst_ref=dst.at[here, pl.ds(0, direct)] if dst is got_rows else dst.at[here],
            send_sem=ssem.at[there],
            recv_sem=rsem.at[here],
            device_id=pair,
            device_id_type=MESH,
        )

    def start(bufs, dg, dr):
        pair = peer(dg, dr)
        copy(*bufs, pair, me, pair[0] * replicas + pair[1]).start()

    def wait_send(bufs, dg, dr):
        pair = peer(dg, dr)
        copy(*bufs, pair, me, pair[0] * replicas + pair[1]).wait_send()

    def wait_recv(bufs, dg, dr):
        pair = source(dg, dr)
        there = pair[0] * replicas + pair[1]
        copy(*bufs, pair, there, there).wait_recv()

    row_bufs = (send_rows, got_rows, row_send, row_recv)
    id_bufs = (send_ids, got_ids, id_send, id_recv)
    ret_bufs = (ret, got_ret, ret_send, ret_recv)
    order = list(range(1, groups)) + [0]

    barrier = pltpu.get_barrier_semaphore()
    for dg in order:
        every(
            dg,
            lambda dr, dg=dg: pl.semaphore_signal(
                barrier, inc=1, device_id=peer(dg, dr), device_id_type=MESH
            ),
        )

    loads = [
        pltpu.make_async_copy(emb_in, emb_ref, in_sems.at[0]),
        pltpu.make_async_copy(ids_in, ids_ref, in_sems.at[1]),
        pltpu.make_async_copy(bounds_in, bounds_ref, in_sems.at[2]),
    ]
    for load in loads:
        load.start()
    for load in loads:
        load.wait()
    ids = ids_ref[...]
    diagonal = iota((owners, owners), 0) == iota((owners, owners), 1)
    edges = jnp.sum(jnp.where(diagonal, bounds_ref[...], 0), axis=1, keepdims=True)
    reached = ones_at(edges <= ids, F32)
    owner = jnp.sum(reached, axis=0, keepdims=True).astype(jnp.int32) - 1
    owned = iota((owners, rows), 0) == owner
    owned_f = ones_at(owned, F32)
    first = jnp.sum(owned_f * edges.astype(F32), axis=0, keepdims=True)
    local = ids.astype(F32) - first
    earlier = ones_at(iota((rows, rows), 0) < iota((rows, rows), 1), BF16)
    prefix = jnp.dot(owned_f.astype(BF16), earlier, preferred_element_type=F32)
    rank = jnp.sum(owned_f * prefix, axis=0, keepdims=True).astype(jnp.int32)
    target = jnp.where(rank < direct, owner * direct + rank, -1)
    spot = rank
    if extra:
        late = ones_at(rank >= direct, F32)
        queue = jnp.dot(
            jnp.broadcast_to(late, (8, rows)).astype(BF16), earlier, preferred_element_type=F32
        )[0:1, :].astype(jnp.int32)
        spot = jnp.where(rank < direct, rank, direct + queue)
    place = ones_at(iota((LANES, rows), 0) == spot, BF16)

    values = emb_ref[...].astype(F32)
    unit[...] = (
        values * lax.rsqrt(jnp.sum(values * values, axis=1, keepdims=True) + epsilon)
    ).astype(BF16)

    def pack(dg):
        tg = lax.rem(my_group + dg, groups)
        pick = ones_at(iota((sent, rows), 0) + tg * sent == target, BF16)
        packed = jnp.dot(pick, unit[...], preferred_element_type=F32).astype(BF16)
        send_rows[pl.ds(tg * replicas, replicas)] = packed.reshape(replicas, direct, width)

    def near_copy(pair, owner_at, dr):
        ref = got_rows.at[owner_at, pl.ds(direct, extra)]
        return pltpu.make_async_remote_copy(
            src_ref=ref, dst_ref=ref, send_sem=near_send.at[dr], recv_sem=near_recv.at[dr],
            device_id=pair, device_id_type=MESH,
        )

    def far_copy(group_at, to_group, dg):
        ref = got_rows.at[pl.ds(group_at * replicas, replicas), pl.ds(direct, extra)]
        return pltpu.make_async_remote_copy(
            src_ref=ref, dst_ref=ref, send_sem=far_send.at[dg], recv_sem=far_recv.at[dg],
            device_id=(to_group, my_replica), device_id_type=MESH,
        )

    if extra:
        pick = ones_at(iota((extra, rows), 0) + direct == spot, BF16)
        got_rows[me, direct:slots] = jnp.dot(
            pick, unit[...], preferred_element_type=F32
        ).astype(BF16)
    pack(order[0])
    pl.semaphore_wait(barrier, owners - 1)
    if extra:
        every(0, lambda dr: near_copy(peer(0, dr), me, dr).start())
    every(order[0], lambda dr: start(row_bufs, order[0], dr))

    high = jnp.floor(local * (1.0 / 32.0))
    low = local - 32.0 * high
    owned_d = jnp.where(rank < direct, owned_f, 0.0)
    upper = lax.dot_general((owned_d * high).astype(BF16), place, NT, preferred_element_type=F32)
    lower = lax.dot_general((owned_d * low).astype(BF16), place, NT, preferred_element_type=F32)
    filled = lax.dot_general(owned_d.astype(BF16), place, NT, preferred_element_type=F32)
    id_table = 32.0 * upper + lower + filled - 1.0
    count = jnp.zeros((1, 1), F32)
    if extra:
        named = jnp.broadcast_to(late * (ids.astype(F32) + 1.0), (8, rows))
        others = lax.dot_general(
            named, place.astype(F32), NT, precision=EXACT, preferred_element_type=F32
        )
        id_table = id_table + others[0:1, :]
        count = jnp.sum(late, axis=1, keepdims=True)
    top = iota((8, LANES), 0) == 0
    for o in range(owners):
        send_ids[o] = jnp.where(top, id_table[o : o + 1, :], count)
    got_ids[me] = send_ids[me]

    for dg in order:
        every(dg, lambda dr, dg=dg: start(id_bufs, dg, dr))
    for dg in order[1:]:
        pack(dg)
        every(dg, lambda dr, dg=dg: start(row_bufs, dg, dr))
    got_rows[me, 0:direct] = send_rows[me]
    if extra:
        def near_wait(dr):
            pair = source(0, dr)
            near_copy(pair, pair[0] * replicas + pair[1], dr).wait_recv()

        every(0, near_wait)
        for dg in order[:-1]:
            far_copy(my_group, lax.rem(my_group + dg, groups), dg).start()

    for dg in order:
        every(dg, lambda dr, dg=dg: wait_recv(id_bufs, dg, dr))
    worst = jnp.max(got_ids[:, 1, :], axis=0, keepdims=True)
    over_ref[0, 0] = jnp.where(jnp.max(worst) > extra, 1, 0)
    begin = jnp.sum(
        jnp.where(iota((owners, 1), 0) == me, edges, 0), axis=0, keepdims=True
    ).astype(F32)
    ending = jnp.sum(
        jnp.where(iota((owners, 1), 0) == me + 1, edges, 0), axis=0, keepdims=True
    ).astype(F32) + jnp.where(me == owners - 1, float(CL_DEV * owners), 0.0)

    lane = iota((1, block), 1)
    quotient = jnp.zeros((1, block), jnp.int32)
    for s in range(1, replicas):
        quotient = quotient + jnp.where(lane >= s * slots, 1, 0)
    remainder = lane - quotient * slots
    spread = iota((LANES, block), 0) == remainder
    spread_b, spread_f = ones_at(spread, BF16), ones_at(spread, F32)
    from_source = ones_at(iota((replicas, block), 0) == quotient, F32)
    before = ones_at(iota((block, block), 0) < iota((block, block), 1), BF16)
    cluster = iota((limit, block), 0)

    seen = jnp.zeros((limit, 1), F32)
    for sg in range(groups):
        table = got_ids[sg * replicas : (sg + 1) * replicas, 0, :]
        if extra:
            mine = jnp.where((table >= begin) & (table < ending), table - begin, -1.0)
            table = jnp.where(iota((replicas, LANES), 1) < direct, table, mine)
        flat = jnp.sum(from_source * digits_dot(table, spread_b), axis=0, keepdims=True)
        mask = ones_at(cluster == flat.astype(jnp.int32), F32)
        mask_b = mask.astype(BF16)
        member[sg] = mask_b
        ahead = jnp.dot(mask_b, before, preferred_element_type=F32) + seen
        slot = jnp.sum(mask * ahead, axis=0, keepdims=True)
        seen = seen + jnp.sum(mask, axis=1, keepdims=True)
        slot_mat[sg] = lax.dot_general(
            from_source * slot, spread_f, NT, precision=EXACT, preferred_element_type=F32
        )
    total[...] = jnp.zeros_like(total)
    for dg in order:
        sg = lax.rem(my_group + groups - dg, groups)
        every(dg, lambda dr, dg=dg: wait_recv(row_bufs, dg, dr))
        if extra and dg:
            far_copy(sg, sg, dg).wait_recv()
        block_rows = got_rows[pl.ds(sg * replicas, replicas)].reshape(block, width)
        total[...] += jnp.dot(member[sg], block_rows, preferred_element_type=F32)

    centroid = total[...] / jnp.maximum(seen, 1.0)
    norm = jnp.sqrt(jnp.sum(centroid * centroid, axis=1, keepdims=True))
    cent_ref[...] = (centroid / jnp.maximum(norm, norm_floor)).astype(BF16)

    for dg in order:
        sg = lax.rem(my_group + groups - dg, groups)
        tg = lax.rem(my_group + groups - dg, groups)
        block_rows = got_rows[pl.ds(sg * replicas, replicas)].reshape(block, width)
        score = lax.dot_general(cent_ref[...], block_rows, NT, preferred_element_type=F32)
        near = jnp.sum(member[sg].astype(F32) * score, axis=0, keepdims=True)
        dist_mat = lax.dot_general(
            from_source * (1.0 - near), spread_f, NT, precision=EXACT, preferred_element_type=F32
        )
        rank_mat = slot_mat[sg]
        for s in range(replicas):
            ret[tg * replicas + s] = jnp.where(top, dist_mat[s : s + 1, :], rank_mat[s : s + 1, :])
        back = (groups - dg) % groups
        every(back, lambda dr, back=back: start(ret_bufs, back, dr))
    got_ret[me] = ret[me]

    place_f = ones_at(iota((LANES, rows), 0) == spot, F32)
    for dg in order:
        every(dg, lambda dr, dg=dg: wait_recv(ret_bufs, dg, dr))
    dist_all = jnp.dot(got_ret[:, 0, :], place_f, precision=EXACT, preferred_element_type=F32)
    rank_all = jnp.dot(got_ret[:, 1, :], place_f, precision=EXACT, preferred_element_type=F32)
    dist_ref[...] = jnp.sum(owned_f * dist_all, axis=0, keepdims=True)
    rank_ref[...] = jnp.sum(owned_f * rank_all, axis=0, keepdims=True).astype(jnp.int32)
    for bufs in (id_bufs, row_bufs, ret_bufs):
        for dg in order:
            every(dg, lambda dr, dg=dg, bufs=bufs: wait_send(bufs, dg, dr))
    if extra:
        every(0, lambda dr: near_copy(peer(0, dr), me, dr).wait_send())
        for dg in order[:-1]:
            far_copy(my_group, lax.rem(my_group + dg, groups), dg).wait_send()


def fold(count, size):
    return jnp.floor((iota((1, count), 1).astype(F32) + 0.5) * (1.0 / size)).astype(jnp.int32)


def split(value):
    upper = value.astype(BF16)
    return upper, (value - upper.astype(F32)).astype(BF16)


def digits(value):
    upper = jnp.floor(value * (1.0 / 256.0))
    return upper.astype(BF16), (value - 256.0 * upper).astype(BF16)


def dot(left, right):
    return jnp.dot(left, right, preferred_element_type=F32)


def dot_nt(left, right):
    return lax.dot_general(left, right, NT, preferred_element_type=F32)


def fast_kernel(
    groups, replicas, direct, shared, spare,
    emb_in, ids_in, bounds_in,
    cent_ref, dist_ref, rank_ref, over_ref, ids_ref, bounds_ref,
    emb_ref, in_sems, over,
    unit, send_d, send_q, got_d, got_q, got_e,
    send_ids, got_ids, send_rank, got_rank, send_dist, got_dist,
    masks, total, ranks, spread,
    d_send, d_recv, id_send, id_recv, rank_send, rank_recv, dist_send, dist_recv,
    q_send, q_recv, qf_send, qf_recv, e_send, e_recv, ef_send, ef_recv,
):
    my_group = lax.axis_index("grp")
    my_replica = lax.axis_index("rep")
    me = my_group * replicas + my_replica
    owners = groups * replicas
    rows, width = emb_ref.shape
    limit = cent_ref.shape[0]
    planes, sides = replicas // 2, groups // 2
    my_plane, my_col = lax.div(my_replica, 2), lax.rem(my_replica, 2)
    my_side, my_core = lax.div(my_group, 2), lax.rem(my_group, 2)

    def turn(at, step, size):
        return lax.rem(at + step, size)

    def back(at, step, size):
        return lax.rem(at + (size - step), size)

    to_group = [turn(my_group, s, groups) for s in range(groups)]
    to_replica = [turn(my_replica, s, replicas) for s in range(replicas)]
    from_group = [back(my_group, s, groups) for s in range(groups)]
    from_replica = [back(my_replica, s, replicas) for s in range(replicas)]
    steps = [
        (dg, dr) for dg in range(groups) for dr in range(replicas) if dg or dr
    ]

    barrier = pltpu.get_barrier_semaphore()
    far_first = sorted(range(replicas), key=lambda dr: -min(dr, replicas - dr))
    greeted = [(dg, dr) for dr in far_first for dg in reversed(range(groups)) if dg or dr]
    for dg, dr in greeted:
        pl.semaphore_signal(
            barrier, inc=1, device_id=(to_group[dg], to_replica[dr]), device_id_type=MESH
        )

    def remote(src, dst, ssem, rsem, pair):
        return pltpu.make_async_remote_copy(
            src_ref=src, dst_ref=dst, send_sem=ssem, recv_sem=rsem,
            device_id=pair, device_id_type=MESH,
        )

    def pair_out(bufs, dg, dr):
        src, dst, ssem, rsem = bufs
        pair = (to_group[dg], to_replica[dr])
        there = pair[0] * replicas + pair[1]
        return remote(src.at[there], dst.at[me], ssem.at[there], rsem.at[me], pair)

    def pair_in(bufs, dg, dr):
        src, dst, ssem, rsem = bufs
        pair = (from_group[dg], from_replica[dr])
        there = pair[0] * replicas + pair[1]
        return remote(src.at[there], dst.at[there], ssem.at[there], rsem.at[there], pair)

    id_bufs = (send_ids, got_ids, id_send, id_recv)
    rank_bufs = (send_rank, got_rank, rank_send, rank_recv)

    low, half = lax.rem(my_plane, 2), lax.div(my_plane, 2)
    plane_order = [
        my_plane, half * 2 + (1 - low), (1 - half) * 2 + low, (1 - half) * 2 + (1 - low)
    ]

    def at_plane(plane, dg, dc):
        return to_group[dg], plane * 2 + lax.rem(my_col + dc, 2)

    def d_out(plane, dg, dc):
        pair = at_plane(plane, dg, dc)
        there = pair[0] * replicas + pair[1]
        return remote(
            send_d.at[there], got_d.at[my_group, my_replica],
            d_send.at[there], d_recv.at[me], pair,
        )

    def d_in(plane, dg, dc):
        pair = at_plane(plane, dg, dc)
        there = pair[0] * replicas + pair[1]
        return remote(
            send_d.at[there], got_d.at[pair], d_send.at[there], d_recv.at[there], pair
        )

    def dist_out(part, plane, dg, dc):
        pair = at_plane(plane, dg, dc)
        there = pair[0] * replicas + pair[1]
        return remote(
            send_dist.at[part, there], got_dist.at[me],
            dist_send.at[there], dist_recv.at[me], pair,
        )

    def dist_in(dg, dr):
        pair = (from_group[dg], from_replica[dr])
        there = pair[0] * replicas + pair[1]
        return remote(
            send_dist.at[0, there], got_dist.at[there],
            dist_send.at[there], dist_recv.at[there], pair,
        )

    spots = [
        (plane, dg, dc)
        for plane in plane_order
        for dg in range(groups)
        for dc in range(2)
        if dg or dc or plane is not my_plane
    ]

    def q_out(dr):
        there = to_replica[dr]
        return remote(
            send_q.at[there], got_q.at[my_group, my_replica],
            q_send.at[dr], q_recv.at[dr], (my_group, there),
        )

    def q_in(dr):
        there = from_replica[dr]
        return remote(
            send_q.at[there], got_q.at[my_group, there],
            q_send.at[dr], q_recv.at[dr], (my_group, there),
        )

    sibling = (my_side * 2 + (1 - my_core), my_replica)

    def side_pair(ds, inward):
        side = back(my_side, ds, sides) if inward else turn(my_side, ds, sides)
        return (side * 2 + my_core, my_replica)

    def qf_side(ds, inward):
        pair = side_pair(ds, inward)
        group = pair[0] if inward else my_group
        ref = got_q.at[group]
        return remote(ref, ref, qf_send.at[ds], qf_recv.at[ds], pair)

    def qf_core(ds, inward):
        group = side_pair(ds, True)[0]
        group = group + (1 - 2 * my_core) if inward else group
        ref = got_q.at[group]
        return remote(ref, ref, qf_send.at[sides + ds], qf_recv.at[sides + ds], sibling)

    def e_plane(dp, inward):
        plane = back(my_plane, dp, planes) if inward else turn(my_plane, dp, planes)
        ref = got_e.at[my_group, my_col, plane if inward else my_plane]
        return remote(
            ref, ref, e_send.at[dp], e_recv.at[dp], (my_group, plane * 2 + my_col)
        )

    def e_spot(ds, dc, inward):
        side = back(my_side, ds, sides) if inward else turn(my_side, ds, sides)
        col = lax.rem(my_col + dc, 2)
        return side * 2 + my_core, col

    def ef_side(ds, inward):
        group = e_spot(ds, 0, inward)[0]
        ref = got_e.at[group if inward else my_group, my_col]
        return remote(
            ref, ref, ef_send.at[2 * ds], ef_recv.at[2 * ds], (group, my_replica)
        )

    def ef_col(ds, inward):
        group = e_spot(ds, 0, True)[0]
        ref = got_e.at[group, 1 - my_col if inward else my_col]
        at = 2 * ds + 1
        return remote(
            ref, ref, ef_send.at[at], ef_recv.at[at],
            (my_group, my_plane * 2 + (1 - my_col)),
        )

    def ef_core(ds, dc, inward):
        group, col = e_spot(ds, dc, True)
        group = group + (1 - 2 * my_core) if inward else group
        ref = got_e.at[group, col]
        at = groups + ds * 2 + dc
        return remote(ref, ref, ef_send.at[at], ef_recv.at[at], sibling)

    loads = [
        pltpu.make_async_copy(ids_in, ids_ref, in_sems.at[0]),
        pltpu.make_async_copy(bounds_in, bounds_ref, in_sems.at[1]),
        pltpu.make_async_copy(emb_in, emb_ref, in_sems.at[2]),
    ]
    for load in loads:
        load.start()
    loads[0].wait()
    loads[1].wait()
    ids = ids_ref[...]
    bounds = bounds_ref[...]
    diagonal = iota((owners, owners), 0) == iota((owners, owners), 1)
    edges = jnp.sum(jnp.where(diagonal, bounds, 0), axis=1, keepdims=True)
    owner = jnp.sum(ones_at(edges <= ids, F32), axis=0, keepdims=True).astype(jnp.int32) - 1
    owned = iota((owners, rows), 0) == owner
    owned_f = ones_at(owned, F32)
    earlier = ones_at(iota((rows, rows), 0) < iota((rows, rows), 1), BF16)
    prefix = dot(owned_f.astype(BF16), earlier)
    rank = jnp.sum(owned_f * prefix, axis=0, keepdims=True).astype(jnp.int32)
    column = lax.rem(owner, replicas)
    in_column = iota((replicas, rows), 0) == column
    late = rank >= direct
    column_f = ones_at(in_column, F32)
    late_f = jnp.where(late, column_f, 0.0)
    column_rank = jnp.sum(
        column_f * dot(late_f.astype(BF16), earlier), axis=0, keepdims=True
    ).astype(jnp.int32)
    in_direct = rank < direct
    in_shared = jnp.logical_and(late, column_rank < shared)
    in_spare = jnp.logical_and(late, column_rank >= shared)
    spare_f = ones_at(in_spare, F32)
    spare_rank = dot(
        jnp.broadcast_to(spare_f, (8, rows)).astype(BF16), earlier
    )[0:1, :].astype(jnp.int32)
    count = jnp.sum(spare_f, axis=1, keepdims=True)

    loads[2].wait()
    values = emb_ref[...].astype(F32)
    unit[...] = (
        values * lax.rsqrt(jnp.sum(values * values, axis=1, keepdims=True) + epsilon)
    ).astype(BF16)

    def picked(number, target):
        return dot(ones_at(iota((number, rows), 0) == target, BF16), unit[...]).astype(BF16)

    own_spare = picked(spare, jnp.where(in_spare, spare_rank, -1))
    got_e[my_group, my_col, my_plane] = own_spare
    packed = picked(replicas * shared, jnp.where(in_shared, column * shared + column_rank, -1))
    send_q[...] = packed.reshape(replicas, shared, width)
    got_q[my_group, my_replica] = send_q[my_replica]

    lane = jnp.where(
        in_direct, rank, jnp.where(in_shared, direct + column_rank, direct + shared + spare_rank)
    )
    place = ones_at(iota((LANES, rows), 0) == lane, BF16)
    near_f = jnp.concatenate([column_f] * groups, axis=0)
    chosen = jnp.where(in_direct, owned_f, jnp.where(in_shared, near_f, 1.0))
    id_high = jnp.floor(ids.astype(F32) * (1.0 / 256.0))
    id_low = ids.astype(F32) - 256.0 * id_high
    used = direct + shared + spare
    three = jnp.concatenate([chosen * id_high, chosen * id_low, chosen], axis=0).astype(BF16)
    table = dot_nt(three, place)
    table = 256.0 * table[0:owners] + table[owners : 2 * owners] + table[2 * owners :] - 1.0
    table = jnp.where(iota((owners, LANES), 1) < used, table, count)
    send_ids[...] = table.reshape(owners, 1, LANES)
    got_ids[me] = send_ids[me]

    target = jnp.where(in_direct, owner * direct + rank, -1)
    block = replicas * direct
    for tg in range(groups):
        packed = picked(block, target - tg * block)
        send_d[tg * replicas : (tg + 1) * replicas] = packed.reshape(replicas, direct, width)
    got_d[my_group, my_replica] = send_d[me]

    pl.semaphore_wait(barrier, owners - 1)
    for dp in range(1, planes):
        e_plane(dp, False).start()
    for dr in range(1, replicas):
        q_out(dr).start()
    for dg, dr in steps:
        pair_out(id_bufs, dg, dr).start()

    for spot in spots:
        d_out(*spot).start()

    for dp in range(1, planes):
        e_plane(dp, True).wait_recv()
    for ds in range(1, sides):
        ef_side(ds, False).start()
    ef_col(0, False).start()
    ef_core(0, 0, False).start()
    for dr in range(1, replicas):
        q_in(dr).wait_recv()
    for ds in range(1, sides):
        qf_side(ds, False).start()
    qf_core(0, False).start()

    def forward_sides():
        for ds in range(1, sides):
            ef_side(ds, True).wait_recv()
            ef_col(ds, False).start()
            ef_core(ds, 0, False).start()
        for ds in range(1, sides):
            qf_side(ds, True).wait_recv()
            qf_core(ds, False).start()

    def forward_col(ds):
        ef_col(ds, True).wait_recv()
        ef_core(ds, 1, False).start()

    direct_row, shared_row, spare_row = groups * block, owners * shared, owners * spare
    d_lane, q_lane, e_lane = fold(block, direct), fold(block, shared), fold(replicas * spare, spare)
    e_col = fold(replicas * spare, spare * planes)
    e_source = (e_lane - e_col * planes) * 2 + e_col
    d_slot = iota((1, block), 1) - d_lane * direct
    q_slot = iota((1, block), 1) - q_lane * shared + direct
    e_slot = iota((1, replicas * spare), 1) - e_lane * spare + (direct + shared)
    lane_source = jnp.concatenate([d_lane, q_lane, e_source], axis=1)
    lane_slot = jnp.concatenate([d_slot, q_slot, e_slot], axis=1)
    span = lane_source.shape[1]
    expand = ones_at(iota((LANES, span), 0) == lane_slot, BF16)
    from_source = ones_at(iota((replicas, span), 0) == lane_source, F32)
    key = lane_source * used + lane_slot
    key_col = jnp.sum(
        jnp.where(iota((span, span), 0) == iota((span, span), 1), key, 0), axis=1, keepdims=True
    )
    before = ones_at(key_col < key, BF16)

    def spread_rows(size, offset):
        at = jnp.floor((iota((size, LANES), 0).astype(F32) + 0.5) * (1.0 / offset[0]))
        slot = iota((size, LANES), 0) - at.astype(jnp.int32) * offset[0] + offset[1]
        return ones_at(slot == iota((size, LANES), 1), BF16)

    spread[0:direct_row] = spread_rows(direct_row, (direct, 0))
    spread[direct_row : direct_row + shared_row] = spread_rows(shared_row, (shared, direct))
    spread[direct_row + shared_row :] = spread_rows(spare_row, (spare, direct + shared))

    d_all = fold(direct_row, direct)
    q_all = fold(shared_row, shared)
    e_all = fold(spare_row, spare)
    e_group = fold(spare_row, replicas * spare)
    e_inner = e_all - e_group * replicas
    e_side = fold(spare_row, planes * spare) - e_group * 2
    e_all = e_group * replicas + (e_inner - e_side * planes) * 2 + e_side
    all_source = jnp.concatenate([d_all, q_all, e_all], axis=1)

    def by_source(row, parts):
        held = jnp.where(iota((owners, row.shape[1]), 0) == all_source, row, 0.0)
        upper, lower = parts(held)
        both = dot(jnp.concatenate([upper, lower], axis=0), spread[...])
        return both[0:owners], both[owners:]

    for dg, dr in steps:
        pair_in(id_bufs, dg, dr).wait_recv()
    named = got_ids[...].reshape(owners, LANES)
    over[0, 0] = jnp.where(jnp.max(named[:, used:]) > spare, 1, 0)
    flag = pltpu.make_async_copy(over, over_ref, in_sems.at[3])
    flag.start()
    begin = jnp.sum(jnp.where(iota((owners, 1), 0) == me, edges, 0), axis=0, keepdims=True)
    ending = jnp.sum(
        jnp.where(iota((owners, 1), 0) == me + 1, edges, 0), axis=0, keepdims=True
    ) + jnp.where(me == owners - 1, CL_DEV * owners, 0)
    begin, ending = begin.astype(F32), ending.astype(F32)
    mine = jnp.logical_and(named >= begin, named < ending)
    local = jnp.where(mine, named - begin + 1.0, 0.0)
    local_high, local_low = digits(local)
    flat_both = dot(jnp.concatenate([local_high, local_low], axis=0), expand)
    flat_all = 256.0 * flat_both[0:owners] + flat_both[owners:] - 1.0

    each, width_h = replicas // 2, planes // 2
    half_d, half_q, half_e = direct_row // 2, shared_row // 2, spare_row // 2
    hd, hq, he = fold(half_d, direct), fold(half_q, shared), fold(half_e, spare)
    gd, gq = fold(half_d, direct * each), fold(half_q, shared * each)
    ge = fold(half_e, spare * each)
    xe = fold(half_e, spare * width_h)
    base_source = jnp.concatenate([
        gd * replicas + hd - gd * each,
        gq * replicas + hq - gq * each,
        ge * replicas + (he - xe * width_h) * 2 + xe - ge * 2,
    ], axis=1)
    half_slot = jnp.concatenate([
        iota((1, half_d), 1) - hd * direct,
        iota((1, half_q), 1) - hq * shared + direct,
        iota((1, half_e), 1) - he * spare + (direct + shared),
    ], axis=1)
    part_span = half_d + half_q + half_e
    half_expand = ones_at(iota((LANES, part_span), 0) == half_slot, BF16)
    half_both = dot(jnp.concatenate([local_high, local_low], axis=0), half_expand)
    half_flat = 256.0 * half_both[0:owners] + half_both[owners:] - 1.0
    part_half = [1 - half, half]
    part_source = [base_source + at * each for at in part_half]
    for part in range(2):
        chosen_source = iota((owners, part_span), 0) == part_source[part]
        flat = jnp.sum(jnp.where(chosen_source, half_flat, 0.0), axis=0, keepdims=True)
        masks[part] = ones_at(iota((limit, part_span), 0) == flat.astype(jnp.int32), BF16)

    def part_d(part):
        return got_d[:, pl.ds(part_half[part] * each, each)].reshape(half_d, width)

    def part_q(part):
        return got_q[:, pl.ds(part_half[part] * each, each)].reshape(half_q, width)

    def part_e(part):
        return got_e[:, :, pl.ds(part_half[part] * width_h, width_h)].reshape(half_e, width)

    in_d = slice(0, half_d)
    in_q = slice(half_d, half_d + half_q)
    in_e = slice(half_d + half_q, part_span)

    seen = jnp.zeros((limit, 1), F32)
    cluster = iota((limit, span), 0)
    wide = replicas * spare
    for sg in range(groups):
        flat = jnp.sum(
            from_source * flat_all[sg * replicas : (sg + 1) * replicas], axis=0, keepdims=True
        )
        mask = ones_at(cluster == flat.astype(jnp.int32), F32)
        mask_b = mask.astype(BF16)
        ahead = dot(mask_b, before) + seen
        slot = jnp.sum(mask * ahead, axis=0, keepdims=True)
        ranks[:, sg * block : (sg + 1) * block] = slot[:, 0:block]
        at = direct_row + sg * block
        ranks[:, at : at + block] = slot[:, block : 2 * block]
        at = direct_row + shared_row + sg * wide
        ranks[:, at : at + wide] = slot[:, 2 * block :]
        seen = seen + jnp.sum(mask, axis=1, keepdims=True)
        if sg == 1:
            forward_sides()

    upper, lower = by_source(ranks[...], digits)
    send_rank[...] = (256.0 * upper + lower).reshape(owners, 1, LANES)
    got_rank[me] = send_rank[me]
    for dg, dr in steps:
        pair_out(rank_bufs, dg, dr).start()

    for ds in range(sides):
        forward_col(ds)

    for ds in range(sides):
        qf_core(ds, True).wait_recv()
    total[...] = dot(masks[0, :, in_q], part_q(0)) + dot(masks[1, :, in_q], part_q(1))
    for ds in range(sides):
        for dc in range(2):
            ef_core(ds, dc, True).wait_recv()
    for part in range(2):
        total[...] += dot(masks[part, :, in_e], part_e(part))


    def collect(ref, parts, scale):
        upper, lower = parts(ref[...].reshape(owners, LANES))
        both = dot(jnp.concatenate([upper, lower], axis=0), place)
        return jnp.sum(
            owned_f * (scale * both[0:owners] + both[owners:]), axis=0, keepdims=True
        )


    close = len(spots) - 4 * groups
    for spot in spots[:close]:
        d_in(*spot).wait_recv()
    total[...] += dot(masks[1, :, in_d], part_d(1))
    for spot in spots[close:]:
        d_in(*spot).wait_recv()
    sums = total[...] + dot(masks[0, :, in_d], part_d(0))
    share = 1.0 / jnp.maximum(seen, 1.0)
    norm = share * jnp.sqrt(jnp.sum(sums * sums, axis=1, keepdims=True))
    cent_ref[...] = (sums * (share / jnp.maximum(norm, norm_floor))).astype(BF16)

    def near(part, inside, block_rows):
        score = dot_nt(cent_ref[...], block_rows)
        return jnp.sum(
            masks[part, :, inside].astype(F32) * score, axis=0, keepdims=True
        )

    half_spread = jnp.concatenate([
        spread[0:half_d],
        spread[direct_row : direct_row + half_q],
        spread[direct_row + shared_row : direct_row + shared_row + half_e],
    ], axis=0)
    for part in range(2):
        nears = jnp.concatenate([
            near(part, in_d, part_d(part)),
            near(part, in_q, part_q(part)),
            near(part, in_e, part_e(part)),
        ], axis=1)
        held = jnp.where(iota((owners, part_span), 0) == part_source[part], nears, 0.0)
        upper, lower = split(held)
        both = dot(jnp.concatenate([upper, lower], axis=0), half_spread)
        send_dist[part] = (both[0:owners] + both[owners:]).reshape(owners, 1, LANES)
        for spot in (spots[:close] if part else spots[close:])[::-1]:
            dist_out(part, *spot).start()
    got_dist[me] = send_dist[1, me]

    for dg, dr in steps:
        pair_in(rank_bufs, dg, dr).wait_recv()
    rank_ref[...] = collect(got_rank, digits, 256.0).astype(jnp.int32)
    for bufs in (id_bufs, rank_bufs):
        for dg, dr in steps:
            pair_out(bufs, dg, dr).wait_send()
    for spot in spots:
        d_out(*spot).wait_send()
    for dp in range(1, planes):
        e_plane(dp, False).wait_send()
    for dr in range(1, replicas):
        q_out(dr).wait_send()
    for ds in range(1, sides):
        ef_side(ds, False).wait_send()
    for ds in range(1, sides):
        qf_side(ds, False).wait_send()
    for ds in range(sides):
        qf_core(ds, False).wait_send()
        ef_col(ds, False).wait_send()
        for dc in range(2):
            ef_core(ds, dc, False).wait_send()

    for dg, dr in steps:
        dist_in(dg, dr).wait_recv()
    flag.wait()
    dist_ref[...] = 1.0 - collect(got_dist, split, 1.0)
    for at, spot in enumerate(spots):
        dist_out(1 if at < len(spots) - 4 * groups else 0, *spot).wait_send()


def store_kernel(cent_ref, dist_ref, rank_ref, cent_out, dist_out, rank_out, sems):
    pieces = sems.shape[0] - 2
    size = cent_ref.shape[0] // pieces
    copies = [
        pltpu.make_async_copy(
            cent_ref.at[pl.ds(at * size, size)], cent_out.at[pl.ds(at * size, size)], sems.at[at]
        )
        for at in range(pieces)
    ]
    copies.append(pltpu.make_async_copy(dist_ref, dist_out, sems.at[pieces]))
    copies.append(pltpu.make_async_copy(rank_ref, rank_out, sems.at[pieces + 1]))
    for copy in copies:
        copy.start()
    for copy in copies:
        copy.wait()


def solution(mesh):
    groups, replicas = mesh.shape["grp"], mesh.shape["rep"]
    owners = groups * replicas

    def shards(embeddings, cluster_ids, owner_bounds):
        rows, width = embeddings.shape
        limit = CL_DEV + CL_DEV // 2
        most = -(-(3 * rows // owners) // 16) * 16
        direct, shared, spare = 16, 16, 32
        vmem = pl.BlockSpec(memory_space=pltpu.VMEM)
        scalar = pl.BlockSpec(memory_space=pltpu.SMEM)
        anywhere = pl.BlockSpec(memory_space=pl.ANY)
        outside = pl.BlockSpec(memory_space=pltpu.HBM)
        each = pltpu.SemaphoreType.DMA((owners,))
        ids_row = cluster_ids.reshape(1, rows)
        bounds_row = owner_bounds.reshape(1, owners)
        outs = (
            jax.ShapeDtypeStruct((limit, width), BF16),
            jax.ShapeDtypeStruct((1, rows), F32),
            jax.ShapeDtypeStruct((1, rows), jnp.int32),
            jax.ShapeDtypeStruct((1, 1), jnp.int32),
        )

        def run(number, ids_in, bounds_in):
            small = pltpu.VMEM((owners, 8, LANES), F32)
            near = pltpu.SemaphoreType.DMA((replicas,))
            far = pltpu.SemaphoreType.DMA((groups,))
            return pl.pallas_call(
                functools.partial(kernel, groups, replicas, most, 0),
                out_shape=outs,
                in_specs=[anywhere] * 3,
                out_specs=(vmem, vmem, vmem, scalar),
                scratch_shapes=[
                    pltpu.VMEM((rows, width), BF16),
                    pltpu.VMEM((1, rows), jnp.int32),
                    pltpu.VMEM((1, owners), jnp.int32),
                    pltpu.SemaphoreType.DMA((3,)),
                    pltpu.VMEM((rows, width), BF16),
                    pltpu.VMEM((owners, most, width), BF16),
                    pltpu.VMEM((owners, most, width), BF16),
                    small,
                    small,
                    pltpu.VMEM((groups, limit, replicas * most), BF16),
                    pltpu.VMEM((limit, width), F32),
                    small,
                    small,
                    pltpu.VMEM((groups, replicas, LANES), F32),
                    each, each, each, each, each, each, near, near, far, far,
                ],
                compiler_params=pltpu.CompilerParams(
                    collective_id=number,
                    has_side_effects=True,
                    vmem_limit_bytes=48 * 1024 * 1024,
                ),
            )(embeddings, ids_in, bounds_in)

        def run_fast(number):
            small = pltpu.VMEM((owners, 1, LANES), F32)
            slots = owners * (direct + shared + spare)
            return pl.pallas_call(
                functools.partial(fast_kernel, groups, replicas, direct, shared, spare),
                out_shape=outs + (
                    jax.ShapeDtypeStruct((1, rows), jnp.int32),
                    jax.ShapeDtypeStruct((1, owners), jnp.int32),
                ),
                in_specs=[outside] * 3,
                out_specs=(vmem, vmem, vmem, outside, vmem, vmem),
                scratch_shapes=[
                    pltpu.VMEM((rows, width), BF16),
                    pltpu.SemaphoreType.DMA((4,)),
                    pltpu.SMEM((1, 1), jnp.int32),
                    pltpu.VMEM((rows, width), BF16),
                    pltpu.VMEM((owners, direct, width), BF16),
                    pltpu.VMEM((replicas, shared, width), BF16),
                    pltpu.VMEM((groups, replicas, direct, width), BF16),
                    pltpu.VMEM((groups, replicas, shared, width), BF16),
                    pltpu.VMEM((groups, 2, replicas // 2, spare, width), BF16),
                    small, small, small, small,
                    pltpu.VMEM((2, owners, 1, LANES), F32), small,
                    pltpu.VMEM((2, limit, slots // 2), BF16),
                    pltpu.VMEM((limit, width), F32),
                    pltpu.VMEM((1, slots), F32),
                    pltpu.VMEM((slots, LANES), BF16),
                    each, each, each, each, each, each, each, each,
                    pltpu.SemaphoreType.DMA((replicas,)),
                    pltpu.SemaphoreType.DMA((replicas,)),
                    pltpu.SemaphoreType.DMA((groups,)),
                    pltpu.SemaphoreType.DMA((groups,)),
                    pltpu.SemaphoreType.DMA((replicas // 2,)),
                    pltpu.SemaphoreType.DMA((replicas // 2,)),
                    pltpu.SemaphoreType.DMA((2 * groups,)),
                    pltpu.SemaphoreType.DMA((2 * groups,)),
                ],
                compiler_params=pltpu.CompilerParams(
                    collective_id=number,
                    has_side_effects=True,
                    vmem_limit_bytes=48 * 1024 * 1024,
                ),
            )(*(pltpu.with_memory_space_constraint(x, pltpu.HBM) for x in (embeddings, ids_row, bounds_row)))

        def stored(results):
            return tuple(
                pl.pallas_call(
                    store_kernel,
                    out_shape=outs[:3],
                    in_specs=[vmem] * 3,
                    out_specs=(anywhere,) * 3,
                    scratch_shapes=[pltpu.SemaphoreType.DMA((6,))],
                    compiler_params=pltpu.CompilerParams(vmem_limit_bytes=4 * 1024 * 1024),
                )(*results[:3])
            )

        whole = groups == 4 and replicas * direct == LANES and rows // owners <= direct
        if most > 2 * direct and whole:
            first = run_fast(0)
            kept = stored(first)
            centroids, distance, rank = lax.cond(
                first[3][0, 0] > 0, lambda: stored(run(1, first[4], first[5])), lambda: kept
            )
        else:
            centroids, distance, rank, _ = run(0, ids_row, bounds_row)
        return distance.reshape(rows), rank.reshape(rows), centroids[None]

    placed = (P(("grp", "rep"), None), P(("grp", "rep")), P())
    return jax.shard_map(
        shards,
        mesh=mesh,
        in_specs=placed,
        out_specs=(P(("grp", "rep")), P(("grp", "rep")), P(("grp", "rep"), None, None)),
        check_vma=False,
    )
```

```python
import functools

import jax
import jax.numpy as jnp
from jax import lax
from jax.experimental import pallas as pl
from jax.experimental.pallas import tpu as pltpu
from jax.sharding import PartitionSpec as P

CL_DEV = 384
LANES = 128

epsilon = 1e-06
norm_floor = 0.25
MESH = pl.DeviceIdType.MESH
F32 = jnp.float32
BF16 = jnp.bfloat16
EXACT = lax.Precision.HIGHEST
NT = (((1,), (1,)), ((), ()))


def iota(shape, dim):
    return lax.broadcasted_iota(jnp.int32, shape, dim)


def ones_at(mask, kind):
    return jnp.where(mask, 1.0, 0.0).astype(kind)


def digits_dot(table, place):
    high = jnp.floor(table * (1.0 / 32.0))
    low = table - 32.0 * high
    upper = jnp.dot(high.astype(BF16), place, preferred_element_type=F32)
    lower = jnp.dot(low.astype(BF16), place, preferred_element_type=F32)
    return 32.0 * upper + lower


def kernel(
    groups, replicas, direct, extra,
    emb_in, ids_in, bounds_in,
    cent_ref, dist_ref, rank_ref, over_ref,
    emb_ref, ids_ref, bounds_ref, in_sems,
    unit, send_rows, got_rows, send_ids, got_ids, member, total, ret, got_ret, slot_mat,
    row_send, row_recv, id_send, id_recv, ret_send, ret_recv,
    near_send, near_recv, far_send, far_recv,
):
    my_group = lax.axis_index("grp")
    my_replica = lax.axis_index("rep")
    me = my_group * replicas + my_replica
    owners = groups * replicas
    rows, width = emb_ref.shape
    limit = cent_ref.shape[0]
    slots = direct + extra
    block = replicas * slots
    sent = replicas * direct

    def peer(dg, dr):
        return lax.rem(my_group + dg, groups), lax.rem(my_replica + dr, replicas)

    def source(dg, dr):
        return (
            lax.rem(my_group + groups - dg, groups),
            lax.rem(my_replica + replicas - dr, replicas),
        )

    def every(dg, act):
        def one(dr, carry):
            act(dr)
            return carry

        lax.fori_loop(1 if dg == 0 else 0, replicas, one, 0)

    def copy(src, dst, ssem, rsem, pair, here, there):
        return pltpu.make_async_remote_copy(
            src_ref=src.at[there],
            dst_ref=dst.at[here, pl.ds(0, direct)] if dst is got_rows else dst.at[here],
            send_sem=ssem.at[there],
            recv_sem=rsem.at[here],
            device_id=pair,
            device_id_type=MESH,
        )

    def start(bufs, dg, dr):
        pair = peer(dg, dr)
        copy(*bufs, pair, me, pair[0] * replicas + pair[1]).start()

    def wait_send(bufs, dg, dr):
        pair = peer(dg, dr)
        copy(*bufs, pair, me, pair[0] * replicas + pair[1]).wait_send()

    def wait_recv(bufs, dg, dr):
        pair = source(dg, dr)
        there = pair[0] * replicas + pair[1]
        copy(*bufs, pair, there, there).wait_recv()

    row_bufs = (send_rows, got_rows, row_send, row_recv)
    id_bufs = (send_ids, got_ids, id_send, id_recv)
    ret_bufs = (ret, got_ret, ret_send, ret_recv)
    order = list(range(1, groups)) + [0]

    barrier = pltpu.get_barrier_semaphore()
    for dg in order:
        every(
            dg,
            lambda dr, dg=dg: pl.semaphore_signal(
                barrier, inc=1, device_id=peer(dg, dr), device_id_type=MESH
            ),
        )

    loads = [
        pltpu.make_async_copy(emb_in, emb_ref, in_sems.at[0]),
        pltpu.make_async_copy(ids_in, ids_ref, in_sems.at[1]),
        pltpu.make_async_copy(bounds_in, bounds_ref, in_sems.at[2]),
    ]
    for load in loads:
        load.start()
    for load in loads:
        load.wait()
    ids = ids_ref[...]
    diagonal = iota((owners, owners), 0) == iota((owners, owners), 1)
    edges = jnp.sum(jnp.where(diagonal, bounds_ref[...], 0), axis=1, keepdims=True)
    reached = ones_at(edges <= ids, F32)
    owner = jnp.sum(reached, axis=0, keepdims=True).astype(jnp.int32) - 1
    owned = iota((owners, rows), 0) == owner
    owned_f = ones_at(owned, F32)
    first = jnp.sum(owned_f * edges.astype(F32), axis=0, keepdims=True)
    local = ids.astype(F32) - first
    earlier = ones_at(iota((rows, rows), 0) < iota((rows, rows), 1), BF16)
    prefix = jnp.dot(owned_f.astype(BF16), earlier, preferred_element_type=F32)
    rank = jnp.sum(owned_f * prefix, axis=0, keepdims=True).astype(jnp.int32)
    target = jnp.where(rank < direct, owner * direct + rank, -1)
    spot = rank
    if extra:
        late = ones_at(rank >= direct, F32)
        queue = jnp.dot(
            jnp.broadcast_to(late, (8, rows)).astype(BF16), earlier, preferred_element_type=F32
        )[0:1, :].astype(jnp.int32)
        spot = jnp.where(rank < direct, rank, direct + queue)
    place = ones_at(iota((LANES, rows), 0) == spot, BF16)

    values = emb_ref[...].astype(F32)
    unit[...] = (
        values * lax.rsqrt(jnp.sum(values * values, axis=1, keepdims=True) + epsilon)
    ).astype(BF16)

    def pack(dg):
        tg = lax.rem(my_group + dg, groups)
        pick = ones_at(iota((sent, rows), 0) + tg * sent == target, BF16)
        packed = jnp.dot(pick, unit[...], preferred_element_type=F32).astype(BF16)
        send_rows[pl.ds(tg * replicas, replicas)] = packed.reshape(replicas, direct, width)

    def near_copy(pair, owner_at, dr):
        ref = got_rows.at[owner_at, pl.ds(direct, extra)]
        return pltpu.make_async_remote_copy(
            src_ref=ref, dst_ref=ref, send_sem=near_send.at[dr], recv_sem=near_recv.at[dr],
            device_id=pair, device_id_type=MESH,
        )

    def far_copy(group_at, to_group, dg):
        ref = got_rows.at[pl.ds(group_at * replicas, replicas), pl.ds(direct, extra)]
        return pltpu.make_async_remote_copy(
            src_ref=ref, dst_ref=ref, send_sem=far_send.at[dg], recv_sem=far_recv.at[dg],
            device_id=(to_group, my_replica), device_id_type=MESH,
        )

    if extra:
        pick = ones_at(iota((extra, rows), 0) + direct == spot, BF16)
        got_rows[me, direct:slots] = jnp.dot(
            pick, unit[...], preferred_element_type=F32
        ).astype(BF16)
    pack(order[0])
    pl.semaphore_wait(barrier, owners - 1)
    if extra:
        every(0, lambda dr: near_copy(peer(0, dr), me, dr).start())
    every(order[0], lambda dr: start(row_bufs, order[0], dr))

    high = jnp.floor(local * (1.0 / 32.0))
    low = local - 32.0 * high
    owned_d = jnp.where(rank < direct, owned_f, 0.0)
    upper = lax.dot_general((owned_d * high).astype(BF16), place, NT, preferred_element_type=F32)
    lower = lax.dot_general((owned_d * low).astype(BF16), place, NT, preferred_element_type=F32)
    filled = lax.dot_general(owned_d.astype(BF16), place, NT, preferred_element_type=F32)
    id_table = 32.0 * upper + lower + filled - 1.0
    count = jnp.zeros((1, 1), F32)
    if extra:
        named = jnp.broadcast_to(late * (ids.astype(F32) + 1.0), (8, rows))
        others = lax.dot_general(
            named, place.astype(F32), NT, precision=EXACT, preferred_element_type=F32
        )
        id_table = id_table + others[0:1, :]
        count = jnp.sum(late, axis=1, keepdims=True)
    top = iota((8, LANES), 0) == 0
    for o in range(owners):
        send_ids[o] = jnp.where(top, id_table[o : o + 1, :], count)
    got_ids[me] = send_ids[me]

    for dg in order:
        every(dg, lambda dr, dg=dg: start(id_bufs, dg, dr))
    for dg in order[1:]:
        pack(dg)
        every(dg, lambda dr, dg=dg: start(row_bufs, dg, dr))
    got_rows[me, 0:direct] = send_rows[me]
    if extra:
        def near_wait(dr):
            pair = source(0, dr)
            near_copy(pair, pair[0] * replicas + pair[1], dr).wait_recv()

        every(0, near_wait)
        for dg in order[:-1]:
            far_copy(my_group, lax.rem(my_group + dg, groups), dg).start()

    for dg in order:
        every(dg, lambda dr, dg=dg: wait_recv(id_bufs, dg, dr))
    worst = jnp.max(got_ids[:, 1, :], axis=0, keepdims=True)
    over_ref[0, 0] = jnp.where(jnp.max(worst) > extra, 1, 0)
    begin = jnp.sum(
        jnp.where(iota((owners, 1), 0) == me, edges, 0), axis=0, keepdims=True
    ).astype(F32)
    ending = jnp.sum(
        jnp.where(iota((owners, 1), 0) == me + 1, edges, 0), axis=0, keepdims=True
    ).astype(F32) + jnp.where(me == owners - 1, float(CL_DEV * owners), 0.0)

    lane = iota((1, block), 1)
    quotient = jnp.zeros((1, block), jnp.int32)
    for s in range(1, replicas):
        quotient = quotient + jnp.where(lane >= s * slots, 1, 0)
    remainder = lane - quotient * slots
    spread = iota((LANES, block), 0) == remainder
    spread_b, spread_f = ones_at(spread, BF16), ones_at(spread, F32)
    from_source = ones_at(iota((replicas, block), 0) == quotient, F32)
    before = ones_at(iota((block, block), 0) < iota((block, block), 1), BF16)
    cluster = iota((limit, block), 0)

    seen = jnp.zeros((limit, 1), F32)
    for sg in range(groups):
        table = got_ids[sg * replicas : (sg + 1) * replicas, 0, :]
        if extra:
            mine = jnp.where((table >= begin) & (table < ending), table - begin, -1.0)
            table = jnp.where(iota((replicas, LANES), 1) < direct, table, mine)
        flat = jnp.sum(from_source * digits_dot(table, spread_b), axis=0, keepdims=True)
        mask = ones_at(cluster == flat.astype(jnp.int32), F32)
        mask_b = mask.astype(BF16)
        member[sg] = mask_b
        ahead = jnp.dot(mask_b, before, preferred_element_type=F32) + seen
        slot = jnp.sum(mask * ahead, axis=0, keepdims=True)
        seen = seen + jnp.sum(mask, axis=1, keepdims=True)
        slot_mat[sg] = lax.dot_general(
            from_source * slot, spread_f, NT, precision=EXACT, preferred_element_type=F32
        )
    total[...] = jnp.zeros_like(total)
    for dg in order:
        sg = lax.rem(my_group + groups - dg, groups)
        every(dg, lambda dr, dg=dg: wait_recv(row_bufs, dg, dr))
        if extra and dg:
            far_copy(sg, sg, dg).wait_recv()
        block_rows = got_rows[pl.ds(sg * replicas, replicas)].reshape(block, width)
        total[...] += jnp.dot(member[sg], block_rows, preferred_element_type=F32)

    centroid = total[...] / jnp.maximum(seen, 1.0)
    norm = jnp.sqrt(jnp.sum(centroid * centroid, axis=1, keepdims=True))
    cent_ref[...] = (centroid / jnp.maximum(norm, norm_floor)).astype(BF16)

    for dg in order:
        sg = lax.rem(my_group + groups - dg, groups)
        tg = lax.rem(my_group + groups - dg, groups)
        block_rows = got_rows[pl.ds(sg * replicas, replicas)].reshape(block, width)
        score = lax.dot_general(cent_ref[...], block_rows, NT, preferred_element_type=F32)
        near = jnp.sum(member[sg].astype(F32) * score, axis=0, keepdims=True)
        dist_mat = lax.dot_general(
            from_source * (1.0 - near), spread_f, NT, precision=EXACT, preferred_element_type=F32
        )
        rank_mat = slot_mat[sg]
        for s in range(replicas):
            ret[tg * replicas + s] = jnp.where(top, dist_mat[s : s + 1, :], rank_mat[s : s + 1, :])
        back = (groups - dg) % groups
        every(back, lambda dr, back=back: start(ret_bufs, back, dr))
    got_ret[me] = ret[me]

    place_f = ones_at(iota((LANES, rows), 0) == spot, F32)
    for dg in order:
        every(dg, lambda dr, dg=dg: wait_recv(ret_bufs, dg, dr))
    dist_all = jnp.dot(got_ret[:, 0, :], place_f, precision=EXACT, preferred_element_type=F32)
    rank_all = jnp.dot(got_ret[:, 1, :], place_f, precision=EXACT, preferred_element_type=F32)
    dist_ref[...] = jnp.sum(owned_f * dist_all, axis=0, keepdims=True)
    rank_ref[...] = jnp.sum(owned_f * rank_all, axis=0, keepdims=True).astype(jnp.int32)
    for bufs in (id_bufs, row_bufs, ret_bufs):
        for dg in order:
            every(dg, lambda dr, dg=dg, bufs=bufs: wait_send(bufs, dg, dr))
    if extra:
        every(0, lambda dr: near_copy(peer(0, dr), me, dr).wait_send())
        for dg in order[:-1]:
            far_copy(my_group, lax.rem(my_group + dg, groups), dg).wait_send()


def fold(count, size):
    return jnp.floor((iota((1, count), 1).astype(F32) + 0.5) * (1.0 / size)).astype(jnp.int32)


def split(value):
    upper = value.astype(BF16)
    return upper, (value - upper.astype(F32)).astype(BF16)


def digits(value):
    upper = jnp.floor(value * (1.0 / 256.0))
    return upper.astype(BF16), (value - 256.0 * upper).astype(BF16)


def dot(left, right):
    return jnp.dot(left, right, preferred_element_type=F32)


def dot_nt(left, right):
    return lax.dot_general(left, right, NT, preferred_element_type=F32)


def fast_kernel(
    groups, replicas, direct, shared, spare,
    emb_in, ids_in, bounds_in,
    cent_ref, dist_ref, rank_ref, over_ref, ids_ref, bounds_ref,
    emb_ref, in_sems, over,
    unit, send_d, send_q, got_d, got_q, got_e,
    send_ids, got_ids, send_rank, got_rank, send_dist, got_dist,
    masks, total, ranks, spread,
    d_send, d_recv, id_send, id_recv, rank_send, rank_recv, dist_send, dist_recv,
    q_send, q_recv, qf_send, qf_recv, e_send, e_recv, ef_send, ef_recv,
):
    my_group = lax.axis_index("grp")
    my_replica = lax.axis_index("rep")
    me = my_group * replicas + my_replica
    owners = groups * replicas
    rows, width = emb_ref.shape
    limit = cent_ref.shape[0]
    planes, sides = replicas // 2, groups // 2
    my_plane, my_col = lax.div(my_replica, 2), lax.rem(my_replica, 2)
    my_side, my_core = lax.div(my_group, 2), lax.rem(my_group, 2)

    def turn(at, step, size):
        return lax.rem(at + step, size)

    def back(at, step, size):
        return lax.rem(at + (size - step), size)

    to_group = [turn(my_group, s, groups) for s in range(groups)]
    to_replica = [turn(my_replica, s, replicas) for s in range(replicas)]
    from_group = [back(my_group, s, groups) for s in range(groups)]
    from_replica = [back(my_replica, s, replicas) for s in range(replicas)]
    steps = [
        (dg, dr) for dg in range(groups) for dr in range(replicas) if dg or dr
    ]

    barrier = pltpu.get_barrier_semaphore()
    far_first = sorted(range(replicas), key=lambda dr: -min(dr, replicas - dr))
    greeted = [(dg, dr) for dr in far_first for dg in reversed(range(groups)) if dg or dr]
    for dg, dr in greeted:
        pl.semaphore_signal(
            barrier, inc=1, device_id=(to_group[dg], to_replica[dr]), device_id_type=MESH
        )

    def remote(src, dst, ssem, rsem, pair):
        return pltpu.make_async_remote_copy(
            src_ref=src, dst_ref=dst, send_sem=ssem, recv_sem=rsem,
            device_id=pair, device_id_type=MESH,
        )

    def pair_out(bufs, dg, dr):
        src, dst, ssem, rsem = bufs
        pair = (to_group[dg], to_replica[dr])
        there = pair[0] * replicas + pair[1]
        return remote(src.at[there], dst.at[me], ssem.at[there], rsem.at[me], pair)

    def pair_in(bufs, dg, dr):
        src, dst, ssem, rsem = bufs
        pair = (from_group[dg], from_replica[dr])
        there = pair[0] * replicas + pair[1]
        return remote(src.at[there], dst.at[there], ssem.at[there], rsem.at[there], pair)

    id_bufs = (send_ids, got_ids, id_send, id_recv)
    rank_bufs = (send_rank, got_rank, rank_send, rank_recv)

    low, half = lax.rem(my_plane, 2), lax.div(my_plane, 2)
    plane_order = [
        my_plane, half * 2 + (1 - low), (1 - half) * 2 + low, (1 - half) * 2 + (1 - low)
    ]

    def at_plane(plane, dg, dc):
        return to_group[dg], plane * 2 + lax.rem(my_col + dc, 2)

    def d_out(plane, dg, dc):
        pair = at_plane(plane, dg, dc)
        there = pair[0] * replicas + pair[1]
        return remote(
            send_d.at[there], got_d.at[my_group, my_replica],
            d_send.at[there], d_recv.at[me], pair,
        )

    def d_in(plane, dg, dc):
        pair = at_plane(plane, dg, dc)
        there = pair[0] * replicas + pair[1]
        return remote(
            send_d.at[there], got_d.at[pair], d_send.at[there], d_recv.at[there], pair
        )

    def dist_out(part, plane, dg, dc):
        pair = at_plane(plane, dg, dc)
        there = pair[0] * replicas + pair[1]
        return remote(
            send_dist.at[part, there], got_dist.at[me],
            dist_send.at[there], dist_recv.at[me], pair,
        )

    def dist_in(dg, dr):
        pair = (from_group[dg], from_replica[dr])
        there = pair[0] * replicas + pair[1]
        return remote(
            send_dist.at[0, there], got_dist.at[there],
            dist_send.at[there], dist_recv.at[there], pair,
        )

    spots = [
        (plane, dg, dc)
        for plane in plane_order
        for dg in list(range(1, groups)) + [0]
        for dc in range(2)
        if dg or dc or plane is not my_plane
    ]

    def q_out(dr):
        there = to_replica[dr]
        return remote(
            send_q.at[there], got_q.at[my_group, my_replica],
            q_send.at[dr], q_recv.at[dr], (my_group, there),
        )

    def q_in(dr):
        there = from_replica[dr]
        return remote(
            send_q.at[there], got_q.at[my_group, there],
            q_send.at[dr], q_recv.at[dr], (my_group, there),
        )

    sibling = (my_side * 2 + (1 - my_core), my_replica)

    def side_pair(ds, inward):
        side = back(my_side, ds, sides) if inward else turn(my_side, ds, sides)
        return (side * 2 + my_core, my_replica)

    def qf_side(ds, inward):
        pair = side_pair(ds, inward)
        group = pair[0] if inward else my_group
        ref = got_q.at[group]
        return remote(ref, ref, qf_send.at[ds], qf_recv.at[ds], pair)

    def qf_core(ds, inward):
        group = side_pair(ds, True)[0]
        group = group + (1 - 2 * my_core) if inward else group
        ref = got_q.at[group]
        return remote(ref, ref, qf_send.at[sides + ds], qf_recv.at[sides + ds], sibling)

    def e_plane(dp, inward):
        plane = back(my_plane, dp, planes) if inward else turn(my_plane, dp, planes)
        ref = got_e.at[my_group, my_col, plane if inward else my_plane]
        return remote(
            ref, ref, e_send.at[dp], e_recv.at[dp], (my_group, plane * 2 + my_col)
        )

    def e_spot(ds, dc, inward):
        side = back(my_side, ds, sides) if inward else turn(my_side, ds, sides)
        col = lax.rem(my_col + dc, 2)
        return side * 2 + my_core, col

    def ef_side(ds, inward):
        group = e_spot(ds, 0, inward)[0]
        ref = got_e.at[group if inward else my_group, my_col]
        return remote(
            ref, ref, ef_send.at[2 * ds], ef_recv.at[2 * ds], (group, my_replica)
        )

    def ef_col(ds, inward):
        group = e_spot(ds, 0, True)[0]
        ref = got_e.at[group, 1 - my_col if inward else my_col]
        at = 2 * ds + 1
        return remote(
            ref, ref, ef_send.at[at], ef_recv.at[at],
            (my_group, my_plane * 2 + (1 - my_col)),
        )

    def ef_core(ds, dc, inward):
        group, col = e_spot(ds, dc, True)
        group = group + (1 - 2 * my_core) if inward else group
        ref = got_e.at[group, col]
        at = groups + ds * 2 + dc
        return remote(ref, ref, ef_send.at[at], ef_recv.at[at], sibling)

    loads = [
        pltpu.make_async_copy(ids_in, ids_ref, in_sems.at[0]),
        pltpu.make_async_copy(bounds_in, bounds_ref, in_sems.at[1]),
        pltpu.make_async_copy(emb_in, emb_ref, in_sems.at[2]),
    ]
    for load in loads:
        load.start()
    loads[0].wait()
    loads[1].wait()
    ids = ids_ref[...]
    bounds = bounds_ref[...]
    diagonal = iota((owners, owners), 0) == iota((owners, owners), 1)
    edges = jnp.sum(jnp.where(diagonal, bounds, 0), axis=1, keepdims=True)
    owner = jnp.sum(ones_at(edges <= ids, F32), axis=0, keepdims=True).astype(jnp.int32) - 1
    owned = iota((owners, rows), 0) == owner
    owned_f = ones_at(owned, F32)
    earlier = ones_at(iota((rows, rows), 0) < iota((rows, rows), 1), BF16)
    prefix = dot(owned_f.astype(BF16), earlier)
    rank = jnp.sum(owned_f * prefix, axis=0, keepdims=True).astype(jnp.int32)
    column = lax.rem(owner, replicas)
    in_column = iota((replicas, rows), 0) == column
    late = rank >= direct
    column_f = ones_at(in_column, F32)
    late_f = jnp.where(late, column_f, 0.0)
    column_rank = jnp.sum(
        column_f * dot(late_f.astype(BF16), earlier), axis=0, keepdims=True
    ).astype(jnp.int32)
    in_direct = rank < direct
    in_shared = jnp.logical_and(late, column_rank < shared)
    in_spare = jnp.logical_and(late, column_rank >= shared)
    spare_f = ones_at(in_spare, F32)
    spare_rank = dot(
        jnp.broadcast_to(spare_f, (8, rows)).astype(BF16), earlier
    )[0:1, :].astype(jnp.int32)
    count = jnp.sum(spare_f, axis=1, keepdims=True)

    loads[2].wait()
    values = emb_ref[...].astype(F32)
    unit[...] = (
        values * lax.rsqrt(jnp.sum(values * values, axis=1, keepdims=True) + epsilon)
    ).astype(BF16)

    def picked(number, target):
        return dot(ones_at(iota((number, rows), 0) == target, BF16), unit[...]).astype(BF16)

    own_spare = picked(spare, jnp.where(in_spare, spare_rank, -1))
    got_e[my_group, my_col, my_plane] = own_spare
    packed = picked(replicas * shared, jnp.where(in_shared, column * shared + column_rank, -1))
    send_q[...] = packed.reshape(replicas, shared, width)
    got_q[my_group, my_replica] = send_q[my_replica]

    lane = jnp.where(
        in_direct, rank, jnp.where(in_shared, direct + column_rank, direct + shared + spare_rank)
    )
    place = ones_at(iota((LANES, rows), 0) == lane, BF16)
    near_f = jnp.concatenate([column_f] * groups, axis=0)
    chosen = jnp.where(in_direct, owned_f, jnp.where(in_shared, near_f, 1.0))
    id_high = jnp.floor(ids.astype(F32) * (1.0 / 256.0))
    id_low = ids.astype(F32) - 256.0 * id_high
    used = direct + shared + spare
    three = jnp.concatenate([chosen * id_high, chosen * id_low, chosen], axis=0).astype(BF16)
    table = dot_nt(three, place)
    table = 256.0 * table[0:owners] + table[owners : 2 * owners] + table[2 * owners :] - 1.0
    table = jnp.where(iota((owners, LANES), 1) < used, table, count)
    send_ids[...] = table.reshape(owners, 1, LANES)
    got_ids[me] = send_ids[me]

    target = jnp.where(in_direct, owner * direct + rank, -1)
    block = replicas * direct
    for tg in range(groups):
        packed = picked(block, target - tg * block)
        send_d[tg * replicas : (tg + 1) * replicas] = packed.reshape(replicas, direct, width)
    got_d[my_group, my_replica] = send_d[me]

    pl.semaphore_wait(barrier, owners - 1)
    for dp in range(1, planes):
        e_plane(dp, False).start()
    for dr in range(1, replicas):
        q_out(dr).start()
    for dg, dr in steps:
        pair_out(id_bufs, dg, dr).start()

    for spot in spots:
        d_out(*spot).start()

    for dp in range(1, planes):
        e_plane(dp, True).wait_recv()
    for ds in range(1, sides):
        ef_side(ds, False).start()
    ef_col(0, False).start()
    ef_core(0, 0, False).start()
    for dr in range(1, replicas):
        q_in(dr).wait_recv()
    for ds in range(1, sides):
        qf_side(ds, False).start()
    qf_core(0, False).start()

    def forward_sides():
        for ds in range(1, sides):
            ef_side(ds, True).wait_recv()
            ef_col(ds, False).start()
            ef_core(ds, 0, False).start()
        for ds in range(1, sides):
            qf_side(ds, True).wait_recv()
            qf_core(ds, False).start()

    def forward_col(ds):
        ef_col(ds, True).wait_recv()
        ef_core(ds, 1, False).start()

    direct_row, shared_row, spare_row = groups * block, owners * shared, owners * spare
    d_lane, q_lane, e_lane = fold(block, direct), fold(block, shared), fold(replicas * spare, spare)
    e_col = fold(replicas * spare, spare * planes)
    e_source = (e_lane - e_col * planes) * 2 + e_col
    d_slot = iota((1, block), 1) - d_lane * direct
    q_slot = iota((1, block), 1) - q_lane * shared + direct
    e_slot = iota((1, replicas * spare), 1) - e_lane * spare + (direct + shared)
    lane_source = jnp.concatenate([d_lane, q_lane, e_source], axis=1)
    lane_slot = jnp.concatenate([d_slot, q_slot, e_slot], axis=1)
    span = lane_source.shape[1]
    expand = ones_at(iota((LANES, span), 0) == lane_slot, BF16)
    from_source = ones_at(iota((replicas, span), 0) == lane_source, F32)
    key = lane_source * used + lane_slot
    key_col = jnp.sum(
        jnp.where(iota((span, span), 0) == iota((span, span), 1), key, 0), axis=1, keepdims=True
    )
    before = ones_at(key_col < key, BF16)

    def spread_rows(size, offset):
        at = jnp.floor((iota((size, LANES), 0).astype(F32) + 0.5) * (1.0 / offset[0]))
        slot = iota((size, LANES), 0) - at.astype(jnp.int32) * offset[0] + offset[1]
        return ones_at(slot == iota((size, LANES), 1), BF16)

    spread[0:direct_row] = spread_rows(direct_row, (direct, 0))
    spread[direct_row : direct_row + shared_row] = spread_rows(shared_row, (shared, direct))
    spread[direct_row + shared_row :] = spread_rows(spare_row, (spare, direct + shared))

    d_all = fold(direct_row, direct)
    q_all = fold(shared_row, shared)
    e_all = fold(spare_row, spare)
    e_group = fold(spare_row, replicas * spare)
    e_inner = e_all - e_group * replicas
    e_side = fold(spare_row, planes * spare) - e_group * 2
    e_all = e_group * replicas + (e_inner - e_side * planes) * 2 + e_side
    all_source = jnp.concatenate([d_all, q_all, e_all], axis=1)

    def by_source(row, parts):
        held = jnp.where(iota((owners, row.shape[1]), 0) == all_source, row, 0.0)
        upper, lower = parts(held)
        both = dot(jnp.concatenate([upper, lower], axis=0), spread[...])
        return both[0:owners], both[owners:]

    for dg, dr in steps:
        pair_in(id_bufs, dg, dr).wait_recv()
    named = got_ids[...].reshape(owners, LANES)
    over[0, 0] = jnp.where(jnp.max(named[:, used:]) > spare, 1, 0)
    flag = pltpu.make_async_copy(over, over_ref, in_sems.at[3])
    flag.start()
    begin = jnp.sum(jnp.where(iota((owners, 1), 0) == me, edges, 0), axis=0, keepdims=True)
    ending = jnp.sum(
        jnp.where(iota((owners, 1), 0) == me + 1, edges, 0), axis=0, keepdims=True
    ) + jnp.where(me == owners - 1, CL_DEV * owners, 0)
    begin, ending = begin.astype(F32), ending.astype(F32)
    mine = jnp.logical_and(named >= begin, named < ending)
    local = jnp.where(mine, named - begin + 1.0, 0.0)
    local_high, local_low = digits(local)
    flat_both = dot(jnp.concatenate([local_high, local_low], axis=0), expand)
    flat_all = 256.0 * flat_both[0:owners] + flat_both[owners:] - 1.0

    each, width_h = replicas // 2, planes // 2
    half_d, half_q, half_e = direct_row // 2, shared_row // 2, spare_row // 2
    hd, hq, he = fold(half_d, direct), fold(half_q, shared), fold(half_e, spare)
    gd, gq = fold(half_d, direct * each), fold(half_q, shared * each)
    ge = fold(half_e, spare * each)
    xe = fold(half_e, spare * width_h)
    base_source = jnp.concatenate([
        gd * replicas + hd - gd * each,
        gq * replicas + hq - gq * each,
        ge * replicas + (he - xe * width_h) * 2 + xe - ge * 2,
    ], axis=1)
    half_slot = jnp.concatenate([
        iota((1, half_d), 1) - hd * direct,
        iota((1, half_q), 1) - hq * shared + direct,
        iota((1, half_e), 1) - he * spare + (direct + shared),
    ], axis=1)
    part_span = half_d + half_q + half_e
    half_expand = ones_at(iota((LANES, part_span), 0) == half_slot, BF16)
    half_both = dot(jnp.concatenate([local_high, local_low], axis=0), half_expand)
    half_flat = 256.0 * half_both[0:owners] + half_both[owners:] - 1.0
    part_half = [1 - half, half]
    part_source = [base_source + at * each for at in part_half]
    for part in range(2):
        chosen_source = iota((owners, part_span), 0) == part_source[part]
        flat = jnp.sum(jnp.where(chosen_source, half_flat, 0.0), axis=0, keepdims=True)
        masks[part] = ones_at(iota((limit, part_span), 0) == flat.astype(jnp.int32), BF16)

    def part_d(part):
        return got_d[:, pl.ds(part_half[part] * each, each)].reshape(half_d, width)

    def part_q(part):
        return got_q[:, pl.ds(part_half[part] * each, each)].reshape(half_q, width)

    def part_e(part):
        return got_e[:, :, pl.ds(part_half[part] * width_h, width_h)].reshape(half_e, width)

    in_d = slice(0, half_d)
    in_q = slice(half_d, half_d + half_q)
    in_e = slice(half_d + half_q, part_span)

    seen = jnp.zeros((limit, 1), F32)
    cluster = iota((limit, span), 0)
    wide = replicas * spare
    for sg in range(groups):
        flat = jnp.sum(
            from_source * flat_all[sg * replicas : (sg + 1) * replicas], axis=0, keepdims=True
        )
        mask = ones_at(cluster == flat.astype(jnp.int32), F32)
        mask_b = mask.astype(BF16)
        ahead = dot(mask_b, before) + seen
        slot = jnp.sum(mask * ahead, axis=0, keepdims=True)
        ranks[:, sg * block : (sg + 1) * block] = slot[:, 0:block]
        at = direct_row + sg * block
        ranks[:, at : at + block] = slot[:, block : 2 * block]
        at = direct_row + shared_row + sg * wide
        ranks[:, at : at + wide] = slot[:, 2 * block :]
        seen = seen + jnp.sum(mask, axis=1, keepdims=True)
        if sg == 1:
            forward_sides()

    upper, lower = by_source(ranks[...], digits)
    send_rank[...] = (256.0 * upper + lower).reshape(owners, 1, LANES)
    got_rank[me] = send_rank[me]
    for dg, dr in steps:
        pair_out(rank_bufs, dg, dr).start()

    for ds in range(sides):
        forward_col(ds)

    for ds in range(sides):
        qf_core(ds, True).wait_recv()
    total[...] = dot(masks[0, :, in_q], part_q(0)) + dot(masks[1, :, in_q], part_q(1))
    for ds in range(sides):
        for dc in range(2):
            ef_core(ds, dc, True).wait_recv()
    for part in range(2):
        total[...] += dot(masks[part, :, in_e], part_e(part))


    def collect(ref, parts, scale):
        upper, lower = parts(ref[...].reshape(owners, LANES))
        both = dot(jnp.concatenate([upper, lower], axis=0), place)
        return jnp.sum(
            owned_f * (scale * both[0:owners] + both[owners:]), axis=0, keepdims=True
        )


    close = len(spots) - 4 * groups
    for spot in spots[:close]:
        d_in(*spot).wait_recv()
    total[...] += dot(masks[1, :, in_d], part_d(1))
    for spot in spots[close:]:
        d_in(*spot).wait_recv()
    sums = total[...] + dot(masks[0, :, in_d], part_d(0))
    share = 1.0 / jnp.maximum(seen, 1.0)
    norm = share * jnp.sqrt(jnp.sum(sums * sums, axis=1, keepdims=True))
    cent_ref[...] = (sums * (share / jnp.maximum(norm, norm_floor))).astype(BF16)

    def near(part, inside, block_rows):
        score = dot_nt(cent_ref[...], block_rows)
        return jnp.sum(
            masks[part, :, inside].astype(F32) * score, axis=0, keepdims=True
        )

    half_spread = jnp.concatenate([
        spread[0:half_d],
        spread[direct_row : direct_row + half_q],
        spread[direct_row + shared_row : direct_row + shared_row + half_e],
    ], axis=0)
    for part in range(2):
        nears = jnp.concatenate([
            near(part, in_d, part_d(part)),
            near(part, in_q, part_q(part)),
            near(part, in_e, part_e(part)),
        ], axis=1)
        held = jnp.where(iota((owners, part_span), 0) == part_source[part], nears, 0.0)
        upper, lower = split(held)
        both = dot(jnp.concatenate([upper, lower], axis=0), half_spread)
        send_dist[part] = (both[0:owners] + both[owners:]).reshape(owners, 1, LANES)
        for spot in (spots[:close] if part else spots[close:])[::-1]:
            dist_out(part, *spot).start()
    got_dist[me] = send_dist[1, me]

    for dg, dr in steps:
        pair_in(rank_bufs, dg, dr).wait_recv()
    rank_ref[...] = collect(got_rank, digits, 256.0).astype(jnp.int32)
    for bufs in (id_bufs, rank_bufs):
        for dg, dr in steps:
            pair_out(bufs, dg, dr).wait_send()
    for spot in spots:
        d_out(*spot).wait_send()
    for dp in range(1, planes):
        e_plane(dp, False).wait_send()
    for dr in range(1, replicas):
        q_out(dr).wait_send()
    for ds in range(1, sides):
        ef_side(ds, False).wait_send()
    for ds in range(1, sides):
        qf_side(ds, False).wait_send()
    for ds in range(sides):
        qf_core(ds, False).wait_send()
        ef_col(ds, False).wait_send()
        for dc in range(2):
            ef_core(ds, dc, False).wait_send()

    for dg, dr in steps:
        dist_in(dg, dr).wait_recv()
    flag.wait()
    dist_ref[...] = 1.0 - collect(got_dist, split, 1.0)
    for at, spot in enumerate(spots):
        dist_out(1 if at < len(spots) - 4 * groups else 0, *spot).wait_send()


def store_kernel(cent_ref, dist_ref, rank_ref, cent_out, dist_out, rank_out, sems):
    pieces = sems.shape[0] - 2
    size = cent_ref.shape[0] // pieces
    copies = [
        pltpu.make_async_copy(
            cent_ref.at[pl.ds(at * size, size)], cent_out.at[pl.ds(at * size, size)], sems.at[at]
        )
        for at in range(pieces)
    ]
    copies.append(pltpu.make_async_copy(dist_ref, dist_out, sems.at[pieces]))
    copies.append(pltpu.make_async_copy(rank_ref, rank_out, sems.at[pieces + 1]))
    for copy in copies:
        copy.start()
    for copy in copies:
        copy.wait()


def solution(mesh):
    groups, replicas = mesh.shape["grp"], mesh.shape["rep"]
    owners = groups * replicas

    def shards(embeddings, cluster_ids, owner_bounds):
        rows, width = embeddings.shape
        limit = CL_DEV + CL_DEV // 2
        most = -(-(3 * rows // owners) // 16) * 16
        direct, shared, spare = 16, 16, 32
        vmem = pl.BlockSpec(memory_space=pltpu.VMEM)
        scalar = pl.BlockSpec(memory_space=pltpu.SMEM)
        anywhere = pl.BlockSpec(memory_space=pl.ANY)
        outside = pl.BlockSpec(memory_space=pltpu.HBM)
        each = pltpu.SemaphoreType.DMA((owners,))
        ids_row = cluster_ids.reshape(1, rows)
        bounds_row = owner_bounds.reshape(1, owners)
        outs = (
            jax.ShapeDtypeStruct((limit, width), BF16),
            jax.ShapeDtypeStruct((1, rows), F32),
            jax.ShapeDtypeStruct((1, rows), jnp.int32),
            jax.ShapeDtypeStruct((1, 1), jnp.int32),
        )

        def run(number, ids_in, bounds_in):
            small = pltpu.VMEM((owners, 8, LANES), F32)
            near = pltpu.SemaphoreType.DMA((replicas,))
            far = pltpu.SemaphoreType.DMA((groups,))
            return pl.pallas_call(
                functools.partial(kernel, groups, replicas, most, 0),
                out_shape=outs,
                in_specs=[anywhere] * 3,
                out_specs=(vmem, vmem, vmem, scalar),
                scratch_shapes=[
                    pltpu.VMEM((rows, width), BF16),
                    pltpu.VMEM((1, rows), jnp.int32),
                    pltpu.VMEM((1, owners), jnp.int32),
                    pltpu.SemaphoreType.DMA((3,)),
                    pltpu.VMEM((rows, width), BF16),
                    pltpu.VMEM((owners, most, width), BF16),
                    pltpu.VMEM((owners, most, width), BF16),
                    small,
                    small,
                    pltpu.VMEM((groups, limit, replicas * most), BF16),
                    pltpu.VMEM((limit, width), F32),
                    small,
                    small,
                    pltpu.VMEM((groups, replicas, LANES), F32),
                    each, each, each, each, each, each, near, near, far, far,
                ],
                compiler_params=pltpu.CompilerParams(
                    collective_id=number,
                    has_side_effects=True,
                    vmem_limit_bytes=48 * 1024 * 1024,
                ),
            )(embeddings, ids_in, bounds_in)

        def run_fast(number):
            small = pltpu.VMEM((owners, 1, LANES), F32)
            slots = owners * (direct + shared + spare)
            return pl.pallas_call(
                functools.partial(fast_kernel, groups, replicas, direct, shared, spare),
                out_shape=outs + (
                    jax.ShapeDtypeStruct((1, rows), jnp.int32),
                    jax.ShapeDtypeStruct((1, owners), jnp.int32),
                ),
                in_specs=[outside] * 3,
                out_specs=(vmem, vmem, vmem, outside, vmem, vmem),
                scratch_shapes=[
                    pltpu.VMEM((rows, width), BF16),
                    pltpu.SemaphoreType.DMA((4,)),
                    pltpu.SMEM((1, 1), jnp.int32),
                    pltpu.VMEM((rows, width), BF16),
                    pltpu.VMEM((owners, direct, width), BF16),
                    pltpu.VMEM((replicas, shared, width), BF16),
                    pltpu.VMEM((groups, replicas, direct, width), BF16),
                    pltpu.VMEM((groups, replicas, shared, width), BF16),
                    pltpu.VMEM((groups, 2, replicas // 2, spare, width), BF16),
                    small, small, small, small,
                    pltpu.VMEM((2, owners, 1, LANES), F32), small,
                    pltpu.VMEM((2, limit, slots // 2), BF16),
                    pltpu.VMEM((limit, width), F32),
                    pltpu.VMEM((1, slots), F32),
                    pltpu.VMEM((slots, LANES), BF16),
                    each, each, each, each, each, each, each, each,
                    pltpu.SemaphoreType.DMA((replicas,)),
                    pltpu.SemaphoreType.DMA((replicas,)),
                    pltpu.SemaphoreType.DMA((groups,)),
                    pltpu.SemaphoreType.DMA((groups,)),
                    pltpu.SemaphoreType.DMA((replicas // 2,)),
                    pltpu.SemaphoreType.DMA((replicas // 2,)),
                    pltpu.SemaphoreType.DMA((2 * groups,)),
                    pltpu.SemaphoreType.DMA((2 * groups,)),
                ],
                compiler_params=pltpu.CompilerParams(
                    collective_id=number,
                    has_side_effects=True,
                    vmem_limit_bytes=48 * 1024 * 1024,
                ),
            )(*(pltpu.with_memory_space_constraint(x, pltpu.HBM) for x in (embeddings, ids_row, bounds_row)))

        def stored(results):
            return tuple(
                pl.pallas_call(
                    store_kernel,
                    out_shape=outs[:3],
                    in_specs=[vmem] * 3,
                    out_specs=(anywhere,) * 3,
                    scratch_shapes=[pltpu.SemaphoreType.DMA((6,))],
                    compiler_params=pltpu.CompilerParams(vmem_limit_bytes=4 * 1024 * 1024),
                )(*results[:3])
            )

        whole = groups == 4 and replicas * direct == LANES and rows // owners <= direct
        if most > 2 * direct and whole:
            first = run_fast(0)
            kept = stored(first)
            centroids, distance, rank = lax.cond(
                first[3][0, 0] > 0, lambda: stored(run(1, first[4], first[5])), lambda: kept
            )
        else:
            centroids, distance, rank, _ = run(0, ids_row, bounds_row)
        return distance.reshape(rows), rank.reshape(rows), centroids[None]

    placed = (P(("grp", "rep"), None), P(("grp", "rep")), P())
    return jax.shard_map(
        shards,
        mesh=mesh,
        in_specs=placed,
        out_specs=(P(("grp", "rep")), P(("grp", "rep")), P(("grp", "rep"), None, None)),
        check_vma=False,
    )
```
